32 devices in a mesh: mesh: 2 (over core), dom: 16 (over z, y, x).
Axes of the slice: x: 2, y: 2, z: 4, core: 2. Of those that a mesh axis runs over, the one named last changes fastest.
Arguments:
- donor_fields: float32 [5, 512, 4096], P(None, None, ('mesh', 'dom')), may hold values from -6 to 6
- interp_weights: float32 [3, 8, 65536], P(None, None, ('mesh', 'dom')), may hold values from -1 to 1, as said below
- donor_owner: int32 [65536, 1], P(('mesh', 'dom')), may hold values from 0 to 15, as said below
- donor_element: int32 [65536], P(('mesh', 'dom')), may hold values from 0 to 127
- geometry: float32 [4, 4096], P(None, ('mesh', 'dom')), may hold values from 0.25 to 4
- wall_flag: int32 [2, 256], P(None, ('mesh', 'dom')), may hold values 0 or 1
- forcing: float32 [512, 4096], P(None, ('mesh', 'dom')), may hold values from -6 to 6
Outputs:
- velocity: float32 [512, 4096], P(None, ('mesh', 'dom'))
- residual: float32 [512, 4096], P(None, ('mesh', 'dom'))
- interface_values: float32 [5, 65536], P(None, ('mesh', 'dom'))
The draws below stay inside these ranges and needn't reach their ends.
Inputs may be any that keep to these rules, and one draw needn't show every extreme that they name: `interp_weights`: for each receptor and direction, the 8 entries are the Lagrange polynomials of the order-7 Gauss-Lobatto-Legendre points evaluated at one point of [-1, 1]. `donor_owner`: the receptors of block q of a mesh (the rows of one device) name donor dom indices from q - 2 to q + 2 only; among them one index is named exactly 1024 times and no index more often.
All inputs are finite; a program needn't handle non-finite values. No bound on the sum of `wall_flag` on one device may be relied on, other than what follows from the above.
Results may differ from the reference program's by a relative error of at most 0.00026.
Values sent between devices are 32-bit elements; how exact they have to be, the bound alone decides.
A program may use at most 192 MiB of HBM per device.

```python
import math
import jax
import jax.numpy as jnp
import numpy as np
from jax import lax

FIELDS = 5
EX = 8
EY = 16
EZ_DEV = 1
ITERS = 3
PTS = 512
E_DEV = 128
E_TOTAL = 4096
R_DEV = 2048
R_TOTAL = 65536
CAP = 1024
W_TOTAL = 256
N_MESH = 2
N_DOM = 16


def legendre_pair_drawn(values, degree):
    previous = values * 0.0 + 1.0
    current = values * 1.0
    for poly_order in range(2, degree + 1):
        previous, current = (current, ((2 * poly_order - 1) * values * current - (poly_order - 1) * previous) / poly_order)
    return (current, previous)


def gll_abscissae():
    degree = 7
    points_count = degree + 1
    abscissae = np.cos(np.pi * np.arange(points_count) / degree)
    for newton_turn in range(80):
        top_poly, lower_poly = legendre_pair_drawn(abscissae, degree)
        abscissae = abscissae - (abscissae * top_poly - lower_poly) / (points_count * top_poly)
    return np.sort(abscissae)


def draw_interp_weights(key, part):
    abscissae = gll_abscissae()
    location = jax.random.uniform(key, (3, R_TOTAL), jnp.float32, -1.0, 1.0)
    basis_rows = []
    for node_index in range(8):
        product = jnp.ones_like(location)
        for partner in range(8):
            if partner != node_index:
                product = product * (location - abscissae[partner]) / (abscissae[node_index] - abscissae[partner])
        basis_rows.append(product)
    return jnp.stack(basis_rows, 1).astype(jnp.float32)


def draw_donor_owner(key, part):
    block_count = N_MESH * N_DOM
    slab_index = jnp.arange(block_count, dtype=jnp.int32) % N_DOM
    lowest = jnp.maximum(slab_index - 2, 0)
    highest = jnp.minimum(slab_index + 2, N_DOM - 1)
    window = highest - lowest + 1
    hot_owner = lowest + jax.random.randint(jax.random.fold_in(key, 11), (block_count,), 0, window)
    picks = jax.random.randint(jax.random.fold_in(key, 13), (block_count, R_DEV), 0, (window - 1)[:, None])
    other_owner = lowest[:, None] + picks
    other_owner = other_owner + (other_owner >= hot_owner[:, None]).astype(jnp.int32)
    block_keys = jax.random.split(jax.random.fold_in(key, 17), block_count)
    ranks = jax.vmap(lambda one_key: jax.random.permutation(one_key, R_DEV))(block_keys)
    owner = jnp.where(ranks < CAP, hot_owner[:, None], other_owner)
    return owner.reshape(R_TOTAL, 1).astype(jnp.int32)


def place_ends(values, own_key, smallest, largest):
    index_at = [jax.random.randint(jax.random.fold_in(own_key, axis), (), 0, length) for axis, length in enumerate(values.shape)]
    main_axis = values.shape.index(max(values.shape))
    next_to = index_at[:main_axis] + [(index_at[main_axis] + 1) % values.shape[main_axis]] + index_at[main_axis + 1:]
    return values.at[tuple(index_at)].set(smallest).at[tuple(next_to)].set(largest)


def shard_levels(own_key, shape, pieces, least, top_value):
    loudness = 1.0
    for axis_at, blocks in pieces:
        draws = jax.random.uniform(jax.random.fold_in(jax.random.fold_in(own_key, 6), axis_at), (blocks,), jnp.float32, least / len(pieces), top_value / len(pieces))
        loudness = loudness * jnp.repeat(jnp.exp(draws), shape[axis_at] // blocks).reshape((-1,) + (1,) * (len(shape) - 1 - axis_at))
    return loudness


def noise(key, dims, deviation, bound, shards=(), kind=jnp.bfloat16):
    values = jax.random.normal(key, dims, jnp.float32) * deviation
    if len(shards) > 0:
        values = shard_levels(key, dims, shards, -0.22, 0.18) * values
    return jnp.clip(values, min=-bound, max=bound).astype(kind)


def setup_inputs(seed: int = 0) -> dict:
    seeds = jax.random.split(jax.random.key(seed), 8)
    donor_fields = noise(seeds[0], (FIELDS, PTS, E_TOTAL), 1.0, 6.0, ((2, 32),), jnp.float32)
    interp_weights = draw_interp_weights(jax.random.fold_in(seeds[7], 71), 0)
    donor_owner = draw_donor_owner(jax.random.fold_in(seeds[7], 71), 0)
    donor_element = place_ends(jax.random.randint(seeds[3], (R_TOTAL,), 0, E_DEV), jax.random.fold_in(seeds[3], 1), 0, E_DEV - 1).astype(jnp.int32)
    geometry = jnp.clip(jnp.exp(math.log(4.0) - 2.7725887 * jax.random.uniform(seeds[4], (4, E_TOTAL), jnp.float32) ** shard_levels(seeds[4], (4, E_TOTAL), ((1, 32),), -0.2, 0.2)), 0.25, 4.0)
    wall_flag = place_ends((jax.random.randint(seeds[5], (2, W_TOTAL), 0, 4) < 3).astype(jnp.int32), jax.random.fold_in(seeds[5], 1), 0, 1)
    forcing = noise(seeds[6], (PTS, E_TOTAL), 1.0, 6.0, ((1, 32),), jnp.float32)
    return {"donor_fields": donor_fields, "interp_weights": interp_weights, "donor_owner": donor_owner, "donor_element": donor_element, "geometry": geometry, "wall_flag": wall_flag, "forcing": forcing}


HIGHEST = lax.Precision.HIGHEST


def legendre_pair(values, degree):
    previous = values * 0.0 + 1.0
    current = values * 1.0
    for poly_order in range(2, degree + 1):
        previous, current = current, ((2 * poly_order - 1) * values * current - (poly_order - 1) * previous) / poly_order
    return current, previous


def gll_tables():
    degree = 7
    points_count = degree + 1
    abscissae = np.cos(np.pi * np.arange(points_count) / degree)
    for newton_turn in range(80):
        top_poly, lower_poly = legendre_pair(abscissae, degree)
        abscissae = abscissae - (abscissae * top_poly - lower_poly) / (points_count * top_poly)
    abscissae = np.sort(abscissae)
    top_poly, lower_poly = legendre_pair(abscissae, degree)
    quad_weights = 2.0 / (degree * points_count * top_poly * top_poly)
    identity_mat = np.eye(points_count)
    spacing = abscissae[:, None] - abscissae[None, :] + identity_mat
    derivative = (top_poly[:, None] / (top_poly[None, :] * spacing)) * (1.0 - identity_mat)
    derivative[0, 0] = -degree * points_count / 4.0
    derivative[degree, degree] = degree * points_count / 4.0
    return jnp.asarray(derivative, jnp.float32), jnp.asarray(quad_weights, jnp.float32)


def cube_weights(quad_weights):
    return quad_weights[:, None, None, None] * quad_weights[None, :, None, None] * quad_weights[None, None, :, None]


def local_operator(field_data, geometry, derivative, quad_weights):
    weights_cube = cube_weights(quad_weights)
    grad_x = jnp.einsum('ai,kjie->kjae', derivative, field_data, precision=HIGHEST)
    grad_y = jnp.einsum('aj,kjie->kaie', derivative, field_data, precision=HIGHEST)
    grad_z = jnp.einsum('ak,kjie->ajie', derivative, field_data, precision=HIGHEST)
    result = jnp.einsum('ai,kjae->kjie', derivative, grad_x * (weights_cube * geometry[0]), precision=HIGHEST)
    result = result + jnp.einsum('aj,kaie->kjie', derivative, grad_y * (weights_cube * geometry[1]), precision=HIGHEST)
    result = result + jnp.einsum('ak,ajie->kjie', derivative, grad_z * (weights_cube * geometry[2]), precision=HIGHEST)
    return result + (weights_cube * geometry[3]) * field_data


def local_diagonal(geometry, derivative, quad_weights):
    stiff_diag = jnp.sum(derivative * derivative * quad_weights[:, None], axis=0)
    along_x = (quad_weights[:, None, None] * quad_weights[None, :, None] * stiff_diag[None, None, :])[..., None]
    along_y = (quad_weights[:, None, None] * stiff_diag[None, :, None] * quad_weights[None, None, :])[..., None]
    along_z = (stiff_diag[:, None, None] * quad_weights[None, :, None] * quad_weights[None, None, :])[..., None]
    return along_x * geometry[0] + along_y * geometry[1] + along_z * geometry[2] + cube_weights(quad_weights) * geometry[3]


def direct_sum(field_data):
    paired = field_data[:, :, :, -1, :, :, :-1] + field_data[:, :, :, 0, :, :, 1:]
    field_data = field_data.at[:, :, :, -1, :, :, :-1].set(paired).at[:, :, :, 0, :, :, 1:].set(paired)
    paired = field_data[:, :, -1, :, :, :-1, :] + field_data[:, :, 0, :, :, 1:, :]
    field_data = field_data.at[:, :, -1, :, :, :-1, :].set(paired).at[:, :, 0, :, :, 1:, :].set(paired)
    paired = field_data[:, -1, :, :, :-1, :, :] + field_data[:, 0, :, :, 1:, :, :]
    field_data = field_data.at[:, -1, :, :, :-1, :, :].set(paired).at[:, 0, :, :, 1:, :, :].set(paired)
    return field_data


def reference(donor_fields, interp_weights, donor_owner, donor_element, geometry, wall_flag, forcing):
    derivative, quad_weights = gll_tables()
    elem_dev = EX * EY * EZ_DEV
    elem_mesh = elem_dev * N_DOM
    rec_mesh = R_DEV * N_DOM
    layers = EZ_DEV * N_DOM
    receptor_mesh = jnp.arange(R_TOTAL, dtype=jnp.int32) // rec_mesh
    target = ((1 - receptor_mesh) * elem_mesh + donor_owner[:, 0] * elem_dev + donor_element).astype(jnp.int32)
    blocks = N_MESH * N_DOM
    target_blocks = target.reshape(blocks, R_DEV)
    weight_blocks = jnp.transpose(interp_weights.reshape(3, 8, blocks, R_DEV), (2, 0, 1, 3))

    def evaluate(block_pair):
        target_row, weight_row = block_pair
        gathered = jnp.take(donor_fields, target_row, axis=2).reshape(FIELDS, 8, 8, 8, R_DEV)
        reduced = jnp.einsum('fkjib,ib->fkjb', gathered, weight_row[0], precision=HIGHEST)
        reduced = jnp.einsum('fkjb,jb->fkb', reduced, weight_row[1], precision=HIGHEST)
        return jnp.einsum('fkb,kb->fb', reduced, weight_row[2], precision=HIGHEST)

    evaluated = lax.map(evaluate, (target_blocks, weight_blocks))
    interface_values = jnp.transpose(evaluated, (1, 0, 2)).reshape(FIELDS, R_TOTAL)

    brick_shape = (8, 8, 8, layers, EY, EX)
    flat_shape = (8, 8, 8, elem_mesh)
    weights_cube = cube_weights(quad_weights)
    velocities = []
    residuals = []
    for mesh_index in range(N_MESH):
        first_column = mesh_index * elem_mesh
        mesh_geometry = geometry[:, first_column:first_column + elem_mesh]
        source = forcing[:, first_column:first_column + elem_mesh].reshape(flat_shape)
        received = interface_values[0, mesh_index * rec_mesh:(mesh_index + 1) * rec_mesh]
        received = received.reshape(N_DOM, 2, EZ_DEV, EY, 8, 8)
        side_values = jnp.transpose(received, (1, 4, 5, 0, 2, 3)).reshape(2, 8, 8, layers, EY)
        wall_bits = wall_flag[:, mesh_index * EX * layers:(mesh_index + 1) * EX * layers].reshape(2, layers, EX)
        wall_bits = wall_bits.astype(jnp.float32)
        zero_brick = jnp.zeros(brick_shape, jnp.float32)
        rec_value = zero_brick.at[:, :, 0, :, :, 0].set(side_values[0]).at[:, :, -1, :, :, -1].set(side_values[1])
        rec_mark = zero_brick.at[:, :, 0, :, :, 0].set(1.0).at[:, :, -1, :, :, -1].set(1.0)
        wall_low = jnp.broadcast_to(wall_bits[0], (8, 8, layers, EX))
        wall_high = jnp.broadcast_to(wall_bits[1], (8, 8, layers, EX))
        wall_mark = zero_brick.at[:, 0, :, :, 0, :].set(wall_low).at[:, -1, :, :, -1, :].set(wall_high)
        diag_brick = local_diagonal(mesh_geometry, derivative, quad_weights).reshape(brick_shape)
        unit_brick = jnp.ones(brick_shape, jnp.float32)
        summed = direct_sum(jnp.stack([rec_value, rec_mark, wall_mark, unit_brick, diag_brick], 0))
        summed = summed.reshape((5,) + flat_shape)
        free_mask = 1.0 - jnp.minimum(summed[1] + summed[2], 1.0)
        boundary = summed[0] / jnp.maximum(summed[1], 1.0)
        multiplicity = summed[3]
        inverse = free_mask / summed[4]

        def apply_operator(vector):
            local_term = local_operator(vector, mesh_geometry, derivative, quad_weights)
            return free_mask * direct_sum(local_term.reshape((1,) + brick_shape))[0].reshape(flat_shape)

        def inner(left, right):
            return jnp.sum(left * right / multiplicity)

        loaded = (weights_cube * mesh_geometry[3]) * source - local_operator(boundary, mesh_geometry, derivative, quad_weights)
        rhs = free_mask * direct_sum(loaded.reshape((1,) + brick_shape))[0].reshape(flat_shape)
        solution = jnp.zeros(flat_shape, jnp.float32)
        residual_now = rhs
        precond = inverse * residual_now
        direction = precond
        precond_norm = inner(residual_now, precond)
        for iteration in range(ITERS):
            operator_image = apply_operator(direction)
            step_length = precond_norm / inner(direction, operator_image)
            solution = solution + step_length * direction
            residual_now = residual_now - step_length * operator_image
            if iteration + 1 < ITERS:
                precond = inverse * residual_now
                norm_next = inner(residual_now, precond)
                direction = precond + (norm_next / precond_norm) * direction
                precond_norm = norm_next
        velocities.append((boundary + solution).reshape(PTS, elem_mesh))
        residuals.append(residual_now.reshape(PTS, elem_mesh))
    return jnp.concatenate(velocities, 1), jnp.concatenate(residuals, 1), interface_values
```

```python
import functools

import jax
import jax.numpy as jnp
import numpy as np
from jax import lax
from jax.experimental import pallas as pl
from jax.experimental.pallas import tpu as pltpu
from jax.sharding import PartitionSpec as P

EX = 8
EY = 16
ITERS = 3
REACH = 2
CHUNK = 256
ORDER = (0, 7, 1, 2, 3, 4, 5, 6)
MESH = pl.DeviceIdType.MESH


def legendre_pair(values, degree):
    previous = values * 0.0 + 1.0
    current = values * 1.0
    for poly_order in range(2, degree + 1):
        previous, current = (
            current,
            ((2 * poly_order - 1) * values * current - (poly_order - 1) * previous) / poly_order,
        )
    return (current, previous)


def gll_tables():
    degree = 7
    points_count = degree + 1
    abscissae = np.cos(np.pi * np.arange(points_count) / degree)
    for newton_turn in range(80):
        top_poly, lower_poly = legendre_pair(abscissae, degree)
        abscissae = abscissae - (abscissae * top_poly - lower_poly) / (points_count * top_poly)
    abscissae = np.sort(abscissae)
    top_poly, lower_poly = legendre_pair(abscissae, degree)
    quad_weights = 2.0 / (degree * points_count * top_poly * top_poly)
    identity_mat = np.eye(points_count)
    spacing = abscissae[:, None] - abscissae[None, :] + identity_mat
    derivative = top_poly[:, None] / (top_poly[None, :] * spacing) * (1.0 - identity_mat)
    derivative[0, 0] = -degree * points_count / 4.0
    derivative[degree, degree] = degree * points_count / 4.0
    return (abscissae, derivative, quad_weights)


def kernel(
    n,
    donor_hbm,
    weights_hbm,
    owner_hbm,
    element_hbm,
    geometry_hbm,
    wall_hbm,
    forcing_hbm,
    velocity_ref,
    residual_ref,
    interface_ref,
    donor_ref,
    forcing_ref,
    weights_ref,
    owner_ref,
    element_ref,
    geometry_ref,
    wall_ref,
    position_ref,
    request_ref,
    moves,
    along_y_ref,
    along_x_ref,
    plane_ref,
    load_sem,
    split,
    asked,
    answer,
    answered,
    faces,
    halo,
    dots,
    all_dots,
    state,
    image,
    direction,
    direction_image,
    inverse,
    free,
    sharing,
    boundary,
    ask_send,
    ask_recv,
    reply_send,
    reply_recv,
    face_send,
    face_recv,
    dot_send,
    dot_recv,
):
    points, derivative, quad = gll_tables()
    stiff = (derivative.T * quad) @ derivative / quad[:, None]
    fields = donor_ref.shape[0]
    elems = donor_ref.shape[2]
    height = owner_ref.shape[0]
    lanes = owner_ref.shape[1]
    receptors = height * lanes
    room = request_ref.shape[2]
    slots = 2 * REACH + 1
    mesh_id = lax.axis_index("mesh")
    slab = lax.axis_index("dom")
    other = 1 - mesh_id

    pairs = [
        (weights_hbm, weights_ref),
        (owner_hbm, owner_ref),
        (element_hbm, element_ref),
        (donor_hbm, donor_ref),
        (geometry_hbm, geometry_ref),
        (wall_hbm, wall_ref),
        (forcing_hbm, forcing_ref),
    ]
    loads = [
        pltpu.make_async_copy(source, target, load_sem.at[at])
        for at, (source, target) in enumerate(pairs)
    ]
    for load in loads:
        load.start()

    def inside(index):
        return jnp.logical_and(index >= 0, index < n)

    barrier = pltpu.get_barrier_semaphore()
    greeted = n - 1
    for step in range(1, n):
        pl.semaphore_signal(
            barrier, inc=1, device_id=(mesh_id, lax.rem(slab + step, n)), device_id_type=MESH
        )
    for shift in range(-REACH, REACH + 1):
        greeted = greeted + jnp.where(inside(slab + shift), 1, 0)

        @pl.when(inside(slab + shift))
        def _():
            pl.semaphore_signal(
                barrier, inc=1, device_id=(other, slab + shift), device_id_type=MESH
            )

    for load in loads[:3]:
        load.wait()
    depth = lax.broadcasted_iota(jnp.int32, (8, lanes), 0)
    ladder = jnp.zeros((8, lanes), jnp.float32)
    for a in range(8):
        ladder = jnp.where(depth == a, float(points[a]), ladder)
    for d in range(3):
        for row in range(height):
            part = weights_ref[d, :, row * lanes : (row + 1) * lanes] * ladder
            position_ref[d, row : row + 1, :] = jnp.sum(part, axis=0, keepdims=True)
    owner = owner_ref[...]
    element_code = element_ref[...] * receptors
    members = [owner == slab + shift for shift in range(-REACH, REACH + 1)]
    tall = slots * height
    marks = jnp.concatenate([jnp.where(m, 1.0, 0.0) for m in members], 0).astype(jnp.bfloat16)
    before = lax.broadcasted_iota(jnp.int32, (lanes, lanes), 0)
    after = lax.broadcasted_iota(jnp.int32, (lanes, lanes), 1)
    upper = jnp.where(before < after, 1.0, 0.0).astype(jnp.bfloat16)
    left = jnp.dot(marks, upper, preferred_element_type=jnp.float32).astype(jnp.bfloat16)
    above = lax.broadcasted_iota(jnp.int32, (tall, tall), 0)
    below = lax.broadcasted_iota(jnp.int32, (tall, tall), 1)
    same = above // height == below // height
    block = jnp.where(same, 1.0, 0.0).astype(jnp.bfloat16)
    lower = jnp.where(same & (below < above), 1.0, 0.0).astype(jnp.bfloat16)
    rank = jnp.dot(block, left, preferred_element_type=jnp.float32)
    rank = rank + jnp.dot(lower, marks, preferred_element_type=jnp.float32)
    rank = rank.astype(jnp.int32)
    row_index = lax.broadcasted_iota(jnp.int32, (height, lanes), 0)
    place = lax.broadcasted_iota(jnp.int32, (height, lanes), 1) * height + row_index
    row_bits = height.bit_length() - 1
    steps = receptors.bit_length() - 1

    def pull(tile, step):
        if step >= row_bits:
            return pltpu.roll(tile, lanes - (1 << (step - row_bits)), 1)
        jump = 1 << step
        near = pltpu.roll(tile, height - jump, 0)
        far = pltpu.roll(near, lanes - 1, 1)
        return jnp.where(row_index < height - jump, near, far)

    def push(tile, step):
        if step >= row_bits:
            return pltpu.roll(tile, 1 << (step - row_bits), 1)
        jump = 1 << step
        near = pltpu.roll(tile, jump, 0)
        far = pltpu.roll(near, 1, 1)
        return jnp.where(row_index >= jump, near, far)

    words = []
    comps = []
    start = [position_ref[d] for d in range(3)]
    for slot in range(slots):
        shift = place - rank[slot * height : (slot + 1) * height]
        words.append(jnp.where(members[slot], element_code + shift, 0))
        comps.append(list(start))
    for step in range(steps):
        for slot in range(slots):
            word = words[slot]
            moving = word & (1 << step)
            moves[step, slot] = moving
            came = pull(word, step)
            take = (came & (1 << step)) != 0
            words[slot] = jnp.where(take, came - (1 << step), jnp.where(moving != 0, 0, word))
            comps[slot] = [jnp.where(take, pull(c, step), c) for c in comps[slot]]
    half = lanes // 2
    left_half = lax.broadcasted_iota(jnp.int32, (room, lanes), 1) < half
    for slot in range(slots):
        columns = comps[slot] + [(words[slot] // receptors).astype(jnp.float32)]
        for at, column in enumerate(columns):
            request_ref[slot, at] = jnp.where(
                left_half, column[:room], pltpu.roll(column[room:], half, 1)
            )

    pl.semaphore_wait(barrier, greeted)

    def ask(shift):
        return pltpu.make_async_remote_copy(
            src_ref=request_ref.at[shift + REACH],
            dst_ref=asked.at[shift + REACH],
            send_sem=ask_send.at[shift + REACH],
            recv_sem=ask_recv.at[shift + REACH],
            device_id=(other, lax.rem(slab + shift + n, n)),
            device_id_type=MESH,
        )

    def reply(shift):
        return pltpu.make_async_remote_copy(
            src_ref=answer.at[shift + REACH],
            dst_ref=answered.at[shift + REACH],
            send_sem=reply_send.at[shift + REACH],
            recv_sem=reply_recv.at[shift + REACH],
            device_id=(other, lax.rem(slab - shift + n, n)),
            device_id_type=MESH,
        )

    def face_copy(phase, up):
        step = 1 if up else n - 1
        return pltpu.make_async_remote_copy(
            src_ref=faces.at[phase, 1 if up else 0],
            dst_ref=halo.at[phase, 0 if up else 1],
            send_sem=face_send.at[phase, 1 if up else 0],
            recv_sem=face_recv.at[phase, 0 if up else 1],
            device_id=(mesh_id, lax.rem(slab + step, n)),
            device_id_type=MESH,
        )

    def send_faces(phase):
        @pl.when(slab < n - 1)
        def _():
            face_copy(phase, True).start()

        @pl.when(slab > 0)
        def _():
            face_copy(phase, False).start()

    def wait_faces(phase):
        @pl.when(slab > 0)
        def _():
            face_copy(phase, True).wait_recv()

        @pl.when(slab < n - 1)
        def _():
            face_copy(phase, False).wait_recv()

        @pl.when(slab < n - 1)
        def _():
            face_copy(phase, True).wait_send()

        @pl.when(slab > 0)
        def _():
            face_copy(phase, False).wait_send()

    def dot_copy(turn, step):
        return pltpu.make_async_remote_copy(
            src_ref=dots.at[turn],
            dst_ref=all_dots.at[turn, slab],
            send_sem=dot_send.at[turn, step],
            recv_sem=dot_recv.at[turn, step],
            device_id=(mesh_id, lax.rem(slab + step, n)),
            device_id_type=MESH,
        )

    for distance in range(REACH + 1):
        for shift in sorted({distance, -distance}):

            @pl.when(inside(slab + shift))
            def _():
                ask(shift).start()

    phases = halo.shape[0]
    blank = jnp.zeros(halo.shape[2:], jnp.float32)

    @pl.when(slab == 0)
    def _():
        for phase in range(phases):
            halo[phase, 0] = blank

    @pl.when(slab == n - 1)
    def _():
        for phase in range(phases):
            halo[phase, 1] = blank

    node = lax.broadcasted_iota(jnp.int32, (8, elems), 0)
    element = lax.broadcasted_iota(jnp.int32, (8, elems), 1)
    x_index = element % EX
    y_index = element // EX % EY

    across = jnp.zeros((8, elems), jnp.float32)
    for a in range(8):
        across = jnp.where(node == a, float(quad[a]), across)
    for j in range(8):
        plane_ref[j] = across * float(quad[j])
        for m in range(8):
            along_y_ref[m, j] = jnp.full((8, elems), float(stiff[j, m]), jnp.float32)
    for step in range(8):
        turned = jnp.zeros((8, elems), jnp.float32)
        for i in range(8):
            turned = jnp.where(node == i, float(stiff[i, (i - step) % 8]), turned)
        along_x_ref[step] = turned

    def flag(condition):
        return jnp.where(condition, 1.0, 0.0)

    x_low = flag((node == 0) & (x_index > 0))
    x_high = flag((node == 7) & (x_index < EX - 1))
    y_low = flag(y_index > 0)
    y_high = flag(y_index < EY - 1)

    def plane_sum(tile):
        below = pltpu.roll(pltpu.roll(tile, 1, 1), 1, 2)
        above = pltpu.roll(pltpu.roll(tile, 7, 1), elems - 1, 2)
        tile = tile + below * x_low + above * x_high
        low = tile[0] + y_low * pltpu.roll(tile[7], EX, 1)
        high = tile[7] + y_high * pltpu.roll(tile[0], elems - EX, 1)
        return jnp.concatenate([low[None], tile[1:7], high[None]], 0)

    def weights(layer):
        return plane_ref[...] * float(quad[layer])

    loads[4].wait()
    loads[5].wait()
    wall_rows = []
    for side in range(2):
        wall_row = jnp.zeros((1, elems), jnp.float32)
        for x in range(EX):
            bit = wall_ref[side : side + 1, x : x + 1].astype(jnp.float32)
            wall_row = jnp.where(x_index[0:1] == x, bit, wall_row)
        wall_rows.append(wall_row)
    g_x, g_y, g_z, g_m = [geometry_ref[d : d + 1, :] for d in range(4)]

    diag_plane = jnp.zeros((8, 8, elems), jnp.float32) + g_m
    diag_plane = diag_plane + g_x * along_x_ref[0]
    diag_plane = diag_plane + jnp.concatenate(
        [(g_y * float(stiff[j, j]) + jnp.zeros((8, elems), jnp.float32))[None] for j in range(8)], 0
    )
    for layer in ORDER:
        image[layer] = plane_sum(
            weights(layer) * (diag_plane + g_z * float(stiff[layer, layer]))
        )
    wall_low = flag(y_index == 0) * wall_rows[0]
    wall_high = flag(y_index == EY - 1) * wall_rows[1]
    nothing = jnp.zeros((6, 8, elems), jnp.float32)
    wall_plane = plane_sum(jnp.concatenate([wall_low[None], nothing, wall_high[None]], 0))
    faces[0, 0] = image[0]
    faces[0, 1] = image[7]
    faces[1, 0] = wall_plane
    faces[1, 1] = wall_plane
    send_faces(0)
    send_faces(1)

    loads[3].wait()
    donors = donor_ref[...].reshape(fields * 512, elems)
    coarse = donors.astype(jnp.bfloat16)
    split[:, :elems] = coarse
    split[:, elems:] = (donors - coarse.astype(jnp.float32)).astype(jnp.bfloat16)

    code = lax.broadcasted_iota(jnp.int32, (elems, CHUNK), 0)
    code = code.astype(jnp.float32)
    basis = lax.broadcasted_iota(jnp.int32, (8, CHUNK), 0)
    norms = [
        float(1.0 / np.prod([points[a] - points[b] for b in range(8) if b != a])) for a in range(8)
    ]
    scale = jnp.zeros((8, CHUNK), jnp.float32)
    for a in range(8):
        scale = jnp.where(basis == a, norms[a], scale)

    def lagrange(position):
        value = scale
        for b in range(8):
            value = value * jnp.where(basis == b, 1.0, position - float(points[b]))
        return value

    def serve(turn, carry):
        shift = ((turn + 1) // 2) * (2 * (turn % 2) - 1)

        @pl.when(inside(slab - shift))
        def _():
            ask(shift).wait_recv()

            group = CHUNK // lanes
            for chunk in range(room // group):
                block = [
                    jnp.concatenate(
                        [
                            asked[shift + REACH, c, chunk * group + t : chunk * group + t + 1, :]
                            for t in range(group)
                        ],
                        1,
                    )
                    for c in range(4)
                ]
                chosen = jnp.where(block[3] == code, 1.0, 0.0).astype(jnp.bfloat16)
                chosen = jnp.concatenate([chosen, chosen], 0)
                w_x, w_y, w_z = [lagrange(block[d]) for d in range(3)]
                found = jnp.dot(split[...], chosen, preferred_element_type=jnp.float32)
                for field in range(fields):
                    cube = found[field * 512 : (field + 1) * 512].reshape(8, 64, CHUNK)
                    total = cube[0] * w_z[0:1, :]
                    for k in range(1, 8):
                        total = total + cube[k] * w_z[k : k + 1, :]
                    total = total.reshape(8, 8, CHUNK)
                    line = total[0] * w_y[0:1, :]
                    for j in range(1, 8):
                        line = line + total[j] * w_y[j : j + 1, :]
                    value = jnp.sum(line * w_x, axis=0, keepdims=True)
                    for t in range(group):
                        row = chunk * group + t
                        answer[shift + REACH, field, row : row + 1, :] = value[
                            :, t * lanes : (t + 1) * lanes
                        ]

            reply(shift).start()

        return carry

    lax.fori_loop(0, slots, serve, 0)

    z_low = jnp.where(slab > 0, 2.0, 1.0)
    z_high = jnp.where(slab < n - 1, 2.0, 1.0)
    x_count = 1.0 + x_low + x_high
    y_count_low = 1.0 + y_low
    y_count_high = 1.0 + y_high
    plane_count = jnp.concatenate(
        [(x_count * y_count_low)[None]]
        + [x_count[None]] * 6
        + [(x_count * y_count_high)[None]],
        0,
    )
    mark = flag((node == 0) & (x_index == 0)) + flag((node == 7) & (x_index == EX - 1))
    wait_faces(0)
    wait_faces(1)
    image[0] = image[0] + halo[0, 0]
    image[7] = image[7] + halo[0, 1]
    for layer in range(8):
        count = plane_count
        walls = wall_plane
        if layer == 0:
            count = count * z_low
            walls = walls + halo[1, 0]
        if layer == 7:
            count = count * z_high
            walls = walls + halo[1, 1]
        open_part = 1.0 - jnp.minimum(mark * count + walls, 1.0)
        sharing[layer] = 1.0 / count
        free[layer] = open_part
        inverse[layer] = open_part / image[layer]

    for shift in range(-REACH, REACH + 1):

        @pl.when(jnp.logical_not(inside(slab + shift)))
        def _():
            answered[shift + REACH] = jnp.zeros(answered.shape[1:], jnp.float32)

        @pl.when(inside(slab + shift))
        def _():
            reply(shift).wait_recv()

    def gather_field(field):
        result = jnp.zeros((height, lanes), jnp.float32)
        for slot in range(slots):
            packed = answered[slot, field]
            tile = jnp.concatenate([packed, pltpu.roll(packed, half, 1)], 0)
            for step in reversed(range(steps)):
                tile = jnp.where(moves[step, slot] != 0, push(tile, step), tile)
            result = jnp.where(members[slot], tile, result)
        return result

    values = [gather_field(field) for field in range(fields)]
    for row in range(height):
        interface_ref[:, row * lanes : (row + 1) * lanes] = jnp.concatenate(
            [value[row : row + 1] for value in values], 0
        )

    groups = lanes // 64
    rows = jnp.concatenate([values[0][:, t * 64 : (t + 1) * 64] for t in range(groups)], 0)
    per_side = height // 2
    row = lax.broadcasted_iota(jnp.int32, (groups * height, elems), 0)
    spot = lax.broadcasted_iota(jnp.int32, (groups * height, elems), 1)
    piece = row % height
    target = (groups * (piece % per_side) + row // height) * EX + (EX - 1) * (piece // per_side)
    placed = lax.dot_general(
        rows,
        flag(spot == target),
        (((0,), (0,)), ((), ())),
        precision=lax.Precision.HIGHEST,
        preferred_element_type=jnp.float32,
    ).reshape(8, 8, elems)
    for layer in ORDER:
        spread = jnp.concatenate(
            [(jnp.broadcast_to(placed[layer, j : j + 1, :], (8, elems)) * mark)[None] for j in range(8)],
            0,
        )
        boundary[layer] = plane_sum(spread)
        if layer == 7:
            faces[2, 0] = boundary[0]
            faces[2, 1] = boundary[7]
            send_faces(2)
    wait_faces(2)
    boundary[0] = boundary[0] + halo[2, 0]
    boundary[7] = boundary[7] + halo[2, 1]
    for layer in range(8):
        boundary[layer] = boundary[layer] * sharing[layer]

    def local_tile(source, layer):
        tile = source[layer]
        along_z = source[0] * float(stiff[layer, 0])
        for k in range(1, 8):
            along_z = along_z + source[k] * float(stiff[layer, k])
        along_y = along_y_ref[0] * tile[0:1]
        for j in range(1, 8):
            along_y = along_y + along_y_ref[j] * tile[j : j + 1]
        along_x = along_x_ref[0] * tile
        for step in range(1, 8):
            along_x = along_x + along_x_ref[step] * pltpu.roll(tile, step, 1)
        total = g_x * along_x + g_y * along_y + g_z * along_z + g_m * tile
        return weights(layer) * total

    loads[6].wait()
    for layer in ORDER:
        loaded = weights(layer) * g_m * forcing_ref[layer] - local_tile(boundary, layer)
        residual_ref[layer] = plane_sum(loaded)
        if layer == 7:
            faces[3, 0] = residual_ref[0]
            faces[3, 1] = residual_ref[7]
            send_faces(3)
    wait_faces(3)
    residual_ref[0] = residual_ref[0] + halo[3, 0]
    residual_ref[7] = residual_ref[7] + halo[3, 1]
    for layer in range(8):
        residual_ref[layer] = residual_ref[layer] * free[layer]
        velocity_ref[layer] = boundary[layer]
        direction[layer] = jnp.zeros((8, 8, elems), jnp.float32)
        direction_image[layer] = jnp.zeros((8, 8, elems), jnp.float32)

    def iterate(turn, carry):
        norm, length = carry
        phase = turn + 4
        norm_part = jnp.zeros((8, 8, elems), jnp.float32)
        for layer in range(8):
            state[layer] = inverse[layer] * residual_ref[layer]
            norm_part = norm_part + state[layer] * residual_ref[layer] * sharing[layer]
        curve_part = jnp.zeros((8, 8, elems), jnp.float32)
        for layer in ORDER:
            tile = local_tile(state, layer)
            curve_part = curve_part + tile * state[layer]
            image[layer] = plane_sum(tile)
            if layer == 7:
                faces[phase, 0] = image[0]
                faces[phase, 1] = image[7]
                send_faces(phase)
        dots[turn, 0:1, :] = jnp.sum(jnp.sum(norm_part, axis=0), axis=0, keepdims=True)
        dots[turn, 1:2, :] = jnp.sum(jnp.sum(curve_part, axis=0), axis=0, keepdims=True)
        for step in range(1, n):
            dot_copy(turn, step).start()
        all_dots[turn, slab] = dots[turn]
        wait_faces(phase)
        image[0] = image[0] + halo[phase, 0]
        image[7] = image[7] + halo[phase, 1]
        for step in range(1, n):
            dot_copy(turn, step).wait_recv()
        sums = jnp.sum(jnp.sum(all_dots[turn], axis=0), axis=1, keepdims=True)
        norm_next, curvature = sums[0:1, :], sums[1:2, :]
        ratio = jnp.where(turn == 0, 0.0, norm_next / norm)
        length = norm_next / (curvature - ratio * norm_next / length)
        for layer in range(8):
            toward = state[layer] + ratio * direction[layer]
            toward_image = free[layer] * image[layer] + ratio * direction_image[layer]
            direction[layer] = toward
            direction_image[layer] = toward_image
            velocity_ref[layer] = velocity_ref[layer] + length * toward
            residual_ref[layer] = residual_ref[layer] - length * toward_image
        for step in range(1, n):
            dot_copy(turn, step).wait_send()
        return norm_next, length

    one = jnp.ones((1, 1), jnp.float32)
    lax.fori_loop(0, ITERS, iterate, (one, one))

    for shift in range(-REACH, REACH + 1):

        @pl.when(inside(slab + shift))
        def _():
            ask(shift).wait_send()

        @pl.when(inside(slab - shift))
        def _():
            reply(shift).wait_send()


def flush(*refs):
    count = (len(refs) - 1) // 2
    sem = refs[-1]
    copies = [
        pltpu.make_async_copy(refs[at], refs[count + at], sem.at[at]) for at in range(count)
    ]
    for copy in copies:
        copy.start()
    for copy in copies:
        copy.wait()


def body(n, donor_fields, interp_weights, donor_owner, donor_element, geometry, wall_flag, forcing):
    fields = donor_fields.shape[0]
    elems = geometry.shape[1]
    receptors = donor_element.shape[0]
    slots = 2 * REACH + 1
    lanes = 128
    count = receptors // lanes
    cube = (8, 8, 8, elems)
    phases = 4 + ITERS
    room = count // 2
    vmem = pl.BlockSpec(memory_space=pltpu.VMEM)
    hbm = pl.BlockSpec(memory_space=pltpu.HBM)
    shapes = (
        jax.ShapeDtypeStruct(cube, jnp.float32),
        jax.ShapeDtypeStruct(cube, jnp.float32),
        jax.ShapeDtypeStruct((fields, receptors), jnp.float32),
    )
    outputs = pl.pallas_call(
        functools.partial(kernel, n),
        out_shape=shapes,
        in_specs=[hbm] * 7,
        out_specs=(vmem, vmem, vmem),
        scratch_shapes=[
            pltpu.VMEM((fields, 512, elems), jnp.float32),
            pltpu.VMEM(cube, jnp.float32),
            pltpu.VMEM(interp_weights.shape, jnp.float32),
            pltpu.VMEM((count, lanes), jnp.int32),
            pltpu.VMEM((count, lanes), jnp.int32),
            pltpu.VMEM(geometry.shape, jnp.float32),
            pltpu.VMEM(wall_flag.shape, jnp.int32),
            pltpu.VMEM((3, count, lanes), jnp.float32),
            pltpu.VMEM((slots, 4, room, lanes), jnp.float32),
            pltpu.VMEM((receptors.bit_length() - 1, slots, count, lanes), jnp.int32),
            pltpu.VMEM(cube, jnp.float32),
            pltpu.VMEM((8, 8, elems), jnp.float32),
            pltpu.VMEM((8, 8, elems), jnp.float32),
            pltpu.SemaphoreType.DMA((7,)),
            pltpu.VMEM((fields * 512, 2 * elems), jnp.bfloat16),
            pltpu.VMEM((slots, 4, room, lanes), jnp.float32),
            pltpu.VMEM((slots, fields, room, lanes), jnp.float32),
            pltpu.VMEM((slots, fields, room, lanes), jnp.float32),
            pltpu.VMEM((phases, 2, 8, 8, elems), jnp.float32),
            pltpu.VMEM((phases, 2, 8, 8, elems), jnp.float32),
            pltpu.VMEM((ITERS, 2, 128), jnp.float32),
            pltpu.VMEM((ITERS, n, 2, 128), jnp.float32),
        ]
        + [pltpu.VMEM(cube, jnp.float32)] * 8
        + [pltpu.SemaphoreType.DMA((slots,))] * 4
        + [pltpu.SemaphoreType.DMA((phases, 2))] * 2
        + [pltpu.SemaphoreType.DMA((ITERS, n))] * 2,
        compiler_params=pltpu.CompilerParams(
            collective_id=0, has_side_effects=True, vmem_limit_bytes=67043328
        ),
    )(
        donor_fields,
        interp_weights,
        donor_owner.reshape(count, lanes),
        donor_element.reshape(count, lanes),
        geometry,
        wall_flag,
        forcing.reshape(cube),
    )
    velocity, residual, interface = pl.pallas_call(
        flush,
        out_shape=shapes,
        in_specs=[vmem] * 3,
        out_specs=(hbm,) * 3,
        scratch_shapes=[pltpu.SemaphoreType.DMA((3,))],
    )(*outputs)
    return (velocity.reshape(512, elems), residual.reshape(512, elems), interface)


def solution(mesh):
    in_specs = (
        P(None, None, ("mesh", "dom")),
        P(None, None, ("mesh", "dom")),
        P(("mesh", "dom"), None),
        P(("mesh", "dom")),
        P(None, ("mesh", "dom")),
        P(None, ("mesh", "dom")),
        P(None, ("mesh", "dom")),
    )
    out_specs = (P(None, ("mesh", "dom")), P(None, ("mesh", "dom")), P(None, ("mesh", "dom")))
    return jax.shard_map(
        functools.partial(body, mesh.shape["dom"]),
        mesh=mesh,
        in_specs=in_specs,
        out_specs=out_specs,
        check_vma=False,
    )
```

```python
import functools

import jax
import jax.numpy as jnp
import numpy as np
from jax import lax
from jax.experimental import pallas as pl
from jax.experimental.pallas import tpu as pltpu
from jax.sharding import PartitionSpec as P

EX = 8
EY = 16
ITERS = 3
REACH = 2
CHUNK = 256
ORDER = (0, 7, 1, 2, 3, 4, 5, 6)
SHIFTS = (1.5, 0.5)
MESH = pl.DeviceIdType.MESH


def legendre_pair(values, degree):
    previous = values * 0.0 + 1.0
    current = values * 1.0
    for poly_order in range(2, degree + 1):
        previous, current = (
            current,
            ((2 * poly_order - 1) * values * current - (poly_order - 1) * previous) / poly_order,
        )
    return (current, previous)


def gll_tables():
    degree = 7
    points_count = degree + 1
    abscissae = np.cos(np.pi * np.arange(points_count) / degree)
    for newton_turn in range(80):
        top_poly, lower_poly = legendre_pair(abscissae, degree)
        abscissae = abscissae - (abscissae * top_poly - lower_poly) / (points_count * top_poly)
    abscissae = np.sort(abscissae)
    top_poly, lower_poly = legendre_pair(abscissae, degree)
    quad_weights = 2.0 / (degree * points_count * top_poly * top_poly)
    identity_mat = np.eye(points_count)
    spacing = abscissae[:, None] - abscissae[None, :] + identity_mat
    derivative = top_poly[:, None] / (top_poly[None, :] * spacing) * (1.0 - identity_mat)
    derivative[0, 0] = -degree * points_count / 4.0
    derivative[degree, degree] = degree * points_count / 4.0
    return (abscissae, derivative, quad_weights)


def solve(found):
    matrix = [
        [found[(min(a, b), max(a, b))] for b in range(ITERS)] for a in range(ITERS)
    ]
    right = [found[a] for a in range(ITERS)]
    for a in range(ITERS):
        for b in range(a + 1, ITERS):
            factor = matrix[b][a] / matrix[a][a]
            for c in range(a + 1, ITERS):
                matrix[b][c] = matrix[b][c] - factor * matrix[a][c]
            right[b] = right[b] - factor * right[a]
    answer = [None] * ITERS
    for a in reversed(range(ITERS)):
        total = right[a]
        for b in range(a + 1, ITERS):
            total = total - matrix[a][b] * answer[b]
        answer[a] = total / matrix[a][a]
    return answer


def kernel(
    n,
    donor_hbm,
    weights_hbm,
    owner_hbm,
    element_hbm,
    geometry_hbm,
    wall_hbm,
    forcing_hbm,
    velocity_hbm,
    residual_hbm,
    interface_hbm,
    velocity,
    residual,
    interface_ref,
    donor_ref,
    forcing_ref,
    weights_ref,
    owner_ref,
    element_ref,
    geometry_ref,
    wall_ref,
    position_ref,
    request_ref,
    ranks,
    along_y_ref,
    along_x_ref,
    plane_ref,
    load_sem,
    split,
    asked,
    answer,
    answered,
    faces,
    halo,
    dots,
    all_dots,
    vectors,
    images,
    partial,
    rho,
    rim,
    rim_halo,
    geometry_halo,
    inverse,
    free,
    sharing,
    boundary,
    ask_send,
    ask_recv,
    reply_send,
    reply_recv,
    face_send,
    face_recv,
    dot_send,
    dot_recv,
    rim_send,
    rim_recv,
    geometry_send,
    geometry_recv,
    store_sem,
):
    points, derivative, quad = gll_tables()
    stiff = (derivative.T * quad) @ derivative / quad[:, None]
    fields = donor_ref.shape[0]
    elems = donor_ref.shape[2]
    height = owner_ref.shape[0]
    lanes = owner_ref.shape[1]
    receptors = height * lanes
    room = request_ref.shape[2]
    slots = 2 * REACH + 1
    mesh_id = lax.axis_index("mesh")
    slab = lax.axis_index("dom")
    other = 1 - mesh_id

    pairs = [
        (weights_hbm, weights_ref),
        (owner_hbm, owner_ref),
        (element_hbm, element_ref),
        (donor_hbm, donor_ref),
        (geometry_hbm, geometry_ref),
        (wall_hbm, wall_ref),
        (forcing_hbm, forcing_ref),
    ]
    loads = [
        pltpu.make_async_copy(source, target, load_sem.at[at])
        for at, (source, target) in enumerate(pairs)
    ]
    for load in loads:
        load.start()

    def inside(index):
        return jnp.logical_and(index >= 0, index < n)

    barrier = pltpu.get_barrier_semaphore()
    greeted = n - 1
    for step in range(1, n):
        pl.semaphore_signal(
            barrier, inc=1, device_id=(mesh_id, lax.rem(slab + step, n)), device_id_type=MESH
        )
    for shift in range(-REACH, REACH + 1):
        greeted = greeted + jnp.where(inside(slab + shift), 1, 0)

        @pl.when(inside(slab + shift))
        def _():
            pl.semaphore_signal(
                barrier, inc=1, device_id=(other, slab + shift), device_id_type=MESH
            )

    with jax.named_scope('w_loads'):
        for load in loads[:3]:
            load.wait()
    depth = lax.broadcasted_iota(jnp.int32, (8, lanes), 0)
    ladder = jnp.zeros((8, lanes), jnp.float32)
    for a in range(8):
        ladder = jnp.where(depth == a, float(points[a]), ladder)
    for d in range(3):
        for row in range(height):
            part = weights_ref[d, :, row * lanes : (row + 1) * lanes] * ladder
            position_ref[d, row : row + 1, :] = jnp.sum(part, axis=0, keepdims=True)
    owner = owner_ref[...]
    element_code = element_ref[...] * receptors
    members = [owner == slab + shift for shift in range(-REACH, REACH + 1)]
    tall = slots * height
    marks = jnp.concatenate([jnp.where(m, 1.0, 0.0) for m in members], 0).astype(jnp.bfloat16)
    before = lax.broadcasted_iota(jnp.int32, (lanes, lanes), 0)
    after = lax.broadcasted_iota(jnp.int32, (lanes, lanes), 1)
    upper = jnp.where(before < after, 1.0, 0.0).astype(jnp.bfloat16)
    left = jnp.dot(marks, upper, preferred_element_type=jnp.float32).astype(jnp.bfloat16)
    above = lax.broadcasted_iota(jnp.int32, (tall, tall), 0)
    below = lax.broadcasted_iota(jnp.int32, (tall, tall), 1)
    same = above // height == below // height
    block = jnp.where(same, 1.0, 0.0).astype(jnp.bfloat16)
    lower = jnp.where(same & (below < above), 1.0, 0.0).astype(jnp.bfloat16)
    rank = jnp.dot(block, left, preferred_element_type=jnp.float32)
    rank = rank + jnp.dot(lower, marks, preferred_element_type=jnp.float32)
    rank = rank.astype(jnp.int32)
    ranks[...] = rank
    row_index = lax.broadcasted_iota(jnp.int32, (height, lanes), 0)
    place = lax.broadcasted_iota(jnp.int32, (height, lanes), 1) * height + row_index
    row_bits = height.bit_length() - 1
    steps = receptors.bit_length() - 1

    def pull(tile, step):
        if step >= row_bits:
            return pltpu.roll(tile, lanes - (1 << (step - row_bits)), 1)
        jump = 1 << step
        near = pltpu.roll(tile, height - jump, 0)
        far = pltpu.roll(near, lanes - 1, 1)
        return jnp.where(row_index < height - jump, near, far)

    words = []
    comps = []
    start = [position_ref[d] for d in range(3)]
    for slot in range(slots):
        shift = place - rank[slot * height : (slot + 1) * height]
        words.append(jnp.where(members[slot], element_code + shift, 0))
        comps.append(list(start))
    for step in range(steps):
        for slot in range(slots):
            word = words[slot]
            moving = word & (1 << step)
            came = pull(word, step)
            take = (came & (1 << step)) != 0
            words[slot] = jnp.where(take, came - (1 << step), jnp.where(moving != 0, 0, word))
            comps[slot] = [jnp.where(take, pull(c, step), c) for c in comps[slot]]
    half = lanes // 2
    left_half = lax.broadcasted_iota(jnp.int32, (room, lanes), 1) < half
    for slot in range(slots):
        columns = comps[slot] + [(words[slot] >> steps).astype(jnp.float32)]
        for at, column in enumerate(columns):
            request_ref[slot, at] = jnp.where(
                left_half, column[:room], pltpu.roll(column[room:], half, 1)
            )

    with jax.named_scope('w_barrier'):
        pl.semaphore_wait(barrier, greeted)

    def ask(shift):
        return pltpu.make_async_remote_copy(
            src_ref=request_ref.at[shift + REACH],
            dst_ref=asked.at[shift + REACH],
            send_sem=ask_send.at[shift + REACH],
            recv_sem=ask_recv.at[shift + REACH],
            device_id=(other, lax.rem(slab + shift + n, n)),
            device_id_type=MESH,
        )

    def reply(shift):
        return pltpu.make_async_remote_copy(
            src_ref=answer.at[shift + REACH],
            dst_ref=answered.at[shift + REACH],
            send_sem=reply_send.at[shift + REACH],
            recv_sem=reply_recv.at[shift + REACH],
            device_id=(other, lax.rem(slab - shift + n, n)),
            device_id_type=MESH,
        )

    def face_copy(phase, up):
        step = 1 if up else n - 1
        return pltpu.make_async_remote_copy(
            src_ref=faces.at[phase, 1 if up else 0],
            dst_ref=halo.at[phase, 0 if up else 1],
            send_sem=face_send.at[phase, 1 if up else 0],
            recv_sem=face_recv.at[phase, 0 if up else 1],
            device_id=(mesh_id, lax.rem(slab + step, n)),
            device_id_type=MESH,
        )

    def send_faces(phase):
        @pl.when(slab < n - 1)
        def _():
            face_copy(phase, True).start()

        @pl.when(slab > 0)
        def _():
            face_copy(phase, False).start()

    def wait_faces(phase):
        @pl.when(slab > 0)
        def _():
            face_copy(phase, True).wait_recv()

        @pl.when(slab < n - 1)
        def _():
            face_copy(phase, False).wait_recv()

        @pl.when(slab < n - 1)
        def _():
            face_copy(phase, True).wait_send()

        @pl.when(slab > 0)
        def _():
            face_copy(phase, False).wait_send()

    def dot_copy(step):
        return pltpu.make_async_remote_copy(
            src_ref=dots,
            dst_ref=all_dots.at[slab],
            send_sem=dot_send.at[step],
            recv_sem=dot_recv.at[step],
            device_id=(mesh_id, lax.rem(slab + step, n)),
            device_id_type=MESH,
        )

    rim_jumps = (1, -1, 2, -2)
    rim_sends = [inside(slab + jump) for jump in rim_jumps]
    rim_comes = [inside(slab - jump) for jump in rim_jumps]
    near = (slab > 0, slab < n - 1)

    def rim_copy(at):
        return pltpu.make_async_remote_copy(
            src_ref=rim.at[1 - at % 2],
            dst_ref=rim_halo.at[at],
            send_sem=rim_send.at[at],
            recv_sem=rim_recv.at[at],
            device_id=(mesh_id, lax.rem(slab + rim_jumps[at] + n, n)),
            device_id_type=MESH,
        )

    def geometry_copy(up):
        side = 0 if up else 1
        return pltpu.make_async_remote_copy(
            src_ref=geometry_ref,
            dst_ref=geometry_halo.at[side],
            send_sem=geometry_send.at[side],
            recv_sem=geometry_recv.at[side],
            device_id=(mesh_id, lax.rem(slab + (1 if up else n - 1), n)),
            device_id_type=MESH,
        )

    stores = [
        pltpu.make_async_copy(source, target, store_sem.at[at])
        for at, (source, target) in enumerate(
            ((interface_ref, interface_hbm), (velocity, velocity_hbm), (rho, residual_hbm))
        )
    ]

    for distance in range(REACH + 1):
        for shift in sorted({distance, -distance}):

            @pl.when(inside(slab + shift))
            def _():
                ask(shift).start()

    phases = halo.shape[0]
    blank = jnp.zeros(halo.shape[2:], jnp.float32)

    for at in range(4):

        @pl.when(jnp.logical_not(rim_comes[at]))
        def _():
            rim_halo[at] = jnp.zeros(rim_halo.shape[1:], jnp.float32)

    for side in range(2):

        @pl.when(jnp.logical_not(near[side]))
        def _():
            geometry_halo[side] = jnp.zeros(geometry_halo.shape[1:], jnp.float32)

    @pl.when(slab == 0)
    def _():
        for phase in range(phases):
            halo[phase, 0] = blank

    @pl.when(slab == n - 1)
    def _():
        for phase in range(phases):
            halo[phase, 1] = blank

    node = lax.broadcasted_iota(jnp.int32, (8, elems), 0)
    element = lax.broadcasted_iota(jnp.int32, (8, elems), 1)
    x_index = element % EX
    y_index = element // EX % EY

    across = jnp.zeros((8, elems), jnp.float32)
    for a in range(8):
        across = jnp.where(node == a, float(quad[a]), across)
    for j in range(8):
        plane_ref[j] = across * float(quad[j])
        for m in range(8):
            along_y_ref[m, j] = jnp.full((8, elems), float(stiff[j, m]), jnp.float32)
    for step in range(8):
        turned = jnp.zeros((8, elems), jnp.float32)
        for i in range(8):
            turned = jnp.where(node == i, float(stiff[i, (i - step) % 8]), turned)
        along_x_ref[step] = turned

    def flag(condition):
        return jnp.where(condition, 1.0, 0.0)

    x_low = flag((node == 0) & (x_index > 0))
    x_high = flag((node == 7) & (x_index < EX - 1))
    y_low = flag(y_index > 0)
    y_high = flag(y_index < EY - 1)

    def plane_sum(tile):
        below = pltpu.roll(pltpu.roll(tile, 1, 1), 1, 2)
        above = pltpu.roll(pltpu.roll(tile, 7, 1), elems - 1, 2)
        tile = tile + below * x_low + above * x_high
        low = tile[0] + y_low * pltpu.roll(tile[7], EX, 1)
        high = tile[7] + y_high * pltpu.roll(tile[0], elems - EX, 1)
        return jnp.concatenate([low[None], tile[1:7], high[None]], 0)

    def weights(layer):
        return plane_ref[...] * float(quad[layer])

    loads[4].wait()
    loads[5].wait()

    @pl.when(near[1])
    def _():
        geometry_copy(True).start()

    @pl.when(near[0])
    def _():
        geometry_copy(False).start()

    wall_rows = []
    for side in range(2):
        wall_row = jnp.zeros((1, elems), jnp.float32)
        for x in range(EX):
            bit = wall_ref[side : side + 1, x : x + 1].astype(jnp.float32)
            wall_row = jnp.where(x_index[0:1] == x, bit, wall_row)
        wall_rows.append(wall_row)
    g_x, g_y, g_z, g_m = [geometry_ref[d : d + 1, :] for d in range(4)]

    diag_plane = jnp.zeros((8, 8, elems), jnp.float32) + g_m
    diag_plane = diag_plane + g_x * along_x_ref[0]
    diag_plane = diag_plane + jnp.concatenate(
        [(g_y * float(stiff[j, j]) + jnp.zeros((8, elems), jnp.float32))[None] for j in range(8)], 0
    )
    for layer in ORDER:
        images[0, layer] = plane_sum(
            weights(layer) * (diag_plane + g_z * float(stiff[layer, layer]))
        )
    wall_low = flag(y_index == 0) * wall_rows[0]
    wall_high = flag(y_index == EY - 1) * wall_rows[1]
    nothing = jnp.zeros((6, 8, elems), jnp.float32)
    wall_plane = plane_sum(jnp.concatenate([wall_low[None], nothing, wall_high[None]], 0))
    faces[0, 0] = images[0, 0]
    faces[0, 1] = images[0, 7]
    faces[1, 0] = wall_plane
    faces[1, 1] = wall_plane
    send_faces(0)
    send_faces(1)

    with jax.named_scope('w_donor'):
        loads[3].wait()
    donors = donor_ref[...].reshape(fields * 512, elems)
    coarse = donors.astype(jnp.bfloat16)
    split[:, :elems] = coarse
    split[:, elems:] = (donors - coarse.astype(jnp.float32)).astype(jnp.bfloat16)

    code = lax.broadcasted_iota(jnp.int32, (elems, CHUNK), 0)
    code = code.astype(jnp.float32)
    basis = lax.broadcasted_iota(jnp.int32, (8, CHUNK), 0)
    norms = [
        float(1.0 / np.prod([points[a] - points[b] for b in range(8) if b != a])) for a in range(8)
    ]
    scale = jnp.zeros((8, CHUNK), jnp.float32)
    for a in range(8):
        scale = jnp.where(basis == a, norms[a], scale)

    def lagrange(position):
        value = scale
        for b in range(8):
            value = value * jnp.where(basis == b, 1.0, position - float(points[b]))
        return value

    def serve(turn, carry):
        shift = ((turn + 1) // 2) * (2 * (turn % 2) - 1)

        @pl.when(inside(slab - shift))
        def _():
            with jax.named_scope('w_ask'):
                ask(shift).wait_recv()

            group = CHUNK // lanes
            for chunk in range(room // group):
                block = [
                    jnp.concatenate(
                        [
                            asked[shift + REACH, c, chunk * group + t : chunk * group + t + 1, :]
                            for t in range(group)
                        ],
                        1,
                    )
                    for c in range(4)
                ]
                chosen = jnp.where(block[3] == code, 1.0, 0.0).astype(jnp.bfloat16)
                chosen = jnp.concatenate([chosen, chosen], 0)
                w_x, w_y, w_z = [lagrange(block[d]) for d in range(3)]
                found = jnp.dot(split[...], chosen, preferred_element_type=jnp.float32)
                for field in range(fields):
                    cube = found[field * 512 : (field + 1) * 512].reshape(8, 64, CHUNK)
                    total = cube[0] * w_z[0:1, :]
                    for k in range(1, 8):
                        total = total + cube[k] * w_z[k : k + 1, :]
                    total = total.reshape(8, 8, CHUNK)
                    line = total[0] * w_y[0:1, :]
                    for j in range(1, 8):
                        line = line + total[j] * w_y[j : j + 1, :]
                    value = jnp.sum(line * w_x, axis=0, keepdims=True)
                    for t in range(group):
                        row = chunk * group + t
                        answer[shift + REACH, field, row : row + 1, :] = value[
                            :, t * lanes : (t + 1) * lanes
                        ]

            with jax.named_scope('reply'):
                reply(shift).start()

        return carry

    lax.fori_loop(0, slots, serve, 0)

    z_low = jnp.where(slab > 0, 2.0, 1.0)
    z_high = jnp.where(slab < n - 1, 2.0, 1.0)
    x_count = 1.0 + x_low + x_high
    y_count_low = 1.0 + y_low
    y_count_high = 1.0 + y_high
    plane_count = jnp.concatenate(
        [(x_count * y_count_low)[None]]
        + [x_count[None]] * 6
        + [(x_count * y_count_high)[None]],
        0,
    )
    mark = flag((node == 0) & (x_index == 0)) + flag((node == 7) & (x_index == EX - 1))
    with jax.named_scope('w_f01'):
        wait_faces(0)
        wait_faces(1)
    images[0, 0] = images[0, 0] + halo[0, 0]
    images[0, 7] = images[0, 7] + halo[0, 1]
    for layer in range(8):
        count = plane_count
        walls = wall_plane
        if layer == 0:
            count = count * z_low
            walls = walls + halo[1, 0]
        if layer == 7:
            count = count * z_high
            walls = walls + halo[1, 1]
        open_part = 1.0 - jnp.minimum(mark * count + walls, 1.0)
        sharing[layer] = 1.0 / count
        free[layer] = open_part
        inverse[layer] = open_part / images[0, layer]

    for shift in range(-REACH, REACH + 1):

        @pl.when(jnp.logical_not(inside(slab + shift)))
        def _():
            answered[shift + REACH] = jnp.zeros(answered.shape[1:], jnp.float32)

        @pl.when(inside(slab + shift))
        def _():
            with jax.named_scope('w_reply'):
                reply(shift).wait_recv()

    room_index = lax.broadcasted_iota(jnp.int32, (room, lanes), 0)
    plans = []
    for slot in range(slots):
        table = ranks[slot * height : (slot + 1) * height, :]
        base = jnp.broadcast_to(table[0:1], (room, lanes))
        first = jnp.minimum(base >> row_bits, half - 1)
        second = jnp.minimum(first + 1, half - 1)
        offset = base & (height - 1)
        spots = table & (height - 1)
        plans.append((first, second, offset, spots))

    def along_lanes(tile, index):
        return jnp.take_along_axis(tile, index, axis=1, mode="promise_in_bounds")

    def along_rows(tile, index):
        return jnp.take_along_axis(tile, index, axis=0, mode="promise_in_bounds")

    def gather_field(field):
        result = [jnp.zeros((room, lanes), jnp.float32)] * 2
        for slot in range(slots):
            packed = answered[slot, field]
            first, second, offset, spots = plans[slot]
            windows = [
                jnp.where(
                    room_index + part * room >= offset,
                    along_lanes(packed, first + part * half),
                    along_lanes(packed, second + part * half),
                )
                for part in range(2)
            ]
            for part in range(2):
                spot = spots[part * room : (part + 1) * room]
                member = members[slot][part * room : (part + 1) * room]
                low, high = [along_rows(window, spot & (room - 1)) for window in windows]
                tile = jnp.where(spot < room, low, high)
                result[part] = jnp.where(member, tile, result[part])
        return jnp.concatenate(result, 0)

    values = [gather_field(0)]
    groups = lanes // 64
    rows = jnp.concatenate([values[0][:, t * 64 : (t + 1) * 64] for t in range(groups)], 0)
    per_side = height // 2
    row = lax.broadcasted_iota(jnp.int32, (groups * height, elems), 0)
    spot = lax.broadcasted_iota(jnp.int32, (groups * height, elems), 1)
    piece = row % height
    target = (groups * (piece % per_side) + row // height) * EX + (EX - 1) * (piece // per_side)
    placed = lax.dot_general(
        rows,
        flag(spot == target),
        (((0,), (0,)), ((), ())),
        precision=lax.Precision.HIGHEST,
        preferred_element_type=jnp.float32,
    ).reshape(8, 8, elems)
    rim[0] = placed[0]
    rim[1] = placed[7]
    for at in range(4):

        @pl.when(rim_sends[at])
        def _():
            rim_copy(at).start()

    def spread_out(column):
        return plane_sum(
            jnp.concatenate(
                [
                    (jnp.broadcast_to(column[j : j + 1, :], (8, elems)) * mark)[None]
                    for j in range(8)
                ],
                0,
            )
        )

    def in_plane(tile, along):
        along_y = along_y_ref[0] * tile[0:1]
        for j in range(1, 8):
            along_y = along_y + along_y_ref[j] * tile[j : j + 1]
        along_x = along_x_ref[0] * tile
        for step in range(1, 8):
            along_x = along_x + along_x_ref[step] * pltpu.roll(tile, step, 1)
        return along[0] * along_x + along[1] * along_y

    def inner_z(read, layer):
        total = read(1) * float(stiff[layer, 1])
        for k in range(2, 7):
            total = total + read(k) * float(stiff[layer, k])
        return total

    def outer_z(low, high, layer):
        return low * float(stiff[layer, 0]) + high * float(stiff[layer, 7])

    here = (g_x, g_y, g_z, g_m)
    edge = weights(0)

    for layer in ORDER:
        boundary[layer] = spread_out(placed[layer]) * sharing[layer]
    loads[6].wait()
    for layer in ORDER:
        along_z = inner_z(lambda k: boundary[k], layer)
        along_z = along_z + outer_z(boundary[0], boundary[7], layer)
        tile = boundary[layer]
        total = in_plane(tile, here) + g_z * along_z + g_m * (tile - forcing_ref[layer])
        total = weights(layer) * total
        if layer in (0, 7):
            total = plane_sum(total)
        residual[layer] = total
        if layer == 7:
            faces[2, 0] = residual[0]
            faces[2, 1] = residual[7]
            send_faces(2)

    beyond = []
    for side in range(2):

        @pl.when(near[side])
        def _():
            geometry_copy(side == 0).wait_recv()

        along = [geometry_halo[side, d : d + 1, :] for d in range(4)]
        own = boundary[0 if side == 0 else 7]
        term = in_plane(own, along)
        term = term + (along[2] * float(stiff[0, 0]) + along[3]) * own
        beyond.append((term, along[2] * float(stiff[0, 7])))
    values = values + [gather_field(field) for field in range(1, fields)]
    for row in range(height):
        interface_ref[:, row * lanes : (row + 1) * lanes] = jnp.concatenate(
            [value[row : row + 1] for value in values], 0
        )
    stores[0].start()

    with jax.named_scope('w_rim'):
        for at in range(4):

            @pl.when(rim_comes[at])
            def _():
                rim_copy(at).wait_recv()

    low = spread_out(rim_halo[0]) * sharing[0]
    high = spread_out(rim_halo[1]) * sharing[7]
    boundary[0] = boundary[0] + low
    boundary[7] = boundary[7] + high
    for layer in range(1, 7):
        more = weights(layer) * (g_z * outer_z(low, high, layer))
        residual[layer] = -free[layer] * plane_sum(residual[layer] + more)
        rho[layer] = residual[layer]
        vectors[0, layer] = inverse[layer] * residual[layer]
    half_share = 0.5 / plane_count
    ends = []
    for side, (own, layer) in enumerate(((low, 0), (high, 7))):
        more = in_plane(own, here) + g_m * own + g_z * outer_z(low, high, layer)
        term, across_z = beyond[side]
        more = more + term + across_z * (spread_out(rim_halo[2 + side]) * half_share)
        ends.append(residual[layer] + plane_sum(edge * more))

    def prepare(turn):
        def read(k):
            return vectors[turn, k]

        for layer in range(1, 7):
            tile = vectors[turn, layer]
            partial[layer] = (
                in_plane(tile, here) + g_m * tile + g_z * inner_z(read, layer)
            )
        for layer in (0, 7):
            partial[layer] = g_z * inner_z(read, layer)

    prepare(0)
    with jax.named_scope('w_f2'):
        wait_faces(2)
    for side, layer in ((0, 0), (1, 7)):
        residual[layer] = -free[layer] * (ends[side] + halo[2, side])
        rho[layer] = residual[layer]
        vectors[0, layer] = inverse[layer] * residual[layer]

    sums = {}

    def gather_sum(key, value):
        value = jnp.sum(value, axis=0)
        sums[key] = value if key not in sums else sums[key] + value

    for turn in range(ITERS):
        phase = 3 + turn
        low = vectors[turn, 0]
        high = vectors[turn, 7]
        outer = {}
        for layer in (0, 7):
            tile = vectors[turn, layer]
            total = in_plane(tile, here) + g_m * tile + g_z * outer_z(low, high, layer)
            outer[layer] = edge * (total + partial[layer])
            images[turn, layer] = plane_sum(outer[layer])
        faces[phase, 0] = images[turn, 0]
        faces[phase, 1] = images[turn, 7]
        send_faces(phase)
        last = turn == ITERS - 1
        for layer in range(8):
            if layer in outer:
                tile = outer[layer]
            else:
                tile = partial[layer] + g_z * outer_z(low, high, layer)
                tile = weights(layer) * tile
            for other_turn in range(turn + 1):
                gather_sum((other_turn, turn), tile * vectors[other_turn, layer])
            gather_sum(
                turn, vectors[turn, layer] * residual[layer] * sharing[layer]
            )
            if layer not in outer:
                images[turn, layer] = tile if last else free[layer] * plane_sum(tile)
        if last:
            break
        for layer in range(1, 7):
            rho[layer] = images[turn, layer] - SHIFTS[turn] * rho[layer]
            vectors[turn + 1, layer] = inverse[layer] * rho[layer]
        prepare(turn + 1)
        with jax.named_scope('w_fc'):
            wait_faces(phase)
        for side, layer in ((0, 0), (1, 7)):
            images[turn, layer] = free[layer] * (images[turn, layer] + halo[phase, side])
            rho[layer] = images[turn, layer] - SHIFTS[turn] * rho[layer]
            vectors[turn + 1, layer] = inverse[layer] * rho[layer]

    keys = list(range(ITERS)) + [(a, b) for b in range(ITERS) for a in range(b + 1)]
    spot = lax.broadcasted_iota(jnp.int32, (1, 128), 1)
    packed = jnp.zeros((1, 128), jnp.float32)
    for at, key in enumerate(keys):
        value = jnp.sum(jnp.sum(sums[key], axis=0, keepdims=True), axis=1, keepdims=True)
        packed = jnp.where(spot == at, value, packed)
    dots[...] = packed
    for step in range(1, n):
        dot_copy(step).start()
    all_dots[slab] = dots[...]
    for layer in range(1, 7):
        images[ITERS - 1, layer] = free[layer] * plane_sum(images[ITERS - 1, layer])
    with jax.named_scope('w_fc'):
        wait_faces(3 + ITERS - 1)
    for side, layer in ((0, 0), (1, 7)):
        images[ITERS - 1, layer] = free[layer] * (
            images[ITERS - 1, layer] + halo[3 + ITERS - 1, side]
        )
    with jax.named_scope('w_dots'):
        for step in range(1, n):
            dot_copy(step).wait_recv()
    total = jnp.sum(all_dots[...], axis=0)
    found = {key: total[:, at : at + 1] for at, key in enumerate(keys)}
    steps_taken = solve(found)
    for layer in range(8):
        moved = boundary[layer]
        for turn in range(ITERS):
            moved = moved + steps_taken[turn] * vectors[turn, layer]
        velocity[layer] = moved
    stores[1].start()
    for layer in range(8):
        left_over = residual[layer]
        for turn in range(ITERS):
            left_over = left_over - steps_taken[turn] * images[turn, layer]
        rho[layer] = left_over
    stores[2].start()
    for step in range(1, n):
        dot_copy(step).wait_send()
    for side in range(2):

        @pl.when(near[1 - side])
        def _():
            geometry_copy(side == 0).wait_send()

    for at in range(4):

        @pl.when(rim_sends[at])
        def _():
            rim_copy(at).wait_send()

    for shift in range(-REACH, REACH + 1):

        @pl.when(inside(slab + shift))
        def _():
            ask(shift).wait_send()

        @pl.when(inside(slab - shift))
        def _():
            reply(shift).wait_send()

    for store in stores:
        store.wait()


def flush(*refs):
    count = (len(refs) - 1) // 2
    sem = refs[-1]
    copies = [
        pltpu.make_async_copy(refs[at], refs[count + at], sem.at[at]) for at in range(count)
    ]
    for copy in copies:
        copy.start()
    for copy in copies:
        copy.wait()


def body(n, donor_fields, interp_weights, donor_owner, donor_element, geometry, wall_flag, forcing):
    fields = donor_fields.shape[0]
    elems = geometry.shape[1]
    receptors = donor_element.shape[0]
    slots = 2 * REACH + 1
    lanes = 128
    count = receptors // lanes
    cube = (8, 8, 8, elems)
    phases = 3 + ITERS
    room = count // 2
    vmem = pl.BlockSpec(memory_space=pltpu.VMEM)
    hbm = pl.BlockSpec(memory_space=pltpu.HBM)
    shapes = (
        jax.ShapeDtypeStruct(cube, jnp.float32),
        jax.ShapeDtypeStruct(cube, jnp.float32),
        jax.ShapeDtypeStruct((fields, receptors), jnp.float32),
    )
    outputs = pl.pallas_call(
        functools.partial(kernel, n),
        out_shape=shapes,
        in_specs=[hbm] * 7,
        out_specs=(hbm, hbm, hbm),
        scratch_shapes=[
            pltpu.VMEM(cube, jnp.float32),
            pltpu.VMEM(cube, jnp.float32),
            pltpu.VMEM((fields, receptors), jnp.float32),
            pltpu.VMEM((fields, 512, elems), jnp.float32),
            pltpu.VMEM(cube, jnp.float32),
            pltpu.VMEM(interp_weights.shape, jnp.float32),
            pltpu.VMEM((count, lanes), jnp.int32),
            pltpu.VMEM((count, lanes), jnp.int32),
            pltpu.VMEM(geometry.shape, jnp.float32),
            pltpu.VMEM(wall_flag.shape, jnp.int32),
            pltpu.VMEM((3, count, lanes), jnp.float32),
            pltpu.VMEM((slots, 4, room, lanes), jnp.float32),
            pltpu.VMEM((slots * count, lanes), jnp.int32),
            pltpu.VMEM(cube, jnp.float32),
            pltpu.VMEM((8, 8, elems), jnp.float32),
            pltpu.VMEM((8, 8, elems), jnp.float32),
            pltpu.SemaphoreType.DMA((7,)),
            pltpu.VMEM((fields * 512, 2 * elems), jnp.bfloat16),
            pltpu.VMEM((slots, 4, room, lanes), jnp.float32),
            pltpu.VMEM((slots, fields, room, lanes), jnp.float32),
            pltpu.VMEM((slots, fields, room, lanes), jnp.float32),
            pltpu.VMEM((phases, 2, 8, 8, elems), jnp.float32),
            pltpu.VMEM((phases, 2, 8, 8, elems), jnp.float32),
            pltpu.VMEM((1, 128), jnp.float32),
            pltpu.VMEM((n, 1, 128), jnp.float32),
            pltpu.VMEM((ITERS,) + cube, jnp.float32),
            pltpu.VMEM((ITERS,) + cube, jnp.float32),
            pltpu.VMEM(cube, jnp.float32),
            pltpu.VMEM(cube, jnp.float32),
            pltpu.VMEM((2, 8, elems), jnp.float32),
            pltpu.VMEM((4, 8, elems), jnp.float32),
            pltpu.VMEM((2,) + geometry.shape, jnp.float32),
        ]
        + [pltpu.VMEM(cube, jnp.float32)] * 4
        + [pltpu.SemaphoreType.DMA((slots,))] * 4
        + [pltpu.SemaphoreType.DMA((phases, 2))] * 2
        + [pltpu.SemaphoreType.DMA((n,))] * 2
        + [pltpu.SemaphoreType.DMA((4,))] * 2
        + [pltpu.SemaphoreType.DMA((2,))] * 2
        + [pltpu.SemaphoreType.DMA((3,))],
        compiler_params=pltpu.CompilerParams(
            collective_id=0, has_side_effects=True, vmem_limit_bytes=67043328
        ),
    )(
        donor_fields,
        interp_weights,
        donor_owner.reshape(count, lanes),
        donor_element.reshape(count, lanes),
        geometry,
        wall_flag,
        forcing.reshape(cube),
    )
    velocity, residual, interface = pl.pallas_call(
        flush,
        out_shape=shapes,
        in_specs=[vmem] * 3,
        out_specs=(hbm,) * 3,
        scratch_shapes=[pltpu.SemaphoreType.DMA((3,))],
    )(*outputs)
    return (velocity.reshape(512, elems), residual.reshape(512, elems), interface)


def solution(mesh):
    in_specs = (
        P(None, None, ("mesh", "dom")),
        P(None, None, ("mesh", "dom")),
        P(("mesh", "dom"), None),
        P(("mesh", "dom")),
        P(None, ("mesh", "dom")),
        P(None, ("mesh", "dom")),
        P(None, ("mesh", "dom")),
    )
    out_specs = (P(None, ("mesh", "dom")), P(None, ("mesh", "dom")), P(None, ("mesh", "dom")))
    return jax.shard_map(
        functools.partial(body, mesh.shape["dom"]),
        mesh=mesh,
        in_specs=in_specs,
        out_specs=out_specs,
        check_vma=False,
    )
```

```python
import functools

import jax
import jax.numpy as jnp
import numpy as np
from jax import lax
from jax.experimental import pallas as pl
from jax.experimental.pallas import tpu as pltpu
from jax.sharding import PartitionSpec as P

EX = 8
EY = 16
ITERS = 3
REACH = 2
CHUNK = 256
ORDER = (0, 7, 1, 2, 3, 4, 5, 6)
SHIFTS = (1.5, 0.5)
WINDOWS = (1, 1)
MESH = pl.DeviceIdType.MESH


def legendre_pair(values, degree):
    previous = values * 0.0 + 1.0
    current = values * 1.0
    for poly_order in range(2, degree + 1):
        previous, current = (
            current,
            ((2 * poly_order - 1) * values * current - (poly_order - 1) * previous) / poly_order,
        )
    return (current, previous)


def gll_tables():
    degree = 7
    points_count = degree + 1
    abscissae = np.cos(np.pi * np.arange(points_count) / degree)
    for newton_turn in range(80):
        top_poly, lower_poly = legendre_pair(abscissae, degree)
        abscissae = abscissae - (abscissae * top_poly - lower_poly) / (points_count * top_poly)
    abscissae = np.sort(abscissae)
    top_poly, lower_poly = legendre_pair(abscissae, degree)
    quad_weights = 2.0 / (degree * points_count * top_poly * top_poly)
    identity_mat = np.eye(points_count)
    spacing = abscissae[:, None] - abscissae[None, :] + identity_mat
    derivative = top_poly[:, None] / (top_poly[None, :] * spacing) * (1.0 - identity_mat)
    derivative[0, 0] = -degree * points_count / 4.0
    derivative[degree, degree] = degree * points_count / 4.0
    return (abscissae, derivative, quad_weights)


def solve(found):
    matrix = [
        [found[(min(a, b), max(a, b))] for b in range(ITERS)] for a in range(ITERS)
    ]
    right = [found[a] for a in range(ITERS)]
    pivots = []
    for a in range(ITERS):
        pivots.append(1.0 / matrix[a][a])
        for b in range(a + 1, ITERS):
            factor = matrix[b][a] * pivots[a]
            for c in range(a + 1, ITERS):
                matrix[b][c] = matrix[b][c] - factor * matrix[a][c]
            right[b] = right[b] - factor * right[a]
    answer = [None] * ITERS
    for a in reversed(range(ITERS)):
        total = right[a]
        for b in range(a + 1, ITERS):
            total = total - matrix[a][b] * answer[b]
        answer[a] = total * pivots[a]
    return answer


def kernel(
    n,
    donor_hbm,
    weights_hbm,
    owner_hbm,
    element_hbm,
    geometry_hbm,
    wall_hbm,
    forcing_hbm,
    velocity_hbm,
    residual_hbm,
    interface_hbm,
    velocity,
    residual,
    interface_ref,
    donor_ref,
    forcing_ref,
    weights_ref,
    owner_ref,
    element_ref,
    geometry_ref,
    wall_ref,
    position_ref,
    request_ref,
    ranks,
    along_y_ref,
    along_x_ref,
    plane_ref,
    load_sem,
    split,
    asked,
    answer,
    answered,
    faces,
    halo,
    dots,
    all_dots,
    vectors,
    images,
    partial,
    rho,
    rim,
    rim_halo,
    geometry_halo,
    packet,
    inverse,
    free,
    sharing,
    boundary,
    ask_send,
    ask_recv,
    reply_send,
    reply_recv,
    face_send,
    face_recv,
    dot_send,
    dot_recv,
    rim_send,
    rim_recv,
    geometry_send,
    geometry_recv,
    store_sem,
):
    points, derivative, quad = gll_tables()
    stiff = (derivative.T * quad) @ derivative / quad[:, None]
    fields = donor_ref.shape[0]
    elems = donor_ref.shape[2]
    height = owner_ref.shape[0]
    lanes = owner_ref.shape[1]
    receptors = height * lanes
    room = request_ref.shape[2]
    slots = 2 * REACH + 1
    mesh_id = lax.axis_index("mesh")
    slab = lax.axis_index("dom")
    other = 1 - mesh_id

    pairs = [
        (weights_hbm, weights_ref),
        (owner_hbm, owner_ref),
        (element_hbm, element_ref),
        (donor_hbm, donor_ref),
        (geometry_hbm, geometry_ref),
        (wall_hbm, wall_ref),
        (forcing_hbm, forcing_ref),
    ]
    loads = [
        pltpu.make_async_copy(source, target, load_sem.at[at])
        for at, (source, target) in enumerate(pairs)
    ]
    for load in loads:
        load.start()

    def inside(index):
        return jnp.logical_and(index >= 0, index < n)

    barrier = pltpu.get_barrier_semaphore()
    greeted = n - 1
    for step in range(1, n):
        pl.semaphore_signal(
            barrier, inc=1, device_id=(mesh_id, lax.rem(slab + step, n)), device_id_type=MESH
        )
    for shift in range(-REACH, REACH + 1):
        greeted = greeted + jnp.where(inside(slab + shift), 1, 0)

        @pl.when(inside(slab + shift))
        def _():
            pl.semaphore_signal(
                barrier, inc=1, device_id=(other, slab + shift), device_id_type=MESH
            )

    with jax.named_scope('w_loads'):
        for load in loads[:3]:
            load.wait()
    depth = lax.broadcasted_iota(jnp.int32, (8, lanes), 0)
    ladder = jnp.zeros((8, lanes), jnp.float32)
    for a in range(8):
        ladder = jnp.where(depth == a, float(points[a]), ladder)
    for d in range(3):
        for row in range(height):
            part = weights_ref[d, :, row * lanes : (row + 1) * lanes] * ladder
            position_ref[d, row : row + 1, :] = jnp.sum(part, axis=0, keepdims=True)
    owner = owner_ref[...]
    element_code = element_ref[...] * receptors
    members = [owner == slab + shift for shift in range(-REACH, REACH + 1)]
    tall = slots * height
    marks = jnp.concatenate([jnp.where(m, 1.0, 0.0) for m in members], 0).astype(jnp.bfloat16)
    before = lax.broadcasted_iota(jnp.int32, (lanes, lanes), 0)
    after = lax.broadcasted_iota(jnp.int32, (lanes, lanes), 1)
    upper = jnp.where(before < after, 1.0, 0.0).astype(jnp.bfloat16)
    left = jnp.dot(marks, upper, preferred_element_type=jnp.float32).astype(jnp.bfloat16)
    above = lax.broadcasted_iota(jnp.int32, (tall, tall), 0)
    below = lax.broadcasted_iota(jnp.int32, (tall, tall), 1)
    same = above // height == below // height
    block = jnp.where(same, 1.0, 0.0).astype(jnp.bfloat16)
    lower = jnp.where(same & (below < above), 1.0, 0.0).astype(jnp.bfloat16)
    rank = jnp.dot(block, left, preferred_element_type=jnp.float32)
    rank = rank + jnp.dot(lower, marks, preferred_element_type=jnp.float32)
    rank = rank.astype(jnp.int32)
    ranks[...] = rank
    row_index = lax.broadcasted_iota(jnp.int32, (height, lanes), 0)
    place = lax.broadcasted_iota(jnp.int32, (height, lanes), 1) * height + row_index
    row_bits = height.bit_length() - 1
    steps = receptors.bit_length() - 1

    def pull(tile, step):
        if step >= row_bits:
            return pltpu.roll(tile, lanes - (1 << (step - row_bits)), 1)
        jump = 1 << step
        near = pltpu.roll(tile, height - jump, 0)
        far = pltpu.roll(near, lanes - 1, 1)
        return jnp.where(row_index < height - jump, near, far)

    words = []
    comps = []
    start = [position_ref[d] for d in range(3)]
    for slot in range(slots):
        shift = place - rank[slot * height : (slot + 1) * height]
        words.append(jnp.where(members[slot], element_code + shift, 0))
        comps.append(list(start))
    for step in range(steps):
        for slot in range(slots):
            word = words[slot]
            moving = word & (1 << step)
            came = pull(word, step)
            take = (came & (1 << step)) != 0
            words[slot] = jnp.where(take, came - (1 << step), jnp.where(moving != 0, 0, word))
            comps[slot] = [jnp.where(take, pull(c, step), c) for c in comps[slot]]
    half = lanes // 2
    left_half = lax.broadcasted_iota(jnp.int32, (room, lanes), 1) < half
    for slot in range(slots):
        columns = comps[slot] + [(words[slot] >> steps).astype(jnp.float32)]
        for at, column in enumerate(columns):
            request_ref[slot, at] = jnp.where(
                left_half, column[:room], pltpu.roll(column[room:], half, 1)
            )

    with jax.named_scope('w_barrier'):
        pl.semaphore_wait(barrier, greeted)

    def ask(shift):
        return pltpu.make_async_remote_copy(
            src_ref=request_ref.at[shift + REACH],
            dst_ref=asked.at[shift + REACH],
            send_sem=ask_send.at[shift + REACH],
            recv_sem=ask_recv.at[shift + REACH],
            device_id=(other, lax.rem(slab + shift + n, n)),
            device_id_type=MESH,
        )

    def reply(shift, part):
        span = pl.ds(0, 1) if part == 0 else pl.ds(1, fields - 1)
        return pltpu.make_async_remote_copy(
            src_ref=answer.at[shift + REACH, span],
            dst_ref=answered.at[shift + REACH, span],
            send_sem=reply_send.at[part, shift + REACH],
            recv_sem=reply_recv.at[part, shift + REACH],
            device_id=(other, lax.rem(slab - shift + n, n)),
            device_id_type=MESH,
        )

    def face_copy(phase, up):
        step = 1 if up else n - 1
        return pltpu.make_async_remote_copy(
            src_ref=faces.at[phase, 1 if up else 0],
            dst_ref=halo.at[phase, 0 if up else 1],
            send_sem=face_send.at[phase, 1 if up else 0],
            recv_sem=face_recv.at[phase, 0 if up else 1],
            device_id=(mesh_id, lax.rem(slab + step, n)),
            device_id_type=MESH,
        )

    def send_faces(phase):
        @pl.when(slab < n - 1)
        def _():
            face_copy(phase, True).start()

        @pl.when(slab > 0)
        def _():
            face_copy(phase, False).start()

    def wait_faces(phase):
        @pl.when(slab > 0)
        def _():
            face_copy(phase, True).wait_recv()

        @pl.when(slab < n - 1)
        def _():
            face_copy(phase, False).wait_recv()

        @pl.when(slab < n - 1)
        def _():
            face_copy(phase, True).wait_send()

        @pl.when(slab > 0)
        def _():
            face_copy(phase, False).wait_send()

    def dot_copy(step):
        return pltpu.make_async_remote_copy(
            src_ref=dots,
            dst_ref=all_dots.at[slab],
            send_sem=dot_send.at[step],
            recv_sem=dot_recv.at[step],
            device_id=(mesh_id, lax.rem(slab + step, n)),
            device_id_type=MESH,
        )

    rim_jumps = (1, -1, 2, -2)
    rim_sends = [inside(slab + jump) for jump in rim_jumps]
    rim_comes = [inside(slab - jump) for jump in rim_jumps]
    near = (slab > 0, slab < n - 1)

    def rim_copy(at):
        return pltpu.make_async_remote_copy(
            src_ref=rim.at[1 - at % 2],
            dst_ref=rim_halo.at[at],
            send_sem=rim_send.at[at],
            recv_sem=rim_recv.at[at],
            device_id=(mesh_id, lax.rem(slab + rim_jumps[at] + n, n)),
            device_id_type=MESH,
        )

    def geometry_copy(up):
        side = 0 if up else 1
        return pltpu.make_async_remote_copy(
            src_ref=packet,
            dst_ref=geometry_halo.at[side],
            send_sem=geometry_send.at[side],
            recv_sem=geometry_recv.at[side],
            device_id=(mesh_id, lax.rem(slab + (1 if up else n - 1), n)),
            device_id_type=MESH,
        )

    stores = [
        pltpu.make_async_copy(source, target, store_sem.at[at])
        for at, (source, target) in enumerate(
            ((interface_ref, interface_hbm), (velocity, velocity_hbm), (rho, residual_hbm))
        )
    ]

    for distance in range(REACH + 1):
        for shift in sorted({distance, -distance}):

            @pl.when(inside(slab + shift))
            def _():
                ask(shift).start()

    phases = halo.shape[0]
    blank = jnp.zeros(halo.shape[2:], jnp.float32)

    for at in range(4):

        @pl.when(jnp.logical_not(rim_comes[at]))
        def _():
            rim_halo[at] = jnp.zeros(rim_halo.shape[1:], jnp.float32)

    for side in range(2):

        @pl.when(jnp.logical_not(near[side]))
        def _():
            geometry_halo[side] = jnp.zeros(geometry_halo.shape[1:], jnp.float32)

    @pl.when(slab == 0)
    def _():
        for phase in range(phases):
            halo[phase, 0] = blank

    @pl.when(slab == n - 1)
    def _():
        for phase in range(phases):
            halo[phase, 1] = blank

    node = lax.broadcasted_iota(jnp.int32, (8, elems), 0)
    element = lax.broadcasted_iota(jnp.int32, (8, elems), 1)
    x_index = element % EX
    y_index = element // EX % EY

    across = jnp.zeros((8, elems), jnp.float32)
    for a in range(8):
        across = jnp.where(node == a, float(quad[a]), across)
    for j in range(8):
        plane_ref[j] = across * float(quad[j])
        for m in range(8):
            along_y_ref[m, j] = jnp.full((8, elems), float(stiff[j, m]), jnp.float32)
    for step in range(8):
        turned = jnp.zeros((8, elems), jnp.float32)
        for i in range(8):
            turned = jnp.where(node == i, float(stiff[i, (i - step) % 8]), turned)
        along_x_ref[step] = turned

    def flag(condition):
        return jnp.where(condition, 1.0, 0.0)

    x_low = flag((node == 0) & (x_index > 0))
    x_high = flag((node == 7) & (x_index < EX - 1))
    y_low = flag(y_index > 0)
    y_high = flag(y_index < EY - 1)

    def plane_sum(tile):
        below = pltpu.roll(pltpu.roll(tile, 1, 1), 1, 2)
        above = pltpu.roll(pltpu.roll(tile, 7, 1), elems - 1, 2)
        tile = tile + below * x_low + above * x_high
        low = tile[0] + y_low * pltpu.roll(tile[7], EX, 1)
        high = tile[7] + y_high * pltpu.roll(tile[0], elems - EX, 1)
        return jnp.concatenate([low[None], tile[1:7], high[None]], 0)

    def weights(layer):
        return plane_ref[...] * float(quad[layer])

    loads[4].wait()
    loads[5].wait()

    wall_rows = []
    for side in range(2):
        wall_row = jnp.zeros((1, elems), jnp.float32)
        for x in range(EX):
            bit = wall_ref[side : side + 1, x : x + 1].astype(jnp.float32)
            wall_row = jnp.where(x_index[0:1] == x, bit, wall_row)
        wall_rows.append(wall_row)
    g_x, g_y, g_z, g_m = [geometry_ref[d : d + 1, :] for d in range(4)]

    packet[...] = jnp.concatenate(
        [geometry_ref[...]] + wall_rows + [jnp.zeros((2, elems), jnp.float32)], 0
    )

    @pl.when(near[1])
    def _():
        geometry_copy(True).start()

    @pl.when(near[0])
    def _():
        geometry_copy(False).start()

    diag_y = [jnp.full((8, elems), float(stiff[j, j]), jnp.float32)[None] for j in range(8)]
    diag_y = jnp.concatenate(diag_y, 0)

    def diagonal(along, layer):
        total = along[0] * along_x_ref[0] + along[1] * diag_y
        total = total + (along[2] * float(stiff[layer, layer]) + along[3])
        return plane_sum(weights(layer) * total)

    nothing = jnp.zeros((6, 8, elems), jnp.float32)

    def wall_marks(rows):
        low_wall = flag(y_index == 0) * rows[0]
        high_wall = flag(y_index == EY - 1) * rows[1]
        return plane_sum(jnp.concatenate([low_wall[None], nothing, high_wall[None]], 0))

    wall_plane = wall_marks(wall_rows)
    x_count = 1.0 + x_low + x_high
    y_count_low = 1.0 + y_low
    y_count_high = 1.0 + y_high
    plane_count = jnp.concatenate(
        [(x_count * y_count_low)[None]]
        + [x_count[None]] * 6
        + [(x_count * y_count_high)[None]],
        0,
    )
    mark = flag((node == 0) & (x_index == 0)) + flag((node == 7) & (x_index == EX - 1))

    def settle(layer, z_count, walls, diag):
        count = plane_count * z_count
        open_part = 1.0 - jnp.minimum(mark * count + walls, 1.0)
        sharing[layer] = 1.0 / count
        free[layer] = open_part
        inverse[layer] = open_part / diag

    for layer in range(1, 7):
        settle(layer, 1.0, wall_plane, diagonal((g_x, g_y, g_z, g_m), layer))
    z_counts = (jnp.where(slab > 0, 2.0, 1.0), jnp.where(slab < n - 1, 2.0, 1.0))
    for side, layer in ((0, 0), (1, 7)):
        sharing[layer] = 1.0 / (plane_count * z_counts[side])

    with jax.named_scope('w_donor'):
        loads[3].wait()
    donors = donor_ref[...].reshape(fields * 512, elems)
    coarse = donors.astype(jnp.bfloat16)
    split[:, :elems] = coarse
    split[:, elems:] = (donors - coarse.astype(jnp.float32)).astype(jnp.bfloat16)

    code = lax.broadcasted_iota(jnp.int32, (elems, CHUNK), 0)
    code = code.astype(jnp.float32)
    basis = lax.broadcasted_iota(jnp.int32, (8, CHUNK), 0)
    norms = [
        float(1.0 / np.prod([points[a] - points[b] for b in range(8) if b != a])) for a in range(8)
    ]
    scale = jnp.zeros((8, CHUNK), jnp.float32)
    for a in range(8):
        scale = jnp.where(basis == a, norms[a], scale)

    def lagrange(position):
        value = scale
        for b in range(8):
            value = value * jnp.where(basis == b, 1.0, position - float(points[b]))
        return value

    def evaluate(shift, first, last):
        group = CHUNK // lanes
        for chunk in range(room // group):
            block = [
                jnp.concatenate(
                    [
                        asked[shift + REACH, c, chunk * group + t : chunk * group + t + 1, :]
                        for t in range(group)
                    ],
                    1,
                )
                for c in range(4)
            ]
            chosen = jnp.where(block[3] == code, 1.0, 0.0).astype(jnp.bfloat16)
            chosen = jnp.concatenate([chosen, chosen], 0)
            w_x, w_y, w_z = [lagrange(block[d]) for d in range(3)]
            picked = jnp.dot(
                split[first * 512 : last * 512], chosen, preferred_element_type=jnp.float32
            )
            for field in range(first, last):
                cube = picked[(field - first) * 512 : (field - first + 1) * 512]
                cube = cube.reshape(8, 64, CHUNK)
                total = cube[0] * w_z[0:1, :]
                for k in range(1, 8):
                    total = total + cube[k] * w_z[k : k + 1, :]
                total = total.reshape(8, 8, CHUNK)
                line = total[0] * w_y[0:1, :]
                for j in range(1, 8):
                    line = line + total[j] * w_y[j : j + 1, :]
                value = jnp.sum(line * w_x, axis=0, keepdims=True)
                for t in range(group):
                    row = chunk * group + t
                    answer[shift + REACH, field, row : row + 1, :] = value[
                        :, t * lanes : (t + 1) * lanes
                    ]

    def serve(turn, carry):
        shift = ((turn + 1) // 2) * (2 * (turn % 2) - 1)

        @pl.when(inside(slab - shift))
        def _():
            with jax.named_scope('w_ask'):
                ask(shift).wait_recv()
            evaluate(shift, 0, 1)
            with jax.named_scope('reply'):
                reply(shift, 0).start()

        return carry

    lax.fori_loop(0, slots, serve, 0)
    turns_left = list(range(slots))

    def serve_rest(many):
        for _ in range(many):
            turn = turns_left.pop(0)
            shift = ((turn + 1) // 2) * (2 * (turn % 2) - 1)

            @pl.when(inside(slab - shift))
            def _():
                with jax.named_scope('rest'):
                    evaluate(shift, 1, fields)
                reply(shift, 1).start()

    room_index = lax.broadcasted_iota(jnp.int32, (room, lanes), 0)
    plans = []
    for slot in range(slots):
        table = ranks[slot * height : (slot + 1) * height, :]
        base = jnp.broadcast_to(table[0:1], (room, lanes))
        first = jnp.minimum(base >> row_bits, half - 1)
        second = jnp.minimum(first + 1, half - 1)
        offset = base & (height - 1)
        spots = table & (height - 1)
        plans.append((first, second, offset, spots))

    serve_rest(2)
    for shift in range(-REACH, REACH + 1):

        @pl.when(jnp.logical_not(inside(slab + shift)))
        def _():
            answered[shift + REACH] = jnp.zeros(answered.shape[1:], jnp.float32)

        @pl.when(inside(slab + shift))
        def _():
            with jax.named_scope('w_reply'):
                reply(shift, 0).wait_recv()

    def along_lanes(tile, index):
        return jnp.take_along_axis(tile, index, axis=1, mode="promise_in_bounds")

    def along_rows(tile, index):
        return jnp.take_along_axis(tile, index, axis=0, mode="promise_in_bounds")

    def gather_field(field):
        result = [jnp.zeros((room, lanes), jnp.float32)] * 2
        for slot in range(slots):
            packed = answered[slot, field]
            first, second, offset, spots = plans[slot]
            windows = [
                jnp.where(
                    room_index + part * room >= offset,
                    along_lanes(packed, first + part * half),
                    along_lanes(packed, second + part * half),
                )
                for part in range(2)
            ]
            for part in range(2):
                spot = spots[part * room : (part + 1) * room]
                member = members[slot][part * room : (part + 1) * room]
                low, high = [along_rows(window, spot & (room - 1)) for window in windows]
                tile = jnp.where(spot < room, low, high)
                result[part] = jnp.where(member, tile, result[part])
        return jnp.concatenate(result, 0)

    values = [gather_field(0)]
    groups = lanes // 64
    rows = jnp.concatenate([values[0][:, t * 64 : (t + 1) * 64] for t in range(groups)], 0)
    per_side = height // 2
    row = lax.broadcasted_iota(jnp.int32, (groups * height, elems), 0)
    spot = lax.broadcasted_iota(jnp.int32, (groups * height, elems), 1)
    piece = row % height
    target = (groups * (piece % per_side) + row // height) * EX + (EX - 1) * (piece // per_side)
    placed = lax.dot_general(
        rows,
        flag(spot == target),
        (((0,), (0,)), ((), ())),
        precision=lax.Precision.HIGHEST,
        preferred_element_type=jnp.float32,
    ).reshape(8, 8, elems)
    rim[0] = placed[0]
    rim[1] = placed[7]
    for at in range(4):

        @pl.when(rim_sends[at])
        def _():
            rim_copy(at).start()

    def spread_out(column):
        return plane_sum(
            jnp.concatenate(
                [
                    (jnp.broadcast_to(column[j : j + 1, :], (8, elems)) * mark)[None]
                    for j in range(8)
                ],
                0,
            )
        )

    def in_plane(tile, along):
        along_y = along_y_ref[0] * tile[0:1]
        for j in range(1, 8):
            along_y = along_y + along_y_ref[j] * tile[j : j + 1]
        along_x = along_x_ref[0] * tile
        for step in range(1, 8):
            along_x = along_x + along_x_ref[step] * pltpu.roll(tile, step, 1)
        return along[0] * along_x + along[1] * along_y

    def inner_z(read, layer):
        total = read(1) * float(stiff[layer, 1])
        for k in range(2, 7):
            total = total + read(k) * float(stiff[layer, k])
        return total

    def outer_z(low, high, layer):
        return low * float(stiff[layer, 0]) + high * float(stiff[layer, 7])

    here = (g_x, g_y, g_z, g_m)
    edge = weights(0)

    for layer in ORDER:
        boundary[layer] = spread_out(placed[layer]) * sharing[layer]
    loads[6].wait()
    for layer in ORDER:
        along_z = inner_z(lambda k: boundary[k], layer)
        along_z = along_z + outer_z(boundary[0], boundary[7], layer)
        tile = boundary[layer]
        total = in_plane(tile, here) + g_z * along_z + g_m * (tile - forcing_ref[layer])
        total = weights(layer) * total
        if layer in (0, 7):
            total = plane_sum(total)
        residual[layer] = total
        if layer == 7:
            faces[0, 0] = residual[0]
            faces[0, 1] = residual[7]
            send_faces(0)

    beyond = []
    for side in range(2):

        @pl.when(near[side])
        def _():
            geometry_copy(side == 0).wait_recv()

        along = [geometry_halo[side, d : d + 1, :] for d in range(4)]
        own = boundary[0 if side == 0 else 7]
        term = in_plane(own, along)
        term = term + (along[2] * float(stiff[0, 0]) + along[3]) * own
        beyond.append((term, along[2] * float(stiff[0, 7])))
        walls = wall_plane + wall_marks([geometry_halo[side, 4:5, :], geometry_halo[side, 5:6, :]])
        layer, facing = (0, 7) if side == 0 else (7, 0)
        settle(layer, z_counts[side], walls, diagonal(here, layer) + diagonal(along, facing))
    serve_rest(1)

    with jax.named_scope('w_rim'):
        for at in range(4):

            @pl.when(rim_comes[at])
            def _():
                rim_copy(at).wait_recv()

    low = spread_out(rim_halo[0]) * sharing[0]
    high = spread_out(rim_halo[1]) * sharing[7]
    boundary[0] = boundary[0] + low
    boundary[7] = boundary[7] + high
    for layer in range(1, 7):
        more = weights(layer) * (g_z * outer_z(low, high, layer))
        residual[layer] = -free[layer] * plane_sum(residual[layer] + more)
        rho[layer] = residual[layer]
        vectors[0, layer] = inverse[layer] * residual[layer]
    half_share = 0.5 / plane_count
    ends = []
    for side, (own, layer) in enumerate(((low, 0), (high, 7))):
        more = in_plane(own, here) + g_m * own + g_z * outer_z(low, high, layer)
        term, across_z = beyond[side]
        more = more + term + across_z * (spread_out(rim_halo[2 + side]) * half_share)
        ends.append(residual[layer] + plane_sum(edge * more))

    def prepare(turn):
        def read(k):
            return vectors[turn, k]

        for layer in range(1, 7):
            tile = vectors[turn, layer]
            partial[layer] = (
                in_plane(tile, here) + g_m * tile + g_z * inner_z(read, layer)
            )
        for layer in (0, 7):
            partial[layer] = g_z * inner_z(read, layer)

    prepare(0)
    with jax.named_scope('w_f2'):
        wait_faces(0)
    for side, layer in ((0, 0), (1, 7)):
        residual[layer] = -free[layer] * (ends[side] + halo[0, side])
        rho[layer] = residual[layer]
        vectors[0, layer] = inverse[layer] * residual[layer]

    sums = {}

    def gather_sum(key, value):
        value = jnp.sum(value, axis=0)
        sums[key] = value if key not in sums else sums[key] + value

    for turn in range(ITERS):
        phase = 1 + turn
        low = vectors[turn, 0]
        high = vectors[turn, 7]
        outer = {}
        for layer in (0, 7):
            tile = vectors[turn, layer]
            total = in_plane(tile, here) + g_m * tile + g_z * outer_z(low, high, layer)
            outer[layer] = edge * (total + partial[layer])
            images[turn, layer] = plane_sum(outer[layer])
        faces[phase, 0] = images[turn, 0]
        faces[phase, 1] = images[turn, 7]
        send_faces(phase)
        last = turn == ITERS - 1
        for layer in range(8):
            if layer in outer:
                tile = outer[layer]
            else:
                tile = partial[layer] + g_z * outer_z(low, high, layer)
                tile = weights(layer) * tile
            for other_turn in range(turn + 1):
                gather_sum((other_turn, turn), tile * vectors[other_turn, layer])
            gather_sum(
                turn, vectors[turn, layer] * residual[layer] * sharing[layer]
            )
            if layer not in outer:
                images[turn, layer] = tile if last else free[layer] * plane_sum(tile)
        if last:
            break
        for layer in range(1, 7):
            rho[layer] = images[turn, layer] - SHIFTS[turn] * rho[layer]
            vectors[turn + 1, layer] = inverse[layer] * rho[layer]
        prepare(turn + 1)
        serve_rest(WINDOWS[turn])
        with jax.named_scope('w_fc'):
            wait_faces(phase)
        for side, layer in ((0, 0), (1, 7)):
            images[turn, layer] = free[layer] * (images[turn, layer] + halo[phase, side])
            rho[layer] = images[turn, layer] - SHIFTS[turn] * rho[layer]
            vectors[turn + 1, layer] = inverse[layer] * rho[layer]

    keys = list(range(ITERS)) + [(a, b) for b in range(ITERS) for a in range(b + 1)]
    spot = lax.broadcasted_iota(jnp.int32, (1, 128), 1)
    packed = jnp.zeros((1, 128), jnp.float32)
    for at, key in enumerate(keys):
        value = jnp.sum(jnp.sum(sums[key], axis=0, keepdims=True), axis=1, keepdims=True)
        packed = jnp.where(spot == at, value, packed)
    dots[...] = packed
    for step in range(1, n):
        dot_copy(step).start()
    all_dots[slab] = dots[...]
    for shift in range(-REACH, REACH + 1):

        @pl.when(inside(slab + shift))
        def _():
            with jax.named_scope('w_rest'):
                reply(shift, 1).wait_recv()

    values = values + [gather_field(field) for field in range(1, fields)]
    for row in range(height):
        interface_ref[:, row * lanes : (row + 1) * lanes] = jnp.concatenate(
            [value[row : row + 1] for value in values], 0
        )
    stores[0].start()
    for layer in range(1, 7):
        images[ITERS - 1, layer] = free[layer] * plane_sum(images[ITERS - 1, layer])
    with jax.named_scope('w_fc'):
        wait_faces(ITERS)
    for side, layer in ((0, 0), (1, 7)):
        images[ITERS - 1, layer] = free[layer] * (
            images[ITERS - 1, layer] + halo[ITERS, side]
        )
    with jax.named_scope('w_dots'):
        for step in range(1, n):
            dot_copy(step).wait_recv()
    with jax.named_scope('solve'):
        total = jnp.sum(all_dots[...], axis=0)
        found = {
            key: jnp.broadcast_to(total[:, at : at + 1], (8, elems))
            for at, key in enumerate(keys)
        }
        steps_taken = solve(found)
    for layer in range(8):
        moved = boundary[layer]
        for turn in range(ITERS):
            moved = moved + steps_taken[turn] * vectors[turn, layer]
        velocity[layer] = moved
    stores[1].start()
    for layer in range(8):
        left_over = residual[layer]
        for turn in range(ITERS):
            left_over = left_over - steps_taken[turn] * images[turn, layer]
        rho[layer] = left_over
    stores[2].start()
    for step in range(1, n):
        dot_copy(step).wait_send()
    for side in range(2):

        @pl.when(near[1 - side])
        def _():
            geometry_copy(side == 0).wait_send()

    for at in range(4):

        @pl.when(rim_sends[at])
        def _():
            rim_copy(at).wait_send()

    for shift in range(-REACH, REACH + 1):

        @pl.when(inside(slab + shift))
        def _():
            ask(shift).wait_send()

        @pl.when(inside(slab - shift))
        def _():
            reply(shift, 0).wait_send()
            reply(shift, 1).wait_send()

    with jax.named_scope('w_store'):
        for store in stores:
            store.wait()


def flush(*refs):
    count = (len(refs) - 1) // 2
    sem = refs[-1]
    copies = [
        pltpu.make_async_copy(refs[at], refs[count + at], sem.at[at]) for at in range(count)
    ]
    for copy in copies:
        copy.start()
    for copy in copies:
        copy.wait()


def body(n, donor_fields, interp_weights, donor_owner, donor_element, geometry, wall_flag, forcing):
    fields = donor_fields.shape[0]
    elems = geometry.shape[1]
    receptors = donor_element.shape[0]
    slots = 2 * REACH + 1
    lanes = 128
    count = receptors // lanes
    cube = (8, 8, 8, elems)
    phases = 1 + ITERS
    room = count // 2
    vmem = pl.BlockSpec(memory_space=pltpu.VMEM)
    hbm = pl.BlockSpec(memory_space=pltpu.HBM)
    shapes = (
        jax.ShapeDtypeStruct(cube, jnp.float32),
        jax.ShapeDtypeStruct(cube, jnp.float32),
        jax.ShapeDtypeStruct((fields, receptors), jnp.float32),
    )
    outputs = pl.pallas_call(
        functools.partial(kernel, n),
        out_shape=shapes,
        in_specs=[hbm] * 7,
        out_specs=(hbm, hbm, hbm),
        scratch_shapes=[
            pltpu.VMEM(cube, jnp.float32),
            pltpu.VMEM(cube, jnp.float32),
            pltpu.VMEM((fields, receptors), jnp.float32),
            pltpu.VMEM((fields, 512, elems), jnp.float32),
            pltpu.VMEM(cube, jnp.float32),
            pltpu.VMEM(interp_weights.shape, jnp.float32),
            pltpu.VMEM((count, lanes), jnp.int32),
            pltpu.VMEM((count, lanes), jnp.int32),
            pltpu.VMEM(geometry.shape, jnp.float32),
            pltpu.VMEM(wall_flag.shape, jnp.int32),
            pltpu.VMEM((3, count, lanes), jnp.float32),
            pltpu.VMEM((slots, 4, room, lanes), jnp.float32),
            pltpu.VMEM((slots * count, lanes), jnp.int32),
            pltpu.VMEM(cube, jnp.float32),
            pltpu.VMEM((8, 8, elems), jnp.float32),
            pltpu.VMEM((8, 8, elems), jnp.float32),
            pltpu.SemaphoreType.DMA((7,)),
            pltpu.VMEM((fields * 512, 2 * elems), jnp.bfloat16),
            pltpu.VMEM((slots, 4, room, lanes), jnp.float32),
            pltpu.VMEM((slots, fields, room, lanes), jnp.float32),
            pltpu.VMEM((slots, fields, room, lanes), jnp.float32),
            pltpu.VMEM((phases, 2, 8, 8, elems), jnp.float32),
            pltpu.VMEM((phases, 2, 8, 8, elems), jnp.float32),
            pltpu.VMEM((1, 128), jnp.float32),
            pltpu.VMEM((n, 1, 128), jnp.float32),
            pltpu.VMEM((ITERS,) + cube, jnp.float32),
            pltpu.VMEM((ITERS,) + cube, jnp.float32),
            pltpu.VMEM(cube, jnp.float32),
            pltpu.VMEM(cube, jnp.float32),
            pltpu.VMEM((2, 8, elems), jnp.float32),
            pltpu.VMEM((4, 8, elems), jnp.float32),
            pltpu.VMEM((2, 8, elems), jnp.float32),
            pltpu.VMEM((8, elems), jnp.float32),
        ]
        + [pltpu.VMEM(cube, jnp.float32)] * 4
        + [pltpu.SemaphoreType.DMA((slots,))] * 2
        + [pltpu.SemaphoreType.DMA((2, slots))] * 2
        + [pltpu.SemaphoreType.DMA((phases, 2))] * 2
        + [pltpu.SemaphoreType.DMA((n,))] * 2
        + [pltpu.SemaphoreType.DMA((4,))] * 2
        + [pltpu.SemaphoreType.DMA((2,))] * 2
        + [pltpu.SemaphoreType.DMA((3,))],
        compiler_params=pltpu.CompilerParams(
            collective_id=0, has_side_effects=True, vmem_limit_bytes=67043328
        ),
    )(
        donor_fields,
        interp_weights,
        donor_owner.reshape(count, lanes),
        donor_element.reshape(count, lanes),
        geometry,
        wall_flag,
        forcing.reshape(cube),
    )
    velocity, residual, interface = pl.pallas_call(
        flush,
        out_shape=shapes,
        in_specs=[vmem] * 3,
        out_specs=(hbm,) * 3,
        scratch_shapes=[pltpu.SemaphoreType.DMA((3,))],
    )(*outputs)
    return (velocity.reshape(512, elems), residual.reshape(512, elems), interface)


def solution(mesh):
    in_specs = (
        P(None, None, ("mesh", "dom")),
        P(None, None, ("mesh", "dom")),
        P(("mesh", "dom"), None),
        P(("mesh", "dom")),
        P(None, ("mesh", "dom")),
        P(None, ("mesh", "dom")),
        P(None, ("mesh", "dom")),
    )
    out_specs = (P(None, ("mesh", "dom")), P(None, ("mesh", "dom")), P(None, ("mesh", "dom")))
    return jax.shard_map(
        functools.partial(body, mesh.shape["dom"]),
        mesh=mesh,
        in_specs=in_specs,
        out_specs=out_specs,
        check_vma=False,
    )
```

```python
import functools

import jax
import jax.numpy as jnp
import numpy as np
from jax import lax
from jax.experimental import pallas as pl
from jax.experimental.pallas import tpu as pltpu
from jax.sharding import PartitionSpec as P

EX = 8
EY = 16
ITERS = 3
REACH = 2
CHUNK = 256
ORDER = (0, 7, 1, 2, 3, 4, 5, 6)
SHIFTS = (1.5, 0.5)
WINDOWS = (1, 1)
MESH = pl.DeviceIdType.MESH


def legendre_pair(values, degree):
    previous = values * 0.0 + 1.0
    current = values * 1.0
    for poly_order in range(2, degree + 1):
        previous, current = (
            current,
            ((2 * poly_order - 1) * values * current - (poly_order - 1) * previous) / poly_order,
        )
    return (current, previous)


def gll_tables():
    degree = 7
    points_count = degree + 1
    abscissae = np.cos(np.pi * np.arange(points_count) / degree)
    for newton_turn in range(80):
        top_poly, lower_poly = legendre_pair(abscissae, degree)
        abscissae = abscissae - (abscissae * top_poly - lower_poly) / (points_count * top_poly)
    abscissae = np.sort(abscissae)
    top_poly, lower_poly = legendre_pair(abscissae, degree)
    quad_weights = 2.0 / (degree * points_count * top_poly * top_poly)
    identity_mat = np.eye(points_count)
    spacing = abscissae[:, None] - abscissae[None, :] + identity_mat
    derivative = top_poly[:, None] / (top_poly[None, :] * spacing) * (1.0 - identity_mat)
    derivative[0, 0] = -degree * points_count / 4.0
    derivative[degree, degree] = degree * points_count / 4.0
    return (abscissae, derivative, quad_weights)


def solve(found):
    matrix = [
        [found[(min(a, b), max(a, b))] for b in range(ITERS)] for a in range(ITERS)
    ]
    right = [found[a] for a in range(ITERS)]
    pivots = []
    for a in range(ITERS):
        pivots.append(1.0 / matrix[a][a])
        for b in range(a + 1, ITERS):
            factor = matrix[b][a] * pivots[a]
            for c in range(a + 1, ITERS):
                matrix[b][c] = matrix[b][c] - factor * matrix[a][c]
            right[b] = right[b] - factor * right[a]
    answer = [None] * ITERS
    for a in reversed(range(ITERS)):
        total = right[a]
        for b in range(a + 1, ITERS):
            total = total - matrix[a][b] * answer[b]
        answer[a] = total * pivots[a]
    return answer


def kernel(
    n,
    donor_hbm,
    weights_hbm,
    owner_hbm,
    element_hbm,
    geometry_hbm,
    wall_hbm,
    forcing_hbm,
    velocity_hbm,
    residual_hbm,
    interface_hbm,
    velocity,
    residual,
    interface_ref,
    donor_ref,
    forcing_ref,
    weights_ref,
    owner_ref,
    element_ref,
    geometry_ref,
    wall_ref,
    position_ref,
    request_ref,
    ranks,
    along_y_ref,
    along_x_ref,
    plane_ref,
    load_sem,
    split,
    asked,
    answer,
    answered,
    faces,
    halo,
    dots,
    all_dots,
    vectors,
    images,
    partial,
    rho,
    rim,
    rim_halo,
    geometry_halo,
    packet,
    inverse,
    free,
    sharing,
    boundary,
    ask_sem,
    reply_sem,
    face_send,
    face_recv,
    dot_sem,
    rim_sem,
    geometry_send,
    geometry_recv,
    store_sem,
):
    points, derivative, quad = gll_tables()
    stiff = (derivative.T * quad) @ derivative / quad[:, None]
    fields = donor_ref.shape[0]
    elems = donor_ref.shape[2]
    height = owner_ref.shape[0]
    lanes = owner_ref.shape[1]
    receptors = height * lanes
    room = request_ref.shape[2]
    slots = 2 * REACH + 1
    mesh_id = lax.axis_index("mesh")
    slab = lax.axis_index("dom")
    other = 1 - mesh_id

    pairs = [
        (weights_hbm, weights_ref),
        (owner_hbm, owner_ref),
        (element_hbm, element_ref),
        (donor_hbm, donor_ref),
        (geometry_hbm, geometry_ref),
        (wall_hbm, wall_ref),
        (forcing_hbm, forcing_ref),
    ]
    loads = [
        pltpu.make_async_copy(source, target, load_sem.at[at])
        for at, (source, target) in enumerate(pairs)
    ]
    for load in loads:
        load.start()

    def inside(index):
        return jnp.logical_and(index >= 0, index < n)

    barrier = pltpu.get_barrier_semaphore()
    greeted = n - 1
    for step in range(1, n):
        pl.semaphore_signal(
            barrier, inc=1, device_id=(mesh_id, lax.rem(slab + step, n)), device_id_type=MESH
        )
    for shift in range(-REACH, REACH + 1):
        greeted = greeted + jnp.where(inside(slab + shift), 1, 0)

        @pl.when(inside(slab + shift))
        def _():
            pl.semaphore_signal(
                barrier, inc=1, device_id=(other, slab + shift), device_id_type=MESH
            )

    with jax.named_scope('w_loads'):
        for load in loads[:3]:
            load.wait()
    depth = lax.broadcasted_iota(jnp.int32, (8, lanes), 0)
    ladder = jnp.zeros((8, lanes), jnp.float32)
    for a in range(8):
        ladder = jnp.where(depth == a, float(points[a]), ladder)
    for d in range(3):
        for row in range(height):
            part = weights_ref[d, :, row * lanes : (row + 1) * lanes] * ladder
            position_ref[d, row : row + 1, :] = jnp.sum(part, axis=0, keepdims=True)
    owner = owner_ref[...]
    element_code = element_ref[...] * receptors
    members = [owner == slab + shift for shift in range(-REACH, REACH + 1)]
    tall = slots * height
    marks = jnp.concatenate([jnp.where(m, 1.0, 0.0) for m in members], 0).astype(jnp.bfloat16)
    before = lax.broadcasted_iota(jnp.int32, (lanes, lanes), 0)
    after = lax.broadcasted_iota(jnp.int32, (lanes, lanes), 1)
    upper = jnp.where(before < after, 1.0, 0.0).astype(jnp.bfloat16)
    left = jnp.dot(marks, upper, preferred_element_type=jnp.float32).astype(jnp.bfloat16)
    above = lax.broadcasted_iota(jnp.int32, (tall, tall), 0)
    below = lax.broadcasted_iota(jnp.int32, (tall, tall), 1)
    same = above // height == below // height
    block = jnp.where(same, 1.0, 0.0).astype(jnp.bfloat16)
    lower = jnp.where(same & (below < above), 1.0, 0.0).astype(jnp.bfloat16)
    rank = jnp.dot(block, left, preferred_element_type=jnp.float32)
    rank = rank + jnp.dot(lower, marks, preferred_element_type=jnp.float32)
    rank = rank.astype(jnp.int32)
    ranks[...] = rank
    row_index = lax.broadcasted_iota(jnp.int32, (height, lanes), 0)
    place = lax.broadcasted_iota(jnp.int32, (height, lanes), 1) * height + row_index
    row_bits = height.bit_length() - 1
    steps = receptors.bit_length() - 1

    def pull(tile, step):
        if step >= row_bits:
            return pltpu.roll(tile, lanes - (1 << (step - row_bits)), 1)
        jump = 1 << step
        near = pltpu.roll(tile, height - jump, 0)
        far = pltpu.roll(near, lanes - 1, 1)
        return jnp.where(row_index < height - jump, near, far)

    words = []
    comps = []
    start = [position_ref[d] for d in range(3)]
    for slot in range(slots):
        shift = place - rank[slot * height : (slot + 1) * height]
        words.append(jnp.where(members[slot], element_code + shift, 0))
        comps.append(list(start))
    for step in range(steps):
        for slot in range(slots):
            word = words[slot]
            moving = word & (1 << step)
            came = pull(word, step)
            take = (came & (1 << step)) != 0
            words[slot] = jnp.where(take, came - (1 << step), jnp.where(moving != 0, 0, word))
            comps[slot] = [jnp.where(take, pull(c, step), c) for c in comps[slot]]
    half = lanes // 2
    left_half = lax.broadcasted_iota(jnp.int32, (room, lanes), 1) < half
    for slot in range(slots):
        columns = comps[slot] + [(words[slot] >> steps).astype(jnp.float32)]
        for at, column in enumerate(columns):
            request_ref[slot, at] = jnp.where(
                left_half, column[:room], pltpu.roll(column[room:], half, 1)
            )

    with jax.named_scope('w_barrier'):
        pl.semaphore_wait(barrier, greeted)

    def ask(shift):
        return pltpu.make_async_remote_copy(
            src_ref=request_ref.at[shift + REACH],
            dst_ref=asked.at[shift + REACH],
            send_sem=ask_sem.at[0],
            recv_sem=ask_sem.at[1 if shift == 0 else 2],
            device_id=(other, lax.rem(slab + shift + n, n)),
            device_id_type=MESH,
        )

    def reply(shift, part):
        span = pl.ds(0, 1) if part == 0 else pl.ds(1, fields - 1)
        return pltpu.make_async_remote_copy(
            src_ref=answer.at[shift + REACH, span],
            dst_ref=answered.at[shift + REACH, span],
            send_sem=reply_sem.at[0, part],
            recv_sem=reply_sem.at[1, part],
            device_id=(other, lax.rem(slab - shift + n, n)),
            device_id_type=MESH,
        )

    def asks(many, sem):
        return pltpu.make_async_remote_copy(
            src_ref=asked.at[pl.ds(0, many)],
            dst_ref=asked.at[pl.ds(0, many)],
            send_sem=ask_sem.at[0],
            recv_sem=ask_sem.at[sem],
            device_id=(other, slab),
            device_id_type=MESH,
        )

    def replies(many, part):
        span = pl.ds(0, 1) if part == 0 else pl.ds(1, fields - 1)
        return pltpu.make_async_remote_copy(
            src_ref=answered.at[pl.ds(0, many), span],
            dst_ref=answered.at[pl.ds(0, many), span],
            send_sem=reply_sem.at[0, part],
            recv_sem=reply_sem.at[1, part],
            device_id=(other, slab),
            device_id_type=MESH,
        )

    partners = 0
    for shift in range(-REACH, REACH + 1):
        partners = partners + jnp.where(inside(slab + shift), 1, 0)

    def with_partners(action):
        for many in range(REACH + 1, slots + 1):

            @pl.when(partners == many)
            def _():
                action(many)

    def face_copy(phase, up):
        step = 1 if up else n - 1
        return pltpu.make_async_remote_copy(
            src_ref=faces.at[phase, 1 if up else 0],
            dst_ref=halo.at[phase, 0 if up else 1],
            send_sem=face_send.at[1 if up else 0],
            recv_sem=face_recv.at[phase % 2, 0 if up else 1],
            device_id=(mesh_id, lax.rem(slab + step, n)),
            device_id_type=MESH,
        )

    def send_faces(phase):
        @pl.when(slab < n - 1)
        def _():
            face_copy(phase, True).start()

        @pl.when(slab > 0)
        def _():
            face_copy(phase, False).start()

    def wait_faces(phase):
        @pl.when(slab > 0)
        def _():
            face_copy(phase, True).wait_recv()

        @pl.when(slab < n - 1)
        def _():
            face_copy(phase, False).wait_recv()

        @pl.when(slab < n - 1)
        def _():
            face_copy(phase, True).wait_send()

        @pl.when(slab > 0)
        def _():
            face_copy(phase, False).wait_send()

    def dot_copy(step):
        return pltpu.make_async_remote_copy(
            src_ref=dots,
            dst_ref=all_dots.at[slab],
            send_sem=dot_sem.at[0],
            recv_sem=dot_sem.at[1],
            device_id=(mesh_id, lax.rem(slab + step, n)),
            device_id_type=MESH,
        )

    def all_dot_copies():
        return pltpu.make_async_remote_copy(
            src_ref=all_dots.at[pl.ds(0, n - 1)],
            dst_ref=all_dots.at[pl.ds(0, n - 1)],
            send_sem=dot_sem.at[0],
            recv_sem=dot_sem.at[1],
            device_id=(mesh_id, lax.rem(slab + 1, n)),
            device_id_type=MESH,
        )

    rim_jumps = (1, -1, 2, -2)
    rim_sends = [inside(slab + jump) for jump in rim_jumps]
    rim_comes = [inside(slab - jump) for jump in rim_jumps]
    near = (slab > 0, slab < n - 1)

    def rim_copy(at):
        return pltpu.make_async_remote_copy(
            src_ref=rim.at[1 - at % 2],
            dst_ref=rim_halo.at[at],
            send_sem=rim_sem.at[0],
            recv_sem=rim_sem.at[1],
            device_id=(mesh_id, lax.rem(slab + rim_jumps[at] + n, n)),
            device_id_type=MESH,
        )

    def rims(many):
        return pltpu.make_async_remote_copy(
            src_ref=rim_halo.at[pl.ds(0, many)],
            dst_ref=rim_halo.at[pl.ds(0, many)],
            send_sem=rim_sem.at[0],
            recv_sem=rim_sem.at[1],
            device_id=(mesh_id, lax.rem(slab + 1, n)),
            device_id_type=MESH,
        )

    def geometry_copy(up):
        side = 0 if up else 1
        return pltpu.make_async_remote_copy(
            src_ref=packet,
            dst_ref=geometry_halo.at[side],
            send_sem=geometry_send.at[side],
            recv_sem=geometry_recv.at[side],
            device_id=(mesh_id, lax.rem(slab + (1 if up else n - 1), n)),
            device_id_type=MESH,
        )

    stores = [
        pltpu.make_async_copy(source, target, store_sem.at[at])
        for at, (source, target) in enumerate(
            ((interface_ref, interface_hbm), (velocity, velocity_hbm), (rho, residual_hbm))
        )
    ]

    for distance in range(REACH + 1):
        for shift in sorted({distance, -distance}):

            @pl.when(inside(slab + shift))
            def _():
                ask(shift).start()

    phases = halo.shape[0]
    blank = jnp.zeros(halo.shape[2:], jnp.float32)

    for shift in range(-REACH, REACH + 1):

        @pl.when(jnp.logical_not(inside(slab + shift)))
        def _():
            answered[shift + REACH] = jnp.zeros(answered.shape[1:], jnp.float32)

        @pl.when(jnp.logical_not(inside(slab - shift)))
        def _():
            asked[shift + REACH] = jnp.zeros(asked.shape[1:], jnp.float32)

    for at in range(4):

        @pl.when(jnp.logical_not(rim_comes[at]))
        def _():
            rim_halo[at] = jnp.zeros(rim_halo.shape[1:], jnp.float32)

    for side in range(2):

        @pl.when(jnp.logical_not(near[side]))
        def _():
            geometry_halo[side] = jnp.zeros(geometry_halo.shape[1:], jnp.float32)

    @pl.when(slab == 0)
    def _():
        for phase in range(phases):
            halo[phase, 0] = blank

    @pl.when(slab == n - 1)
    def _():
        for phase in range(phases):
            halo[phase, 1] = blank

    node = lax.broadcasted_iota(jnp.int32, (8, elems), 0)
    element = lax.broadcasted_iota(jnp.int32, (8, elems), 1)
    x_index = element % EX
    y_index = element // EX % EY

    across = jnp.zeros((8, elems), jnp.float32)
    for a in range(8):
        across = jnp.where(node == a, float(quad[a]), across)
    for j in range(8):
        plane_ref[j] = across * float(quad[j])
        for m in range(8):
            along_y_ref[m, j] = jnp.full((8, elems), float(stiff[j, m]), jnp.float32)
    for step in range(8):
        turned = jnp.zeros((8, elems), jnp.float32)
        for i in range(8):
            turned = jnp.where(node == i, float(stiff[i, (i - step) % 8]), turned)
        along_x_ref[step] = turned

    def flag(condition):
        return jnp.where(condition, 1.0, 0.0)

    x_low = flag((node == 0) & (x_index > 0))
    x_high = flag((node == 7) & (x_index < EX - 1))
    y_low = flag(y_index > 0)
    y_high = flag(y_index < EY - 1)

    def plane_sum(tile):
        below = pltpu.roll(pltpu.roll(tile, 1, 1), 1, 2)
        above = pltpu.roll(pltpu.roll(tile, 7, 1), elems - 1, 2)
        tile = tile + below * x_low + above * x_high
        low = tile[0] + y_low * pltpu.roll(tile[7], EX, 1)
        high = tile[7] + y_high * pltpu.roll(tile[0], elems - EX, 1)
        return jnp.concatenate([low[None], tile[1:7], high[None]], 0)

    def weights(layer):
        return plane_ref[...] * float(quad[layer])

    loads[4].wait()
    loads[5].wait()

    wall_rows = []
    for side in range(2):
        wall_row = jnp.zeros((1, elems), jnp.float32)
        for x in range(EX):
            bit = wall_ref[side : side + 1, x : x + 1].astype(jnp.float32)
            wall_row = jnp.where(x_index[0:1] == x, bit, wall_row)
        wall_rows.append(wall_row)
    g_x, g_y, g_z, g_m = [geometry_ref[d : d + 1, :] for d in range(4)]

    packet[...] = jnp.concatenate(
        [geometry_ref[...]] + wall_rows + [jnp.zeros((2, elems), jnp.float32)], 0
    )

    @pl.when(near[1])
    def _():
        geometry_copy(True).start()

    @pl.when(near[0])
    def _():
        geometry_copy(False).start()

    diag_y = [jnp.full((8, elems), float(stiff[j, j]), jnp.float32)[None] for j in range(8)]
    diag_y = jnp.concatenate(diag_y, 0)

    def diagonal(along, layer):
        total = along[0] * along_x_ref[0] + along[1] * diag_y
        total = total + (along[2] * float(stiff[layer, layer]) + along[3])
        return plane_sum(weights(layer) * total)

    nothing = jnp.zeros((6, 8, elems), jnp.float32)

    def wall_marks(rows):
        low_wall = flag(y_index == 0) * rows[0]
        high_wall = flag(y_index == EY - 1) * rows[1]
        return plane_sum(jnp.concatenate([low_wall[None], nothing, high_wall[None]], 0))

    wall_plane = wall_marks(wall_rows)
    x_count = 1.0 + x_low + x_high
    y_count_low = 1.0 + y_low
    y_count_high = 1.0 + y_high
    plane_count = jnp.concatenate(
        [(x_count * y_count_low)[None]]
        + [x_count[None]] * 6
        + [(x_count * y_count_high)[None]],
        0,
    )
    mark = flag((node == 0) & (x_index == 0)) + flag((node == 7) & (x_index == EX - 1))

    def settle(layer, z_count, walls, diag):
        count = plane_count * z_count
        open_part = 1.0 - jnp.minimum(mark * count + walls, 1.0)
        sharing[layer] = 1.0 / count
        free[layer] = open_part
        inverse[layer] = open_part / diag

    for layer in range(1, 7):
        settle(layer, 1.0, wall_plane, diagonal((g_x, g_y, g_z, g_m), layer))
    z_counts = (jnp.where(slab > 0, 2.0, 1.0), jnp.where(slab < n - 1, 2.0, 1.0))
    for side, layer in ((0, 0), (1, 7)):
        sharing[layer] = 1.0 / (plane_count * z_counts[side])

    with jax.named_scope('w_donor'):
        loads[3].wait()
    donors = donor_ref[...].reshape(fields * 512, elems)
    coarse = donors.astype(jnp.bfloat16)
    split[:, :elems] = coarse
    split[:, elems:] = (donors - coarse.astype(jnp.float32)).astype(jnp.bfloat16)

    code = lax.broadcasted_iota(jnp.int32, (elems, CHUNK), 0)
    code = code.astype(jnp.float32)
    basis = lax.broadcasted_iota(jnp.int32, (8, CHUNK), 0)
    norms = [
        float(1.0 / np.prod([points[a] - points[b] for b in range(8) if b != a])) for a in range(8)
    ]
    scale = jnp.zeros((8, CHUNK), jnp.float32)
    for a in range(8):
        scale = jnp.where(basis == a, norms[a], scale)

    def lagrange(position):
        value = scale
        for b in range(8):
            value = value * jnp.where(basis == b, 1.0, position - float(points[b]))
        return value

    def evaluate(shift, first, last):
        group = CHUNK // lanes
        for chunk in range(room // group):
            block = [
                jnp.concatenate(
                    [
                        asked[shift + REACH, c, chunk * group + t : chunk * group + t + 1, :]
                        for t in range(group)
                    ],
                    1,
                )
                for c in range(4)
            ]
            chosen = jnp.where(block[3] == code, 1.0, 0.0).astype(jnp.bfloat16)
            chosen = jnp.concatenate([chosen, chosen], 0)
            w_x, w_y, w_z = [lagrange(block[d]) for d in range(3)]
            picked = jnp.dot(
                split[first * 512 : last * 512], chosen, preferred_element_type=jnp.float32
            )
            for field in range(first, last):
                cube = picked[(field - first) * 512 : (field - first + 1) * 512]
                cube = cube.reshape(8, 64, CHUNK)
                total = cube[0] * w_z[0:1, :]
                for k in range(1, 8):
                    total = total + cube[k] * w_z[k : k + 1, :]
                total = total.reshape(8, 8, CHUNK)
                line = total[0] * w_y[0:1, :]
                for j in range(1, 8):
                    line = line + total[j] * w_y[j : j + 1, :]
                value = jnp.sum(line * w_x, axis=0, keepdims=True)
                for t in range(group):
                    row = chunk * group + t
                    answer[shift + REACH, field, row : row + 1, :] = value[
                        :, t * lanes : (t + 1) * lanes
                    ]

    near_first = [0] + [sign * reach for reach in range(1, REACH + 1) for sign in (1, -1)]
    with jax.named_scope('w_ask'):
        asks(1, 1).wait_recv()
    evaluate(0, 0, 1)
    reply(0, 0).start()
    with jax.named_scope('w_ask'):
        with_partners(lambda many: asks(many - 1, 2).wait_recv())
    for shift in near_first[1:]:
        evaluate(shift, 0, 1)
    for shift in near_first[1:]:

        @pl.when(inside(slab - shift))
        def _():
            reply(shift, 0).start()

    turns_left = list(range(slots))

    def serve_rest(many):
        for _ in range(many):
            shift = near_first[turns_left.pop(0)]

            @pl.when(inside(slab - shift))
            def _():
                with jax.named_scope('rest'):
                    evaluate(shift, 1, fields)
                reply(shift, 1).start()

    room_index = lax.broadcasted_iota(jnp.int32, (room, lanes), 0)
    plans = []
    for slot in range(slots):
        table = ranks[slot * height : (slot + 1) * height, :]
        base = jnp.broadcast_to(table[0:1], (room, lanes))
        first = jnp.minimum(base >> row_bits, half - 1)
        second = jnp.minimum(first + 1, half - 1)
        offset = base & (height - 1)
        spots = table & (height - 1)
        plans.append((first, second, offset, spots))

    serve_rest(2)
    with jax.named_scope('w_reply'):
        with_partners(lambda many: replies(many, 0).wait_recv())

    def along_lanes(tile, index):
        return jnp.take_along_axis(tile, index, axis=1, mode="promise_in_bounds")

    def along_rows(tile, index):
        return jnp.take_along_axis(tile, index, axis=0, mode="promise_in_bounds")

    def gather_field(field):
        result = [jnp.zeros((room, lanes), jnp.float32)] * 2
        for slot in range(slots):
            packed = answered[slot, field]
            first, second, offset, spots = plans[slot]
            windows = [
                jnp.where(
                    room_index + part * room >= offset,
                    along_lanes(packed, first + part * half),
                    along_lanes(packed, second + part * half),
                )
                for part in range(2)
            ]
            for part in range(2):
                spot = spots[part * room : (part + 1) * room]
                member = members[slot][part * room : (part + 1) * room]
                low, high = [along_rows(window, spot & (room - 1)) for window in windows]
                tile = jnp.where(spot < room, low, high)
                result[part] = jnp.where(member, tile, result[part])
        return jnp.concatenate(result, 0)

    values = [gather_field(0)]
    groups = lanes // 64
    rows = jnp.concatenate([values[0][:, t * 64 : (t + 1) * 64] for t in range(groups)], 0)
    per_side = height // 2
    row = lax.broadcasted_iota(jnp.int32, (groups * height, elems), 0)
    spot = lax.broadcasted_iota(jnp.int32, (groups * height, elems), 1)
    piece = row % height
    target = (groups * (piece % per_side) + row // height) * EX + (EX - 1) * (piece // per_side)
    placed = lax.dot_general(
        rows,
        flag(spot == target),
        (((0,), (0,)), ((), ())),
        precision=lax.Precision.HIGHEST,
        preferred_element_type=jnp.float32,
    ).reshape(8, 8, elems)
    rim[0] = placed[0]
    rim[1] = placed[7]
    for at in range(4):

        @pl.when(rim_sends[at])
        def _():
            rim_copy(at).start()

    def spread_out(column):
        return plane_sum(
            jnp.concatenate(
                [
                    (jnp.broadcast_to(column[j : j + 1, :], (8, elems)) * mark)[None]
                    for j in range(8)
                ],
                0,
            )
        )

    def in_plane(tile, along):
        along_y = along_y_ref[0] * tile[0:1]
        for j in range(1, 8):
            along_y = along_y + along_y_ref[j] * tile[j : j + 1]
        along_x = along_x_ref[0] * tile
        for step in range(1, 8):
            along_x = along_x + along_x_ref[step] * pltpu.roll(tile, step, 1)
        return along[0] * along_x + along[1] * along_y

    def inner_z(read, layer):
        total = read(1) * float(stiff[layer, 1])
        for k in range(2, 7):
            total = total + read(k) * float(stiff[layer, k])
        return total

    def outer_z(low, high, layer):
        return low * float(stiff[layer, 0]) + high * float(stiff[layer, 7])

    here = (g_x, g_y, g_z, g_m)
    edge = weights(0)

    for layer in ORDER:
        boundary[layer] = spread_out(placed[layer]) * sharing[layer]
    loads[6].wait()
    for layer in ORDER:
        along_z = inner_z(lambda k: boundary[k], layer)
        along_z = along_z + outer_z(boundary[0], boundary[7], layer)
        tile = boundary[layer]
        total = in_plane(tile, here) + g_z * along_z + g_m * (tile - forcing_ref[layer])
        total = weights(layer) * total
        if layer in (0, 7):
            total = plane_sum(total)
        residual[layer] = total
        if layer == 7:
            faces[0, 0] = residual[0]
            faces[0, 1] = residual[7]
            send_faces(0)

    beyond = []
    for side in range(2):

        @pl.when(near[side])
        def _():
            geometry_copy(side == 0).wait_recv()

        along = [geometry_halo[side, d : d + 1, :] for d in range(4)]
        own = boundary[0 if side == 0 else 7]
        term = in_plane(own, along)
        term = term + (along[2] * float(stiff[0, 0]) + along[3]) * own
        beyond.append((term, along[2] * float(stiff[0, 7])))
        walls = wall_plane + wall_marks([geometry_halo[side, 4:5, :], geometry_halo[side, 5:6, :]])
        layer, facing = (0, 7) if side == 0 else (7, 0)
        settle(layer, z_counts[side], walls, diagonal(here, layer) + diagonal(along, facing))
    serve_rest(1)

    with jax.named_scope('w_rim'):
        with_partners(lambda many: rims(many - 1).wait_recv())

    low = spread_out(rim_halo[0]) * sharing[0]
    high = spread_out(rim_halo[1]) * sharing[7]
    boundary[0] = boundary[0] + low
    boundary[7] = boundary[7] + high
    for layer in range(1, 7):
        more = weights(layer) * (g_z * outer_z(low, high, layer))
        residual[layer] = -free[layer] * plane_sum(residual[layer] + more)
        rho[layer] = residual[layer]
        vectors[0, layer] = inverse[layer] * residual[layer]
    half_share = 0.5 / plane_count
    ends = []
    for side, (own, layer) in enumerate(((low, 0), (high, 7))):
        more = in_plane(own, here) + g_m * own + g_z * outer_z(low, high, layer)
        term, across_z = beyond[side]
        more = more + term + across_z * (spread_out(rim_halo[2 + side]) * half_share)
        ends.append(residual[layer] + plane_sum(edge * more))

    def prepare(turn):
        def read(k):
            return vectors[turn, k]

        for layer in range(1, 7):
            tile = vectors[turn, layer]
            partial[layer] = (
                in_plane(tile, here) + g_m * tile + g_z * inner_z(read, layer)
            )
        for layer in (0, 7):
            partial[layer] = g_z * inner_z(read, layer)

    prepare(0)
    with jax.named_scope('w_f2'):
        wait_faces(0)
    for side, layer in ((0, 0), (1, 7)):
        residual[layer] = -free[layer] * (ends[side] + halo[0, side])
        rho[layer] = residual[layer]
        vectors[0, layer] = inverse[layer] * residual[layer]

    sums = {}

    def gather_sum(key, value):
        value = jnp.sum(value, axis=0)
        sums[key] = value if key not in sums else sums[key] + value

    for turn in range(ITERS):
        phase = 1 + turn
        low = vectors[turn, 0]
        high = vectors[turn, 7]
        outer = {}
        for layer in (0, 7):
            tile = vectors[turn, layer]
            total = in_plane(tile, here) + g_m * tile + g_z * outer_z(low, high, layer)
            outer[layer] = edge * (total + partial[layer])
            images[turn, layer] = plane_sum(outer[layer])
        faces[phase, 0] = images[turn, 0]
        faces[phase, 1] = images[turn, 7]
        send_faces(phase)
        last = turn == ITERS - 1
        for layer in range(8):
            if layer in outer:
                tile = outer[layer]
            else:
                tile = partial[layer] + g_z * outer_z(low, high, layer)
                tile = weights(layer) * tile
            for other_turn in range(turn + 1):
                gather_sum((other_turn, turn), tile * vectors[other_turn, layer])
            gather_sum(
                turn, vectors[turn, layer] * residual[layer] * sharing[layer]
            )
            if layer not in outer:
                images[turn, layer] = tile if last else free[layer] * plane_sum(tile)
        if last:
            break
        for layer in range(1, 7):
            rho[layer] = images[turn, layer] - SHIFTS[turn] * rho[layer]
            vectors[turn + 1, layer] = inverse[layer] * rho[layer]
        prepare(turn + 1)
        serve_rest(WINDOWS[turn])
        with jax.named_scope('w_fc'):
            wait_faces(phase)
        for side, layer in ((0, 0), (1, 7)):
            images[turn, layer] = free[layer] * (images[turn, layer] + halo[phase, side])
            rho[layer] = images[turn, layer] - SHIFTS[turn] * rho[layer]
            vectors[turn + 1, layer] = inverse[layer] * rho[layer]

    keys = list(range(ITERS)) + [(a, b) for b in range(ITERS) for a in range(b + 1)]
    spot = lax.broadcasted_iota(jnp.int32, (1, 128), 1)
    packed = jnp.zeros((1, 128), jnp.float32)
    for at, key in enumerate(keys):
        value = jnp.sum(jnp.sum(sums[key], axis=0, keepdims=True), axis=1, keepdims=True)
        packed = jnp.where(spot == at, value, packed)
    dots[...] = packed
    for step in range(1, n):
        dot_copy(step).start()
    all_dots[slab] = dots[...]
    with jax.named_scope('w_rest'):
        with_partners(lambda many: replies(many, 1).wait_recv())

    values = values + [gather_field(field) for field in range(1, fields)]
    for row in range(height):
        interface_ref[:, row * lanes : (row + 1) * lanes] = jnp.concatenate(
            [value[row : row + 1] for value in values], 0
        )
    stores[0].start()
    for layer in range(1, 7):
        images[ITERS - 1, layer] = free[layer] * plane_sum(images[ITERS - 1, layer])
    with jax.named_scope('w_fc'):
        wait_faces(ITERS)
    for side, layer in ((0, 0), (1, 7)):
        images[ITERS - 1, layer] = free[layer] * (
            images[ITERS - 1, layer] + halo[ITERS, side]
        )
    with jax.named_scope('w_dots'):
        all_dot_copies().wait_recv()
    with jax.named_scope('solve'):
        total = jnp.sum(all_dots[...], axis=0)
        found = {
            key: jnp.broadcast_to(total[:, at : at + 1], (8, elems))
            for at, key in enumerate(keys)
        }
        steps_taken = solve(found)
    for layer in range(8):
        moved = boundary[layer]
        for turn in range(ITERS):
            moved = moved + steps_taken[turn] * vectors[turn, layer]
        velocity[layer] = moved
    stores[1].start()
    for layer in range(8):
        left_over = residual[layer]
        for turn in range(ITERS):
            left_over = left_over - steps_taken[turn] * images[turn, layer]
        rho[layer] = left_over
    stores[2].start()
    all_dot_copies().wait_send()
    for side in range(2):

        @pl.when(near[1 - side])
        def _():
            geometry_copy(side == 0).wait_send()

    with_partners(lambda many: rims(many - 1).wait_send())
    with_partners(lambda many: asks(many, 1).wait_send())
    for part in range(2):
        with_partners(lambda many: replies(many, part).wait_send())

    with jax.named_scope('w_store'):
        for store in stores:
            store.wait()


def flush(*refs):
    count = (len(refs) - 1) // 2
    sem = refs[-1]
    copies = [
        pltpu.make_async_copy(refs[at], refs[count + at], sem.at[at]) for at in range(count)
    ]
    for copy in copies:
        copy.start()
    for copy in copies:
        copy.wait()


def body(n, donor_fields, interp_weights, donor_owner, donor_element, geometry, wall_flag, forcing):
    fields = donor_fields.shape[0]
    elems = geometry.shape[1]
    receptors = donor_element.shape[0]
    slots = 2 * REACH + 1
    lanes = 128
    count = receptors // lanes
    cube = (8, 8, 8, elems)
    phases = 1 + ITERS
    room = count // 2
    vmem = pl.BlockSpec(memory_space=pltpu.VMEM)
    hbm = pl.BlockSpec(memory_space=pltpu.HBM)
    shapes = (
        jax.ShapeDtypeStruct(cube, jnp.float32),
        jax.ShapeDtypeStruct(cube, jnp.float32),
        jax.ShapeDtypeStruct((fields, receptors), jnp.float32),
    )
    outputs = pl.pallas_call(
        functools.partial(kernel, n),
        out_shape=shapes,
        in_specs=[hbm] * 7,
        out_specs=(hbm, hbm, hbm),
        scratch_shapes=[
            pltpu.VMEM(cube, jnp.float32),
            pltpu.VMEM(cube, jnp.float32),
            pltpu.VMEM((fields, receptors), jnp.float32),
            pltpu.VMEM((fields, 512, elems), jnp.float32),
            pltpu.VMEM(cube, jnp.float32),
            pltpu.VMEM(interp_weights.shape, jnp.float32),
            pltpu.VMEM((count, lanes), jnp.int32),
            pltpu.VMEM((count, lanes), jnp.int32),
            pltpu.VMEM(geometry.shape, jnp.float32),
            pltpu.VMEM(wall_flag.shape, jnp.int32),
            pltpu.VMEM((3, count, lanes), jnp.float32),
            pltpu.VMEM((slots, 4, room, lanes), jnp.float32),
            pltpu.VMEM((slots * count, lanes), jnp.int32),
            pltpu.VMEM(cube, jnp.float32),
            pltpu.VMEM((8, 8, elems), jnp.float32),
            pltpu.VMEM((8, 8, elems), jnp.float32),
            pltpu.SemaphoreType.DMA((7,)),
            pltpu.VMEM((fields * 512, 2 * elems), jnp.bfloat16),
            pltpu.VMEM((slots, 4, room, lanes), jnp.float32),
            pltpu.VMEM((slots, fields, room, lanes), jnp.float32),
            pltpu.VMEM((slots, fields, room, lanes), jnp.float32),
            pltpu.VMEM((phases, 2, 8, 8, elems), jnp.float32),
            pltpu.VMEM((phases, 2, 8, 8, elems), jnp.float32),
            pltpu.VMEM((1, 128), jnp.float32),
            pltpu.VMEM((n, 1, 128), jnp.float32),
            pltpu.VMEM((ITERS,) + cube, jnp.float32),
            pltpu.VMEM((ITERS,) + cube, jnp.float32),
            pltpu.VMEM(cube, jnp.float32),
            pltpu.VMEM(cube, jnp.float32),
            pltpu.VMEM((2, 8, elems), jnp.float32),
            pltpu.VMEM((4, 8, elems), jnp.float32),
            pltpu.VMEM((2, 8, elems), jnp.float32),
            pltpu.VMEM((8, elems), jnp.float32),
        ]
        + [pltpu.VMEM(cube, jnp.float32)] * 4
        + [pltpu.SemaphoreType.DMA((3,)), pltpu.SemaphoreType.DMA((2, 2))]
        + [pltpu.SemaphoreType.DMA((2,)), pltpu.SemaphoreType.DMA((2, 2))]
        + [pltpu.SemaphoreType.DMA((2,))]
        + [pltpu.SemaphoreType.DMA((2,))]
        + [pltpu.SemaphoreType.DMA((2,))] * 2
        + [pltpu.SemaphoreType.DMA((3,))],
        compiler_params=pltpu.CompilerParams(
            collective_id=0, has_side_effects=True, vmem_limit_bytes=67043328
        ),
    )(
        donor_fields,
        interp_weights,
        donor_owner.reshape(count, lanes),
        donor_element.reshape(count, lanes),
        geometry,
        wall_flag,
        forcing.reshape(cube),
    )
    velocity, residual, interface = pl.pallas_call(
        flush,
        out_shape=shapes,
        in_specs=[vmem] * 3,
        out_specs=(hbm,) * 3,
        scratch_shapes=[pltpu.SemaphoreType.DMA((3,))],
    )(*outputs)
    return (velocity.reshape(512, elems), residual.reshape(512, elems), interface)


def solution(mesh):
    in_specs = (
        P(None, None, ("mesh", "dom")),
        P(None, None, ("mesh", "dom")),
        P(("mesh", "dom"), None),
        P(("mesh", "dom")),
        P(None, ("mesh", "dom")),
        P(None, ("mesh", "dom")),
        P(None, ("mesh", "dom")),
    )
    out_specs = (P(None, ("mesh", "dom")), P(None, ("mesh", "dom")), P(None, ("mesh", "dom")))
    return jax.shard_map(
        functools.partial(body, mesh.shape["dom"]),
        mesh=mesh,
        in_specs=in_specs,
        out_specs=out_specs,
        check_vma=False,
    )
```

```python
import functools

import jax
import jax.numpy as jnp
import numpy as np
from jax import lax
from jax.experimental import pallas as pl
from jax.experimental.pallas import tpu as pltpu
from jax.sharding import PartitionSpec as P

EX = 8
EY = 16
ITERS = 3
REACH = 2
CHUNK = 256
ORDER = (0, 7, 1, 2, 3, 4, 5, 6)
SHIFTS = (1.5, 0.5)
WINDOWS = (1, 1)
MESH = pl.DeviceIdType.MESH


def legendre_pair(values, degree):
    previous = values * 0.0 + 1.0
    current = values * 1.0
    for poly_order in range(2, degree + 1):
        previous, current = (
            current,
            ((2 * poly_order - 1) * values * current - (poly_order - 1) * previous) / poly_order,
        )
    return (current, previous)


def gll_tables():
    degree = 7
    points_count = degree + 1
    abscissae = np.cos(np.pi * np.arange(points_count) / degree)
    for newton_turn in range(80):
        top_poly, lower_poly = legendre_pair(abscissae, degree)
        abscissae = abscissae - (abscissae * top_poly - lower_poly) / (points_count * top_poly)
    abscissae = np.sort(abscissae)
    top_poly, lower_poly = legendre_pair(abscissae, degree)
    quad_weights = 2.0 / (degree * points_count * top_poly * top_poly)
    identity_mat = np.eye(points_count)
    spacing = abscissae[:, None] - abscissae[None, :] + identity_mat
    derivative = top_poly[:, None] / (top_poly[None, :] * spacing) * (1.0 - identity_mat)
    derivative[0, 0] = -degree * points_count / 4.0
    derivative[degree, degree] = degree * points_count / 4.0
    return (abscissae, derivative, quad_weights)


def solve(found):
    matrix = [
        [found[(min(a, b), max(a, b))] for b in range(ITERS)] for a in range(ITERS)
    ]
    right = [found[a] for a in range(ITERS)]
    pivots = []
    for a in range(ITERS):
        pivots.append(1.0 / matrix[a][a])
        for b in range(a + 1, ITERS):
            factor = matrix[b][a] * pivots[a]
            for c in range(a + 1, ITERS):
                matrix[b][c] = matrix[b][c] - factor * matrix[a][c]
            right[b] = right[b] - factor * right[a]
    answer = [None] * ITERS
    for a in reversed(range(ITERS)):
        total = right[a]
        for b in range(a + 1, ITERS):
            total = total - matrix[a][b] * answer[b]
        answer[a] = total * pivots[a]
    return answer


def kernel(
    n,
    donor_hbm,
    weights_hbm,
    owner_hbm,
    element_hbm,
    geometry_hbm,
    wall_hbm,
    forcing_hbm,
    velocity,
    residual_out,
    interface_ref,
    residual,
    donor_ref,
    forcing_ref,
    weights_ref,
    owner_ref,
    element_ref,
    geometry_ref,
    wall_ref,
    position_ref,
    request_ref,
    ranks,
    along_y_ref,
    along_x_ref,
    plane_ref,
    load_sem,
    split,
    asked,
    answer,
    answered,
    faces,
    halo,
    dots,
    all_dots,
    vectors,
    images,
    partial,
    rho,
    rim,
    rim_halo,
    geometry_halo,
    packet,
    inverse,
    free,
    sharing,
    boundary,
    ask_sem,
    reply_sem,
    face_send,
    face_recv,
    dot_sem,
    rim_sem,
    geometry_send,
    geometry_recv,
):
    points, derivative, quad = gll_tables()
    stiff = (derivative.T * quad) @ derivative / quad[:, None]
    fields = donor_ref.shape[0]
    elems = donor_ref.shape[2]
    height = owner_ref.shape[0]
    lanes = owner_ref.shape[1]
    receptors = height * lanes
    room = request_ref.shape[2]
    slots = 2 * REACH + 1
    mesh_id = lax.axis_index("mesh")
    slab = lax.axis_index("dom")
    other = 1 - mesh_id

    pairs = [
        (weights_hbm, weights_ref),
        (owner_hbm, owner_ref),
        (element_hbm, element_ref),
        (donor_hbm, donor_ref),
        (geometry_hbm, geometry_ref),
        (wall_hbm, wall_ref),
        (forcing_hbm, forcing_ref),
    ]
    loads = [
        pltpu.make_async_copy(source, target, load_sem.at[at])
        for at, (source, target) in enumerate(pairs)
    ]
    for load in loads:
        load.start()

    def inside(index):
        return jnp.logical_and(index >= 0, index < n)

    barrier = pltpu.get_barrier_semaphore()
    greeted = n - 1
    for step in range(1, n):
        pl.semaphore_signal(
            barrier, inc=1, device_id=(mesh_id, lax.rem(slab + step, n)), device_id_type=MESH
        )
    for shift in range(-REACH, REACH + 1):
        greeted = greeted + jnp.where(inside(slab + shift), 1, 0)

        @pl.when(inside(slab + shift))
        def _():
            pl.semaphore_signal(
                barrier, inc=1, device_id=(other, slab + shift), device_id_type=MESH
            )

    with jax.named_scope('w_loads'):
        for load in loads[:3]:
            load.wait()
    depth = lax.broadcasted_iota(jnp.int32, (8, lanes), 0)
    ladder = jnp.zeros((8, lanes), jnp.float32)
    for a in range(8):
        ladder = jnp.where(depth == a, float(points[a]), ladder)
    for d in range(3):
        for row in range(height):
            part = weights_ref[d, :, row * lanes : (row + 1) * lanes] * ladder
            position_ref[d, row : row + 1, :] = jnp.sum(part, axis=0, keepdims=True)
    owner = owner_ref[...]
    element_code = element_ref[...] * receptors
    members = [owner == slab + shift for shift in range(-REACH, REACH + 1)]
    tall = slots * height
    marks = jnp.concatenate([jnp.where(m, 1.0, 0.0) for m in members], 0).astype(jnp.bfloat16)
    before = lax.broadcasted_iota(jnp.int32, (lanes, lanes), 0)
    after = lax.broadcasted_iota(jnp.int32, (lanes, lanes), 1)
    upper = jnp.where(before < after, 1.0, 0.0).astype(jnp.bfloat16)
    left = jnp.dot(marks, upper, preferred_element_type=jnp.float32).astype(jnp.bfloat16)
    above = lax.broadcasted_iota(jnp.int32, (tall, tall), 0)
    below = lax.broadcasted_iota(jnp.int32, (tall, tall), 1)
    same = above // height == below // height
    block = jnp.where(same, 1.0, 0.0).astype(jnp.bfloat16)
    lower = jnp.where(same & (below < above), 1.0, 0.0).astype(jnp.bfloat16)
    rank = jnp.dot(block, left, preferred_element_type=jnp.float32)
    rank = rank + jnp.dot(lower, marks, preferred_element_type=jnp.float32)
    rank = rank.astype(jnp.int32)
    ranks[...] = rank
    row_index = lax.broadcasted_iota(jnp.int32, (height, lanes), 0)
    place = lax.broadcasted_iota(jnp.int32, (height, lanes), 1) * height + row_index
    row_bits = height.bit_length() - 1
    steps = receptors.bit_length() - 1

    def pull(tile, step):
        if step >= row_bits:
            return pltpu.roll(tile, lanes - (1 << (step - row_bits)), 1)
        jump = 1 << step
        near = pltpu.roll(tile, height - jump, 0)
        far = pltpu.roll(near, lanes - 1, 1)
        return jnp.where(row_index < height - jump, near, far)

    words = []
    comps = []
    start = [position_ref[d] for d in range(3)]
    for slot in range(slots):
        shift = place - rank[slot * height : (slot + 1) * height]
        words.append(jnp.where(members[slot], element_code + shift, 0))
        comps.append(list(start))
    for step in range(steps):
        for slot in range(slots):
            word = words[slot]
            moving = word & (1 << step)
            came = pull(word, step)
            take = (came & (1 << step)) != 0
            words[slot] = jnp.where(take, came - (1 << step), jnp.where(moving != 0, 0, word))
            comps[slot] = [jnp.where(take, pull(c, step), c) for c in comps[slot]]
    half = lanes // 2
    left_half = lax.broadcasted_iota(jnp.int32, (room, lanes), 1) < half
    for slot in range(slots):
        columns = comps[slot] + [(words[slot] >> steps).astype(jnp.float32)]
        for at, column in enumerate(columns):
            request_ref[slot, at] = jnp.where(
                left_half, column[:room], pltpu.roll(column[room:], half, 1)
            )

    with jax.named_scope('w_barrier'):
        pl.semaphore_wait(barrier, greeted)

    def ask(shift):
        return pltpu.make_async_remote_copy(
            src_ref=request_ref.at[shift + REACH],
            dst_ref=asked.at[shift + REACH],
            send_sem=ask_sem.at[0],
            recv_sem=ask_sem.at[1 if shift == 0 else 2],
            device_id=(other, lax.rem(slab + shift + n, n)),
            device_id_type=MESH,
        )

    def reply(shift, part):
        span = pl.ds(0, 1) if part == 0 else pl.ds(1, fields - 1)
        return pltpu.make_async_remote_copy(
            src_ref=answer.at[shift + REACH, span],
            dst_ref=answered.at[shift + REACH, span],
            send_sem=reply_sem.at[0, part],
            recv_sem=reply_sem.at[1, part],
            device_id=(other, lax.rem(slab - shift + n, n)),
            device_id_type=MESH,
        )

    def asks(many, sem):
        return pltpu.make_async_remote_copy(
            src_ref=asked.at[pl.ds(0, many)],
            dst_ref=asked.at[pl.ds(0, many)],
            send_sem=ask_sem.at[0],
            recv_sem=ask_sem.at[sem],
            device_id=(other, slab),
            device_id_type=MESH,
        )

    def replies(many, part):
        span = pl.ds(0, 1) if part == 0 else pl.ds(1, fields - 1)
        return pltpu.make_async_remote_copy(
            src_ref=answered.at[pl.ds(0, many), span],
            dst_ref=answered.at[pl.ds(0, many), span],
            send_sem=reply_sem.at[0, part],
            recv_sem=reply_sem.at[1, part],
            device_id=(other, slab),
            device_id_type=MESH,
        )

    partners = 0
    for shift in range(-REACH, REACH + 1):
        partners = partners + jnp.where(inside(slab + shift), 1, 0)

    def with_partners(action):
        for many in range(REACH + 1, slots + 1):

            @pl.when(partners == many)
            def _():
                action(many)

    def face_copy(phase, up):
        step = 1 if up else n - 1
        return pltpu.make_async_remote_copy(
            src_ref=faces.at[phase, 1 if up else 0],
            dst_ref=halo.at[phase, 0 if up else 1],
            send_sem=face_send.at[1 if up else 0],
            recv_sem=face_recv.at[phase % 2, 0 if up else 1],
            device_id=(mesh_id, lax.rem(slab + step, n)),
            device_id_type=MESH,
        )

    def send_faces(phase):
        @pl.when(slab < n - 1)
        def _():
            face_copy(phase, True).start()

        @pl.when(slab > 0)
        def _():
            face_copy(phase, False).start()

    def wait_faces(phase):
        @pl.when(slab > 0)
        def _():
            face_copy(phase, True).wait_recv()

        @pl.when(slab < n - 1)
        def _():
            face_copy(phase, False).wait_recv()

        @pl.when(slab < n - 1)
        def _():
            face_copy(phase, True).wait_send()

        @pl.when(slab > 0)
        def _():
            face_copy(phase, False).wait_send()

    def dot_copy(step):
        return pltpu.make_async_remote_copy(
            src_ref=dots,
            dst_ref=all_dots.at[slab],
            send_sem=dot_sem.at[0],
            recv_sem=dot_sem.at[1],
            device_id=(mesh_id, lax.rem(slab + step, n)),
            device_id_type=MESH,
        )

    def all_dot_copies():
        return pltpu.make_async_remote_copy(
            src_ref=all_dots.at[pl.ds(0, n - 1)],
            dst_ref=all_dots.at[pl.ds(0, n - 1)],
            send_sem=dot_sem.at[0],
            recv_sem=dot_sem.at[1],
            device_id=(mesh_id, lax.rem(slab + 1, n)),
            device_id_type=MESH,
        )

    rim_jumps = (1, -1, 2, -2)
    rim_sends = [inside(slab + jump) for jump in rim_jumps]
    rim_comes = [inside(slab - jump) for jump in rim_jumps]
    near = (slab > 0, slab < n - 1)

    def rim_copy(at):
        return pltpu.make_async_remote_copy(
            src_ref=rim.at[1 - at % 2],
            dst_ref=rim_halo.at[at],
            send_sem=rim_sem.at[0],
            recv_sem=rim_sem.at[1],
            device_id=(mesh_id, lax.rem(slab + rim_jumps[at] + n, n)),
            device_id_type=MESH,
        )

    def rims(many):
        return pltpu.make_async_remote_copy(
            src_ref=rim_halo.at[pl.ds(0, many)],
            dst_ref=rim_halo.at[pl.ds(0, many)],
            send_sem=rim_sem.at[0],
            recv_sem=rim_sem.at[1],
            device_id=(mesh_id, lax.rem(slab + 1, n)),
            device_id_type=MESH,
        )

    def geometry_copy(up):
        side = 0 if up else 1
        return pltpu.make_async_remote_copy(
            src_ref=packet,
            dst_ref=geometry_halo.at[side],
            send_sem=geometry_send.at[side],
            recv_sem=geometry_recv.at[side],
            device_id=(mesh_id, lax.rem(slab + (1 if up else n - 1), n)),
            device_id_type=MESH,
        )

    for distance in range(REACH + 1):
        for shift in sorted({distance, -distance}):

            @pl.when(inside(slab + shift))
            def _():
                ask(shift).start()

    phases = halo.shape[0]
    blank = jnp.zeros(halo.shape[2:], jnp.float32)

    for shift in range(-REACH, REACH + 1):

        @pl.when(jnp.logical_not(inside(slab + shift)))
        def _():
            answered[shift + REACH] = jnp.zeros(answered.shape[1:], jnp.float32)

        @pl.when(jnp.logical_not(inside(slab - shift)))
        def _():
            asked[shift + REACH] = jnp.zeros(asked.shape[1:], jnp.float32)

    for at in range(4):

        @pl.when(jnp.logical_not(rim_comes[at]))
        def _():
            rim_halo[at] = jnp.zeros(rim_halo.shape[1:], jnp.float32)

    for side in range(2):

        @pl.when(jnp.logical_not(near[side]))
        def _():
            geometry_halo[side] = jnp.zeros(geometry_halo.shape[1:], jnp.float32)

    @pl.when(slab == 0)
    def _():
        for phase in range(phases):
            halo[phase, 0] = blank

    @pl.when(slab == n - 1)
    def _():
        for phase in range(phases):
            halo[phase, 1] = blank

    node = lax.broadcasted_iota(jnp.int32, (8, elems), 0)
    element = lax.broadcasted_iota(jnp.int32, (8, elems), 1)
    x_index = element % EX
    y_index = element // EX % EY

    across = jnp.zeros((8, elems), jnp.float32)
    for a in range(8):
        across = jnp.where(node == a, float(quad[a]), across)
    for j in range(8):
        plane_ref[j] = across * float(quad[j])
        for m in range(8):
            along_y_ref[m, j] = jnp.full((8, elems), float(stiff[j, m]), jnp.float32)
    for step in range(8):
        turned = jnp.zeros((8, elems), jnp.float32)
        for i in range(8):
            turned = jnp.where(node == i, float(stiff[i, (i - step) % 8]), turned)
        along_x_ref[step] = turned

    def flag(condition):
        return jnp.where(condition, 1.0, 0.0)

    x_low = flag((node == 0) & (x_index > 0))
    x_high = flag((node == 7) & (x_index < EX - 1))
    y_low = flag(y_index > 0)
    y_high = flag(y_index < EY - 1)

    def plane_sum(tile):
        below = pltpu.roll(pltpu.roll(tile, 1, 1), 1, 2)
        above = pltpu.roll(pltpu.roll(tile, 7, 1), elems - 1, 2)
        tile = tile + below * x_low + above * x_high
        low = tile[0] + y_low * pltpu.roll(tile[7], EX, 1)
        high = tile[7] + y_high * pltpu.roll(tile[0], elems - EX, 1)
        return jnp.concatenate([low[None], tile[1:7], high[None]], 0)

    def weights(layer):
        return plane_ref[...] * float(quad[layer])

    loads[4].wait()
    loads[5].wait()

    wall_rows = []
    for side in range(2):
        wall_row = jnp.zeros((1, elems), jnp.float32)
        for x in range(EX):
            bit = wall_ref[side : side + 1, x : x + 1].astype(jnp.float32)
            wall_row = jnp.where(x_index[0:1] == x, bit, wall_row)
        wall_rows.append(wall_row)
    g_x, g_y, g_z, g_m = [geometry_ref[d : d + 1, :] for d in range(4)]

    packet[...] = jnp.concatenate(
        [geometry_ref[...]] + wall_rows + [jnp.zeros((2, elems), jnp.float32)], 0
    )

    @pl.when(near[1])
    def _():
        geometry_copy(True).start()

    @pl.when(near[0])
    def _():
        geometry_copy(False).start()

    diag_y = [jnp.full((8, elems), float(stiff[j, j]), jnp.float32)[None] for j in range(8)]
    diag_y = jnp.concatenate(diag_y, 0)

    def diagonal(along, layer):
        total = along[0] * along_x_ref[0] + along[1] * diag_y
        total = total + (along[2] * float(stiff[layer, layer]) + along[3])
        return plane_sum(weights(layer) * total)

    nothing = jnp.zeros((6, 8, elems), jnp.float32)

    def wall_marks(rows):
        low_wall = flag(y_index == 0) * rows[0]
        high_wall = flag(y_index == EY - 1) * rows[1]
        return plane_sum(jnp.concatenate([low_wall[None], nothing, high_wall[None]], 0))

    wall_plane = wall_marks(wall_rows)
    x_count = 1.0 + x_low + x_high
    y_count_low = 1.0 + y_low
    y_count_high = 1.0 + y_high
    plane_count = jnp.concatenate(
        [(x_count * y_count_low)[None]]
        + [x_count[None]] * 6
        + [(x_count * y_count_high)[None]],
        0,
    )
    mark = flag((node == 0) & (x_index == 0)) + flag((node == 7) & (x_index == EX - 1))

    def settle(layer, z_count, walls, diag):
        count = plane_count * z_count
        open_part = 1.0 - jnp.minimum(mark * count + walls, 1.0)
        sharing[layer] = 1.0 / count
        free[layer] = open_part
        inverse[layer] = open_part / diag

    for layer in range(1, 7):
        settle(layer, 1.0, wall_plane, diagonal((g_x, g_y, g_z, g_m), layer))
    z_counts = (jnp.where(slab > 0, 2.0, 1.0), jnp.where(slab < n - 1, 2.0, 1.0))
    for side, layer in ((0, 0), (1, 7)):
        sharing[layer] = 1.0 / (plane_count * z_counts[side])

    with jax.named_scope('w_donor'):
        loads[3].wait()
    donors = donor_ref[...].reshape(fields * 512, elems)
    coarse = donors.astype(jnp.bfloat16)
    split[:, :elems] = coarse
    split[:, elems:] = (donors - coarse.astype(jnp.float32)).astype(jnp.bfloat16)

    code = lax.broadcasted_iota(jnp.int32, (elems, CHUNK), 0)
    code = code.astype(jnp.float32)
    basis = lax.broadcasted_iota(jnp.int32, (8, CHUNK), 0)
    norms = [
        float(1.0 / np.prod([points[a] - points[b] for b in range(8) if b != a])) for a in range(8)
    ]
    scale = jnp.zeros((8, CHUNK), jnp.float32)
    for a in range(8):
        scale = jnp.where(basis == a, norms[a], scale)

    def lagrange(position):
        value = scale
        for b in range(8):
            value = value * jnp.where(basis == b, 1.0, position - float(points[b]))
        return value

    def evaluate(shift, first, last):
        group = CHUNK // lanes
        for chunk in range(room // group):
            block = [
                jnp.concatenate(
                    [
                        asked[shift + REACH, c, chunk * group + t : chunk * group + t + 1, :]
                        for t in range(group)
                    ],
                    1,
                )
                for c in range(4)
            ]
            chosen = jnp.where(block[3] == code, 1.0, 0.0).astype(jnp.bfloat16)
            chosen = jnp.concatenate([chosen, chosen], 0)
            w_x, w_y, w_z = [lagrange(block[d]) for d in range(3)]
            picked = jnp.dot(
                split[first * 512 : last * 512], chosen, preferred_element_type=jnp.float32
            )
            for field in range(first, last):
                cube = picked[(field - first) * 512 : (field - first + 1) * 512]
                cube = cube.reshape(8, 64, CHUNK)
                total = cube[0] * w_z[0:1, :]
                for k in range(1, 8):
                    total = total + cube[k] * w_z[k : k + 1, :]
                total = total.reshape(8, 8, CHUNK)
                line = total[0] * w_y[0:1, :]
                for j in range(1, 8):
                    line = line + total[j] * w_y[j : j + 1, :]
                value = jnp.sum(line * w_x, axis=0, keepdims=True)
                for t in range(group):
                    row = chunk * group + t
                    answer[shift + REACH, field, row : row + 1, :] = value[
                        :, t * lanes : (t + 1) * lanes
                    ]

    near_first = [0] + [sign * reach for reach in range(1, REACH + 1) for sign in (1, -1)]
    with jax.named_scope('w_ask'):
        asks(1, 1).wait_recv()
    evaluate(0, 0, 1)
    reply(0, 0).start()
    with jax.named_scope('w_ask'):
        with_partners(lambda many: asks(many - 1, 2).wait_recv())
    for shift in near_first[1:]:
        evaluate(shift, 0, 1)
    for shift in near_first[1:]:

        @pl.when(inside(slab - shift))
        def _():
            reply(shift, 0).start()

    turns_left = list(range(slots))

    def serve_rest(many):
        for _ in range(many):
            shift = near_first[turns_left.pop(0)]

            @pl.when(inside(slab - shift))
            def _():
                with jax.named_scope('rest'):
                    evaluate(shift, 1, fields)
                reply(shift, 1).start()

    room_index = lax.broadcasted_iota(jnp.int32, (room, lanes), 0)
    plans = []
    for slot in range(slots):
        table = ranks[slot * height : (slot + 1) * height, :]
        base = jnp.broadcast_to(table[0:1], (room, lanes))
        first = jnp.minimum(base >> row_bits, half - 1)
        second = jnp.minimum(first + 1, half - 1)
        offset = base & (height - 1)
        spots = table & (height - 1)
        plans.append((first, second, offset, spots))

    serve_rest(2)
    with jax.named_scope('w_reply'):
        with_partners(lambda many: replies(many, 0).wait_recv())

    def along_lanes(tile, index):
        return jnp.take_along_axis(tile, index, axis=1, mode="promise_in_bounds")

    def along_rows(tile, index):
        return jnp.take_along_axis(tile, index, axis=0, mode="promise_in_bounds")

    def gather_field(field):
        result = [jnp.zeros((room, lanes), jnp.float32)] * 2
        for slot in range(slots):
            packed = answered[slot, field]
            first, second, offset, spots = plans[slot]
            windows = [
                jnp.where(
                    room_index + part * room >= offset,
                    along_lanes(packed, first + part * half),
                    along_lanes(packed, second + part * half),
                )
                for part in range(2)
            ]
            for part in range(2):
                spot = spots[part * room : (part + 1) * room]
                member = members[slot][part * room : (part + 1) * room]
                low, high = [along_rows(window, spot & (room - 1)) for window in windows]
                tile = jnp.where(spot < room, low, high)
                result[part] = jnp.where(member, tile, result[part])
        return jnp.concatenate(result, 0)

    values = [gather_field(0)]
    groups = lanes // 64
    rows = jnp.concatenate([values[0][:, t * 64 : (t + 1) * 64] for t in range(groups)], 0)
    per_side = height // 2
    row = lax.broadcasted_iota(jnp.int32, (groups * height, elems), 0)
    spot = lax.broadcasted_iota(jnp.int32, (groups * height, elems), 1)
    piece = row % height
    target = (groups * (piece % per_side) + row // height) * EX + (EX - 1) * (piece // per_side)
    placed = lax.dot_general(
        rows,
        flag(spot == target),
        (((0,), (0,)), ((), ())),
        precision=lax.Precision.HIGHEST,
        preferred_element_type=jnp.float32,
    ).reshape(8, 8, elems)
    rim[0] = placed[0]
    rim[1] = placed[7]
    for at in range(4):

        @pl.when(rim_sends[at])
        def _():
            rim_copy(at).start()

    def spread_out(column):
        return plane_sum(
            jnp.concatenate(
                [
                    (jnp.broadcast_to(column[j : j + 1, :], (8, elems)) * mark)[None]
                    for j in range(8)
                ],
                0,
            )
        )

    def in_plane(tile, along):
        along_y = along_y_ref[0] * tile[0:1]
        for j in range(1, 8):
            along_y = along_y + along_y_ref[j] * tile[j : j + 1]
        along_x = along_x_ref[0] * tile
        for step in range(1, 8):
            along_x = along_x + along_x_ref[step] * pltpu.roll(tile, step, 1)
        return along[0] * along_x + along[1] * along_y

    def inner_z(read, layer):
        total = read(1) * float(stiff[layer, 1])
        for k in range(2, 7):
            total = total + read(k) * float(stiff[layer, k])
        return total

    def outer_z(low, high, layer):
        return low * float(stiff[layer, 0]) + high * float(stiff[layer, 7])

    here = (g_x, g_y, g_z, g_m)
    edge = weights(0)

    for layer in ORDER:
        boundary[layer] = spread_out(placed[layer]) * sharing[layer]
    loads[6].wait()
    for layer in ORDER:
        along_z = inner_z(lambda k: boundary[k], layer)
        along_z = along_z + outer_z(boundary[0], boundary[7], layer)
        tile = boundary[layer]
        total = in_plane(tile, here) + g_z * along_z + g_m * (tile - forcing_ref[layer])
        total = weights(layer) * total
        if layer in (0, 7):
            total = plane_sum(total)
        residual[layer] = total
        if layer == 7:
            faces[0, 0] = residual[0]
            faces[0, 1] = residual[7]
            send_faces(0)

    beyond = []
    for side in range(2):

        @pl.when(near[side])
        def _():
            geometry_copy(side == 0).wait_recv()

        along = [geometry_halo[side, d : d + 1, :] for d in range(4)]
        own = boundary[0 if side == 0 else 7]
        term = in_plane(own, along)
        term = term + (along[2] * float(stiff[0, 0]) + along[3]) * own
        beyond.append((term, along[2] * float(stiff[0, 7])))
        walls = wall_plane + wall_marks([geometry_halo[side, 4:5, :], geometry_halo[side, 5:6, :]])
        layer, facing = (0, 7) if side == 0 else (7, 0)
        settle(layer, z_counts[side], walls, diagonal(here, layer) + diagonal(along, facing))
    serve_rest(1)

    with jax.named_scope('w_rim'):
        with_partners(lambda many: rims(many - 1).wait_recv())

    low = spread_out(rim_halo[0]) * sharing[0]
    high = spread_out(rim_halo[1]) * sharing[7]
    boundary[0] = boundary[0] + low
    boundary[7] = boundary[7] + high
    for layer in range(1, 7):
        more = weights(layer) * (g_z * outer_z(low, high, layer))
        residual[layer] = -free[layer] * plane_sum(residual[layer] + more)
        rho[layer] = residual[layer]
        vectors[0, layer] = inverse[layer] * residual[layer]
    half_share = 0.5 / plane_count
    ends = []
    for side, (own, layer) in enumerate(((low, 0), (high, 7))):
        more = in_plane(own, here) + g_m * own + g_z * outer_z(low, high, layer)
        term, across_z = beyond[side]
        more = more + term + across_z * (spread_out(rim_halo[2 + side]) * half_share)
        ends.append(residual[layer] + plane_sum(edge * more))

    def prepare(turn):
        def read(k):
            return vectors[turn, k]

        for layer in range(1, 7):
            tile = vectors[turn, layer]
            partial[layer] = (
                in_plane(tile, here) + g_m * tile + g_z * inner_z(read, layer)
            )
        for layer in (0, 7):
            partial[layer] = g_z * inner_z(read, layer)

    prepare(0)
    with jax.named_scope('w_f2'):
        wait_faces(0)
    for side, layer in ((0, 0), (1, 7)):
        residual[layer] = -free[layer] * (ends[side] + halo[0, side])
        rho[layer] = residual[layer]
        vectors[0, layer] = inverse[layer] * residual[layer]

    sums = {}

    def gather_sum(key, value):
        value = jnp.sum(value, axis=0)
        sums[key] = value if key not in sums else sums[key] + value

    for turn in range(ITERS):
        phase = 1 + turn
        low = vectors[turn, 0]
        high = vectors[turn, 7]
        outer = {}
        for layer in (0, 7):
            tile = vectors[turn, layer]
            total = in_plane(tile, here) + g_m * tile + g_z * outer_z(low, high, layer)
            outer[layer] = edge * (total + partial[layer])
            images[turn, layer] = plane_sum(outer[layer])
        faces[phase, 0] = images[turn, 0]
        faces[phase, 1] = images[turn, 7]
        send_faces(phase)
        last = turn == ITERS - 1
        for layer in range(8):
            if layer in outer:
                tile = outer[layer]
            else:
                tile = partial[layer] + g_z * outer_z(low, high, layer)
                tile = weights(layer) * tile
            for other_turn in range(turn + 1):
                gather_sum((other_turn, turn), tile * vectors[other_turn, layer])
            gather_sum(
                turn, vectors[turn, layer] * residual[layer] * sharing[layer]
            )
            if layer not in outer:
                images[turn, layer] = tile if last else free[layer] * plane_sum(tile)
        if last:
            break
        for layer in range(1, 7):
            rho[layer] = images[turn, layer] - SHIFTS[turn] * rho[layer]
            vectors[turn + 1, layer] = inverse[layer] * rho[layer]
        prepare(turn + 1)
        serve_rest(WINDOWS[turn])
        with jax.named_scope('w_fc'):
            wait_faces(phase)
        for side, layer in ((0, 0), (1, 7)):
            images[turn, layer] = free[layer] * (images[turn, layer] + halo[phase, side])
            rho[layer] = images[turn, layer] - SHIFTS[turn] * rho[layer]
            vectors[turn + 1, layer] = inverse[layer] * rho[layer]

    keys = list(range(ITERS)) + [(a, b) for b in range(ITERS) for a in range(b + 1)]
    spot = lax.broadcasted_iota(jnp.int32, (1, 128), 1)
    packed = jnp.zeros((1, 128), jnp.float32)
    for at, key in enumerate(keys):
        value = jnp.sum(jnp.sum(sums[key], axis=0, keepdims=True), axis=1, keepdims=True)
        packed = jnp.where(spot == at, value, packed)
    dots[...] = packed
    for step in range(1, n):
        dot_copy(step).start()
    all_dots[slab] = dots[...]
    with jax.named_scope('w_rest'):
        with_partners(lambda many: replies(many, 1).wait_recv())

    values = values + [gather_field(field) for field in range(1, fields)]
    for row in range(height):
        interface_ref[:, row * lanes : (row + 1) * lanes] = jnp.concatenate(
            [value[row : row + 1] for value in values], 0
        )
    for layer in range(1, 7):
        images[ITERS - 1, layer] = free[layer] * plane_sum(images[ITERS - 1, layer])
    with jax.named_scope('w_fc'):
        wait_faces(ITERS)
    for side, layer in ((0, 0), (1, 7)):
        images[ITERS - 1, layer] = free[layer] * (
            images[ITERS - 1, layer] + halo[ITERS, side]
        )
    with jax.named_scope('w_dots'):
        all_dot_copies().wait_recv()
    with jax.named_scope('solve'):
        total = jnp.sum(all_dots[...], axis=0)
        found = {
            key: jnp.broadcast_to(total[:, at : at + 1], (8, elems))
            for at, key in enumerate(keys)
        }
        steps_taken = solve(found)
    for layer in range(8):
        moved = boundary[layer]
        for turn in range(ITERS):
            moved = moved + steps_taken[turn] * vectors[turn, layer]
        velocity[layer] = moved
    for layer in range(8):
        left_over = residual[layer]
        for turn in range(ITERS):
            left_over = left_over - steps_taken[turn] * images[turn, layer]
        residual_out[layer] = left_over
    all_dot_copies().wait_send()
    for side in range(2):

        @pl.when(near[1 - side])
        def _():
            geometry_copy(side == 0).wait_send()

    with_partners(lambda many: rims(many - 1).wait_send())
    with_partners(lambda many: asks(many, 1).wait_send())
    for part in range(2):
        with_partners(lambda many: replies(many, part).wait_send())


def flush(*refs):
    count = (len(refs) - 1) // 2
    sem = refs[-1]
    copies = [
        pltpu.make_async_copy(refs[at], refs[count + at], sem.at[at]) for at in range(count)
    ]
    for copy in copies:
        copy.start()
    for copy in copies:
        copy.wait()


def body(n, donor_fields, interp_weights, donor_owner, donor_element, geometry, wall_flag, forcing):
    fields = donor_fields.shape[0]
    elems = geometry.shape[1]
    receptors = donor_element.shape[0]
    slots = 2 * REACH + 1
    lanes = 128
    count = receptors // lanes
    cube = (8, 8, 8, elems)
    phases = 1 + ITERS
    room = count // 2
    vmem = pl.BlockSpec(memory_space=pltpu.VMEM)
    hbm = pl.BlockSpec(memory_space=pltpu.HBM)
    shapes = (
        jax.ShapeDtypeStruct(cube, jnp.float32),
        jax.ShapeDtypeStruct(cube, jnp.float32),
        jax.ShapeDtypeStruct((fields, receptors), jnp.float32),
    )
    outputs = pl.pallas_call(
        functools.partial(kernel, n),
        out_shape=shapes,
        in_specs=[hbm] * 7,
        out_specs=(vmem, vmem, vmem),
        scratch_shapes=[
            pltpu.VMEM(cube, jnp.float32),
            pltpu.VMEM((fields, 512, elems), jnp.float32),
            pltpu.VMEM(cube, jnp.float32),
            pltpu.VMEM(interp_weights.shape, jnp.float32),
            pltpu.VMEM((count, lanes), jnp.int32),
            pltpu.VMEM((count, lanes), jnp.int32),
            pltpu.VMEM(geometry.shape, jnp.float32),
            pltpu.VMEM(wall_flag.shape, jnp.int32),
            pltpu.VMEM((3, count, lanes), jnp.float32),
            pltpu.VMEM((slots, 4, room, lanes), jnp.float32),
            pltpu.VMEM((slots * count, lanes), jnp.int32),
            pltpu.VMEM(cube, jnp.float32),
            pltpu.VMEM((8, 8, elems), jnp.float32),
            pltpu.VMEM((8, 8, elems), jnp.float32),
            pltpu.SemaphoreType.DMA((7,)),
            pltpu.VMEM((fields * 512, 2 * elems), jnp.bfloat16),
            pltpu.VMEM((slots, 4, room, lanes), jnp.float32),
            pltpu.VMEM((slots, fields, room, lanes), jnp.float32),
            pltpu.VMEM((slots, fields, room, lanes), jnp.float32),
            pltpu.VMEM((phases, 2, 8, 8, elems), jnp.float32),
            pltpu.VMEM((phases, 2, 8, 8, elems), jnp.float32),
            pltpu.VMEM((1, 128), jnp.float32),
            pltpu.VMEM((n, 1, 128), jnp.float32),
            pltpu.VMEM((ITERS,) + cube, jnp.float32),
            pltpu.VMEM((ITERS,) + cube, jnp.float32),
            pltpu.VMEM(cube, jnp.float32),
            pltpu.VMEM(cube, jnp.float32),
            pltpu.VMEM((2, 8, elems), jnp.float32),
            pltpu.VMEM((4, 8, elems), jnp.float32),
            pltpu.VMEM((2, 8, elems), jnp.float32),
            pltpu.VMEM((8, elems), jnp.float32),
        ]
        + [pltpu.VMEM(cube, jnp.float32)] * 4
        + [pltpu.SemaphoreType.DMA((3,)), pltpu.SemaphoreType.DMA((2, 2))]
        + [pltpu.SemaphoreType.DMA((2,)), pltpu.SemaphoreType.DMA((2, 2))]
        + [pltpu.SemaphoreType.DMA((2,))]
        + [pltpu.SemaphoreType.DMA((2,))]
        + [pltpu.SemaphoreType.DMA((2,))] * 2,
        compiler_params=pltpu.CompilerParams(
            collective_id=0, has_side_effects=True, vmem_limit_bytes=48 * 1024 * 1024
        ),
    )(
        *[
            pltpu.with_memory_space_constraint(array, pltpu.HBM)
            for array in (
                donor_fields,
                interp_weights,
                donor_owner.reshape(count, lanes),
                donor_element.reshape(count, lanes),
                geometry,
                wall_flag,
                forcing.reshape(cube),
            )
        ]
    )
    velocity, residual, interface = pl.pallas_call(
        flush,
        out_shape=shapes,
        in_specs=[vmem] * 3,
        out_specs=(hbm,) * 3,
        scratch_shapes=[pltpu.SemaphoreType.DMA((3,))],
        compiler_params=pltpu.CompilerParams(vmem_limit_bytes=1024 * 1024),
    )(*outputs)
    return (velocity.reshape(512, elems), residual.reshape(512, elems), interface)


def solution(mesh):
    in_specs = (
        P(None, None, ("mesh", "dom")),
        P(None, None, ("mesh", "dom")),
        P(("mesh", "dom"), None),
        P(("mesh", "dom")),
        P(None, ("mesh", "dom")),
        P(None, ("mesh", "dom")),
        P(None, ("mesh", "dom")),
    )
    out_specs = (P(None, ("mesh", "dom")), P(None, ("mesh", "dom")), P(None, ("mesh", "dom")))
    return jax.shard_map(
        functools.partial(body, mesh.shape["dom"]),
        mesh=mesh,
        in_specs=in_specs,
        out_specs=out_specs,
        check_vma=False,
    )
```

```python
import functools

import jax
import jax.numpy as jnp
import numpy as np
from jax import lax
from jax.experimental import pallas as pl
from jax.experimental.pallas import tpu as pltpu
from jax.sharding import PartitionSpec as P

EX = 8
EY = 16
ITERS = 3
REACH = 2
CHUNK = 256
ORDER = (0, 7, 1, 2, 3, 4, 5, 6)
SHIFTS = (1.5, 0.5)
WINDOW = 2
MESH = pl.DeviceIdType.MESH


def legendre_pair(values, degree):
    previous = values * 0.0 + 1.0
    current = values * 1.0
    for poly_order in range(2, degree + 1):
        previous, current = (
            current,
            ((2 * poly_order - 1) * values * current - (poly_order - 1) * previous) / poly_order,
        )
    return (current, previous)


def gll_tables():
    degree = 7
    points_count = degree + 1
    abscissae = np.cos(np.pi * np.arange(points_count) / degree)
    for newton_turn in range(80):
        top_poly, lower_poly = legendre_pair(abscissae, degree)
        abscissae = abscissae - (abscissae * top_poly - lower_poly) / (points_count * top_poly)
    abscissae = np.sort(abscissae)
    top_poly, lower_poly = legendre_pair(abscissae, degree)
    quad_weights = 2.0 / (degree * points_count * top_poly * top_poly)
    identity_mat = np.eye(points_count)
    spacing = abscissae[:, None] - abscissae[None, :] + identity_mat
    derivative = top_poly[:, None] / (top_poly[None, :] * spacing) * (1.0 - identity_mat)
    derivative[0, 0] = -degree * points_count / 4.0
    derivative[degree, degree] = degree * points_count / 4.0
    return (abscissae, derivative, quad_weights)


def solve(found):
    matrix = [
        [found[(min(a, b), max(a, b))] for b in range(ITERS)] for a in range(ITERS)
    ]
    right = [found[a] for a in range(ITERS)]
    pivots = []
    for a in range(ITERS):
        pivots.append(1.0 / matrix[a][a])
        for b in range(a + 1, ITERS):
            factor = matrix[b][a] * pivots[a]
            for c in range(a + 1, ITERS):
                matrix[b][c] = matrix[b][c] - factor * matrix[a][c]
            right[b] = right[b] - factor * right[a]
    answer = [None] * ITERS
    for a in reversed(range(ITERS)):
        total = right[a]
        for b in range(a + 1, ITERS):
            total = total - matrix[a][b] * answer[b]
        answer[a] = total * pivots[a]
    return answer


def kernel(
    n,
    donor_hbm,
    weights_hbm,
    owner_hbm,
    element_hbm,
    geometry_hbm,
    wall_hbm,
    forcing_hbm,
    velocity,
    residual_out,
    interface_ref,
    residual,
    donor_ref,
    forcing_ref,
    weights_ref,
    owner_ref,
    element_ref,
    geometry_ref,
    wall_ref,
    position_ref,
    request_ref,
    ranks,
    along_y_ref,
    along_x_ref,
    plane_ref,
    load_sem,
    split,
    asked,
    answer,
    answered,
    faces,
    halo,
    dots,
    all_dots,
    vectors,
    images,
    partial,
    rho,
    rim,
    rim_halo,
    geometry_halo,
    packet,
    far_faces,
    far_halo,
    inverse,
    free,
    sharing,
    boundary,
    ask_sem,
    reply_sem,
    face_send,
    face_recv,
    far_sem,
    dot_sem,
    rim_sem,
    geometry_send,
    geometry_recv,
):
    points, derivative, quad = gll_tables()
    stiff = (derivative.T * quad) @ derivative / quad[:, None]
    fields = donor_ref.shape[0]
    elems = donor_ref.shape[2]
    height = owner_ref.shape[0]
    lanes = owner_ref.shape[1]
    receptors = height * lanes
    room = request_ref.shape[2]
    slots = 2 * REACH + 1
    mesh_id = lax.axis_index("mesh")
    slab = lax.axis_index("dom")
    other = 1 - mesh_id

    pairs = [
        (weights_hbm, weights_ref),
        (owner_hbm, owner_ref),
        (element_hbm, element_ref),
        (donor_hbm, donor_ref),
        (geometry_hbm, geometry_ref),
        (wall_hbm, wall_ref),
        (forcing_hbm, forcing_ref),
    ]
    loads = [
        pltpu.make_async_copy(source, target, load_sem.at[at])
        for at, (source, target) in enumerate(pairs)
    ]
    for load in loads:
        load.start()

    def inside(index):
        return jnp.logical_and(index >= 0, index < n)

    barrier = pltpu.get_barrier_semaphore()
    greeted = n - 1
    for step in range(1, n):
        pl.semaphore_signal(
            barrier, inc=1, device_id=(mesh_id, lax.rem(slab + step, n)), device_id_type=MESH
        )
    for shift in range(-REACH, REACH + 1):
        greeted = greeted + jnp.where(inside(slab + shift), 1, 0)

        @pl.when(inside(slab + shift))
        def _():
            pl.semaphore_signal(
                barrier, inc=1, device_id=(other, slab + shift), device_id_type=MESH
            )

    with jax.named_scope('w_loads'):
        for load in loads[:3]:
            load.wait()
    depth = lax.broadcasted_iota(jnp.int32, (8, lanes), 0)
    ladder = jnp.zeros((8, lanes), jnp.float32)
    for a in range(8):
        ladder = jnp.where(depth == a, float(points[a]), ladder)
    for d in range(3):
        for row in range(height):
            part = weights_ref[d, :, row * lanes : (row + 1) * lanes] * ladder
            position_ref[d, row : row + 1, :] = jnp.sum(part, axis=0, keepdims=True)
    owner = owner_ref[...]
    element_code = element_ref[...] * receptors
    members = [owner == slab + shift for shift in range(-REACH, REACH + 1)]
    tall = slots * height
    marks = jnp.concatenate([jnp.where(m, 1.0, 0.0) for m in members], 0).astype(jnp.bfloat16)
    before = lax.broadcasted_iota(jnp.int32, (lanes, lanes), 0)
    after = lax.broadcasted_iota(jnp.int32, (lanes, lanes), 1)
    upper = jnp.where(before < after, 1.0, 0.0).astype(jnp.bfloat16)
    left = jnp.dot(marks, upper, preferred_element_type=jnp.float32).astype(jnp.bfloat16)
    above = lax.broadcasted_iota(jnp.int32, (tall, tall), 0)
    below = lax.broadcasted_iota(jnp.int32, (tall, tall), 1)
    same = above // height == below // height
    block = jnp.where(same, 1.0, 0.0).astype(jnp.bfloat16)
    lower = jnp.where(same & (below < above), 1.0, 0.0).astype(jnp.bfloat16)
    rank = jnp.dot(block, left, preferred_element_type=jnp.float32)
    rank = rank + jnp.dot(lower, marks, preferred_element_type=jnp.float32)
    rank = rank.astype(jnp.int32)
    ranks[...] = rank
    row_index = lax.broadcasted_iota(jnp.int32, (height, lanes), 0)
    place = lax.broadcasted_iota(jnp.int32, (height, lanes), 1) * height + row_index
    row_bits = height.bit_length() - 1
    steps = receptors.bit_length() - 1

    def pull(tile, step):
        if step >= row_bits:
            return pltpu.roll(tile, lanes - (1 << (step - row_bits)), 1)
        jump = 1 << step
        near = pltpu.roll(tile, height - jump, 0)
        far = pltpu.roll(near, lanes - 1, 1)
        return jnp.where(row_index < height - jump, near, far)

    words = []
    comps = []
    start = [position_ref[d] for d in range(3)]
    for slot in range(slots):
        shift = place - rank[slot * height : (slot + 1) * height]
        words.append(jnp.where(members[slot], element_code + shift, 0))
        comps.append(list(start))
    for step in range(steps):
        for slot in range(slots):
            word = words[slot]
            moving = word & (1 << step)
            came = pull(word, step)
            take = (came & (1 << step)) != 0
            words[slot] = jnp.where(take, came - (1 << step), jnp.where(moving != 0, 0, word))
            comps[slot] = [jnp.where(take, pull(c, step), c) for c in comps[slot]]
    half = lanes // 2
    left_half = lax.broadcasted_iota(jnp.int32, (room, lanes), 1) < half
    for slot in range(slots):
        columns = comps[slot] + [(words[slot] >> steps).astype(jnp.float32)]
        for at, column in enumerate(columns):
            request_ref[slot, at] = jnp.where(
                left_half, column[:room], pltpu.roll(column[room:], half, 1)
            )

    with jax.named_scope('w_barrier'):
        pl.semaphore_wait(barrier, greeted)

    def ask(shift):
        return pltpu.make_async_remote_copy(
            src_ref=request_ref.at[shift + REACH],
            dst_ref=asked.at[shift + REACH],
            send_sem=ask_sem.at[0],
            recv_sem=ask_sem.at[1 if shift == 0 else 2],
            device_id=(other, lax.rem(slab + shift + n, n)),
            device_id_type=MESH,
        )

    def reply(shift, part):
        span = pl.ds(0, 1) if part == 0 else pl.ds(1, fields - 1)
        return pltpu.make_async_remote_copy(
            src_ref=answer.at[shift + REACH, span],
            dst_ref=answered.at[shift + REACH, span],
            send_sem=reply_sem.at[0, part],
            recv_sem=reply_sem.at[1, part],
            device_id=(other, lax.rem(slab - shift + n, n)),
            device_id_type=MESH,
        )

    def asks(many, sem):
        return pltpu.make_async_remote_copy(
            src_ref=asked.at[pl.ds(0, many)],
            dst_ref=asked.at[pl.ds(0, many)],
            send_sem=ask_sem.at[0],
            recv_sem=ask_sem.at[sem],
            device_id=(other, slab),
            device_id_type=MESH,
        )

    def replies(many, part):
        span = pl.ds(0, 1) if part == 0 else pl.ds(1, fields - 1)
        return pltpu.make_async_remote_copy(
            src_ref=answered.at[pl.ds(0, many), span],
            dst_ref=answered.at[pl.ds(0, many), span],
            send_sem=reply_sem.at[0, part],
            recv_sem=reply_sem.at[1, part],
            device_id=(other, slab),
            device_id_type=MESH,
        )

    partners = 0
    for shift in range(-REACH, REACH + 1):
        partners = partners + jnp.where(inside(slab + shift), 1, 0)

    def with_partners(action):
        for many in range(REACH + 1, slots + 1):

            @pl.when(partners == many)
            def _():
                action(many)

    def face_copy(phase, up):
        step = 1 if up else n - 1
        return pltpu.make_async_remote_copy(
            src_ref=faces.at[phase, 1 if up else 0],
            dst_ref=halo.at[phase, 0 if up else 1],
            send_sem=face_send.at[phase % 3, 1 if up else 0],
            recv_sem=face_recv.at[phase % 3, 0 if up else 1],
            device_id=(mesh_id, lax.rem(slab + step, n)),
            device_id_type=MESH,
        )

    def send_faces(phase):
        @pl.when(slab < n - 1)
        def _():
            face_copy(phase, True).start()

        @pl.when(slab > 0)
        def _():
            face_copy(phase, False).start()

    def wait_faces(phase):
        @pl.when(slab > 0)
        def _():
            face_copy(phase, True).wait_recv()

        @pl.when(slab < n - 1)
        def _():
            face_copy(phase, False).wait_recv()

        @pl.when(slab < n - 1)
        def _():
            face_copy(phase, True).wait_send()

        @pl.when(slab > 0)
        def _():
            face_copy(phase, False).wait_send()

    def dot_copy(step):
        return pltpu.make_async_remote_copy(
            src_ref=dots,
            dst_ref=all_dots.at[slab],
            send_sem=dot_sem.at[0],
            recv_sem=dot_sem.at[1],
            device_id=(mesh_id, lax.rem(slab + step, n)),
            device_id_type=MESH,
        )

    def far_copy(up):
        side = 0 if up else 1
        return pltpu.make_async_remote_copy(
            src_ref=far_faces.at[1 - side],
            dst_ref=far_halo.at[side],
            send_sem=far_sem.at[0, side],
            recv_sem=far_sem.at[1, side],
            device_id=(mesh_id, lax.rem(slab + (2 if up else n - 2), n)),
            device_id_type=MESH,
        )

    above_far = slab < n - 2
    below_far = slab > 1

    def send_far():
        @pl.when(above_far)
        def _():
            far_copy(True).start()

        @pl.when(below_far)
        def _():
            far_copy(False).start()

    def wait_far():
        @pl.when(below_far)
        def _():
            far_copy(True).wait_recv()

        @pl.when(above_far)
        def _():
            far_copy(False).wait_recv()

        @pl.when(above_far)
        def _():
            far_copy(True).wait_send()

        @pl.when(below_far)
        def _():
            far_copy(False).wait_send()

    def all_dot_copies():
        return pltpu.make_async_remote_copy(
            src_ref=all_dots.at[pl.ds(0, n - 1)],
            dst_ref=all_dots.at[pl.ds(0, n - 1)],
            send_sem=dot_sem.at[0],
            recv_sem=dot_sem.at[1],
            device_id=(mesh_id, lax.rem(slab + 1, n)),
            device_id_type=MESH,
        )

    rim_jumps = (1, -1, 2, -2)
    rim_sends = [inside(slab + jump) for jump in rim_jumps]
    rim_comes = [inside(slab - jump) for jump in rim_jumps]
    near = (slab > 0, slab < n - 1)

    def rim_copy(at):
        return pltpu.make_async_remote_copy(
            src_ref=rim.at[1 - at % 2],
            dst_ref=rim_halo.at[at],
            send_sem=rim_sem.at[0],
            recv_sem=rim_sem.at[1],
            device_id=(mesh_id, lax.rem(slab + rim_jumps[at] + n, n)),
            device_id_type=MESH,
        )

    def rims(many):
        return pltpu.make_async_remote_copy(
            src_ref=rim_halo.at[pl.ds(0, many)],
            dst_ref=rim_halo.at[pl.ds(0, many)],
            send_sem=rim_sem.at[0],
            recv_sem=rim_sem.at[1],
            device_id=(mesh_id, lax.rem(slab + 1, n)),
            device_id_type=MESH,
        )

    def geometry_copy(up):
        side = 0 if up else 1
        return pltpu.make_async_remote_copy(
            src_ref=packet,
            dst_ref=geometry_halo.at[side],
            send_sem=geometry_send.at[side],
            recv_sem=geometry_recv.at[side],
            device_id=(mesh_id, lax.rem(slab + (1 if up else n - 1), n)),
            device_id_type=MESH,
        )

    for distance in range(REACH + 1):
        for shift in sorted({distance, -distance}):

            @pl.when(inside(slab + shift))
            def _():
                ask(shift).start()

    phases = halo.shape[0]
    blank = jnp.zeros(halo.shape[2:], jnp.float32)

    for shift in range(-REACH, REACH + 1):

        @pl.when(jnp.logical_not(inside(slab + shift)))
        def _():
            answered[shift + REACH] = jnp.zeros(answered.shape[1:], jnp.float32)

        @pl.when(jnp.logical_not(inside(slab - shift)))
        def _():
            asked[shift + REACH] = jnp.zeros(asked.shape[1:], jnp.float32)

    for at in range(4):

        @pl.when(jnp.logical_not(rim_comes[at]))
        def _():
            rim_halo[at] = jnp.zeros(rim_halo.shape[1:], jnp.float32)

    for side in range(2):

        @pl.when(jnp.logical_not(near[side]))
        def _():
            geometry_halo[side] = jnp.zeros(geometry_halo.shape[1:], jnp.float32)

    @pl.when(jnp.logical_not(below_far))
    def _():
        far_halo[0] = blank

    @pl.when(jnp.logical_not(above_far))
    def _():
        far_halo[1] = blank

    @pl.when(slab == 0)
    def _():
        for phase in range(phases):
            halo[phase, 0] = blank

    @pl.when(slab == n - 1)
    def _():
        for phase in range(phases):
            halo[phase, 1] = blank

    node = lax.broadcasted_iota(jnp.int32, (8, elems), 0)
    element = lax.broadcasted_iota(jnp.int32, (8, elems), 1)
    x_index = element % EX
    y_index = element // EX % EY

    across = jnp.zeros((8, elems), jnp.float32)
    for a in range(8):
        across = jnp.where(node == a, float(quad[a]), across)
    for j in range(8):
        plane_ref[j] = across * float(quad[j])
        for m in range(8):
            along_y_ref[m, j] = jnp.full((8, elems), float(stiff[j, m]), jnp.float32)
    for step in range(8):
        turned = jnp.zeros((8, elems), jnp.float32)
        for i in range(8):
            turned = jnp.where(node == i, float(stiff[i, (i - step) % 8]), turned)
        along_x_ref[step] = turned

    def flag(condition):
        return jnp.where(condition, 1.0, 0.0)

    x_low = flag((node == 0) & (x_index > 0))
    x_high = flag((node == 7) & (x_index < EX - 1))
    y_low = flag(y_index > 0)
    y_high = flag(y_index < EY - 1)

    def plane_sum(tile):
        below = pltpu.roll(pltpu.roll(tile, 1, 1), 1, 2)
        above = pltpu.roll(pltpu.roll(tile, 7, 1), elems - 1, 2)
        tile = tile + below * x_low + above * x_high
        low = tile[0] + y_low * pltpu.roll(tile[7], EX, 1)
        high = tile[7] + y_high * pltpu.roll(tile[0], elems - EX, 1)
        return jnp.concatenate([low[None], tile[1:7], high[None]], 0)

    def weights(layer):
        return plane_ref[...] * float(quad[layer])

    loads[4].wait()
    loads[5].wait()

    wall_rows = []
    for side in range(2):
        wall_row = jnp.zeros((1, elems), jnp.float32)
        for x in range(EX):
            bit = wall_ref[side : side + 1, x : x + 1].astype(jnp.float32)
            wall_row = jnp.where(x_index[0:1] == x, bit, wall_row)
        wall_rows.append(wall_row)
    g_x, g_y, g_z, g_m = [geometry_ref[d : d + 1, :] for d in range(4)]

    packet[...] = jnp.concatenate(
        [geometry_ref[...]] + wall_rows + [jnp.zeros((2, elems), jnp.float32)], 0
    )

    @pl.when(near[1])
    def _():
        geometry_copy(True).start()

    @pl.when(near[0])
    def _():
        geometry_copy(False).start()

    diag_y = [jnp.full((8, elems), float(stiff[j, j]), jnp.float32)[None] for j in range(8)]
    diag_y = jnp.concatenate(diag_y, 0)

    def diagonal(along, layer):
        total = along[0] * along_x_ref[0] + along[1] * diag_y
        total = total + (along[2] * float(stiff[layer, layer]) + along[3])
        return plane_sum(weights(layer) * total)

    nothing = jnp.zeros((6, 8, elems), jnp.float32)

    def wall_marks(rows):
        low_wall = flag(y_index == 0) * rows[0]
        high_wall = flag(y_index == EY - 1) * rows[1]
        return plane_sum(jnp.concatenate([low_wall[None], nothing, high_wall[None]], 0))

    wall_plane = wall_marks(wall_rows)
    x_count = 1.0 + x_low + x_high
    y_count_low = 1.0 + y_low
    y_count_high = 1.0 + y_high
    plane_count = jnp.concatenate(
        [(x_count * y_count_low)[None]]
        + [x_count[None]] * 6
        + [(x_count * y_count_high)[None]],
        0,
    )
    mark = flag((node == 0) & (x_index == 0)) + flag((node == 7) & (x_index == EX - 1))

    def settle(layer, z_count, walls, diag):
        count = plane_count * z_count
        open_part = 1.0 - jnp.minimum(mark * count + walls, 1.0)
        sharing[layer] = 1.0 / count
        free[layer] = open_part
        inverse[layer] = open_part / diag

    for layer in range(1, 7):
        settle(layer, 1.0, wall_plane, diagonal((g_x, g_y, g_z, g_m), layer))
    z_counts = (jnp.where(slab > 0, 2.0, 1.0), jnp.where(slab < n - 1, 2.0, 1.0))
    for side, layer in ((0, 0), (1, 7)):
        sharing[layer] = 1.0 / (plane_count * z_counts[side])

    with jax.named_scope('w_donor'):
        loads[3].wait()
    donors = donor_ref[...].reshape(fields * 512, elems)
    coarse = donors.astype(jnp.bfloat16)
    split[:, :elems] = coarse
    split[:, elems:] = (donors - coarse.astype(jnp.float32)).astype(jnp.bfloat16)

    code = lax.broadcasted_iota(jnp.int32, (elems, CHUNK), 0)
    code = code.astype(jnp.float32)
    basis = lax.broadcasted_iota(jnp.int32, (8, CHUNK), 0)
    norms = [
        float(1.0 / np.prod([points[a] - points[b] for b in range(8) if b != a])) for a in range(8)
    ]
    scale = jnp.zeros((8, CHUNK), jnp.float32)
    for a in range(8):
        scale = jnp.where(basis == a, norms[a], scale)

    def lagrange(position):
        value = scale
        for b in range(8):
            value = value * jnp.where(basis == b, 1.0, position - float(points[b]))
        return value

    def evaluate(shift, first, last):
        group = CHUNK // lanes
        for chunk in range(room // group):
            block = [
                jnp.concatenate(
                    [
                        asked[shift + REACH, c, chunk * group + t : chunk * group + t + 1, :]
                        for t in range(group)
                    ],
                    1,
                )
                for c in range(4)
            ]
            chosen = jnp.where(block[3] == code, 1.0, 0.0).astype(jnp.bfloat16)
            chosen = jnp.concatenate([chosen, chosen], 0)
            w_x, w_y, w_z = [lagrange(block[d]) for d in range(3)]
            picked = jnp.dot(
                split[first * 512 : last * 512], chosen, preferred_element_type=jnp.float32
            )
            for field in range(first, last):
                cube = picked[(field - first) * 512 : (field - first + 1) * 512]
                cube = cube.reshape(8, 64, CHUNK)
                total = cube[0] * w_z[0:1, :]
                for k in range(1, 8):
                    total = total + cube[k] * w_z[k : k + 1, :]
                total = total.reshape(8, 8, CHUNK)
                line = total[0] * w_y[0:1, :]
                for j in range(1, 8):
                    line = line + total[j] * w_y[j : j + 1, :]
                value = jnp.sum(line * w_x, axis=0, keepdims=True)
                for t in range(group):
                    row = chunk * group + t
                    answer[shift + REACH, field, row : row + 1, :] = value[
                        :, t * lanes : (t + 1) * lanes
                    ]

    near_first = [0] + [sign * reach for reach in range(1, REACH + 1) for sign in (1, -1)]
    with jax.named_scope('w_ask'):
        asks(1, 1).wait_recv()
    evaluate(0, 0, 1)
    reply(0, 0).start()
    with jax.named_scope('w_ask'):
        with_partners(lambda many: asks(many - 1, 2).wait_recv())
    for shift in near_first[1:]:
        evaluate(shift, 0, 1)
    for shift in near_first[1:]:

        @pl.when(inside(slab - shift))
        def _():
            reply(shift, 0).start()

    turns_left = list(range(slots))

    def serve_rest(many):
        for _ in range(many):
            shift = near_first[turns_left.pop(0)]

            @pl.when(inside(slab - shift))
            def _():
                with jax.named_scope('rest'):
                    evaluate(shift, 1, fields)
                reply(shift, 1).start()

    room_index = lax.broadcasted_iota(jnp.int32, (room, lanes), 0)
    plans = []
    for slot in range(slots):
        table = ranks[slot * height : (slot + 1) * height, :]
        base = jnp.broadcast_to(table[0:1], (room, lanes))
        first = jnp.minimum(base >> row_bits, half - 1)
        second = jnp.minimum(first + 1, half - 1)
        offset = base & (height - 1)
        spots = table & (height - 1)
        plans.append((first, second, offset, spots))

    serve_rest(2)
    with jax.named_scope('w_reply'):
        with_partners(lambda many: replies(many, 0).wait_recv())

    def along_lanes(tile, index):
        return jnp.take_along_axis(tile, index, axis=1, mode="promise_in_bounds")

    def along_rows(tile, index):
        return jnp.take_along_axis(tile, index, axis=0, mode="promise_in_bounds")

    def gather_field(field):
        result = [jnp.zeros((room, lanes), jnp.float32)] * 2
        for slot in range(slots):
            packed = answered[slot, field]
            first, second, offset, spots = plans[slot]
            windows = [
                jnp.where(
                    room_index + part * room >= offset,
                    along_lanes(packed, first + part * half),
                    along_lanes(packed, second + part * half),
                )
                for part in range(2)
            ]
            for part in range(2):
                spot = spots[part * room : (part + 1) * room]
                member = members[slot][part * room : (part + 1) * room]
                low, high = [along_rows(window, spot & (room - 1)) for window in windows]
                tile = jnp.where(spot < room, low, high)
                result[part] = jnp.where(member, tile, result[part])
        return jnp.concatenate(result, 0)

    values = [gather_field(0)]
    groups = lanes // 64
    rows = jnp.concatenate([values[0][:, t * 64 : (t + 1) * 64] for t in range(groups)], 0)
    per_side = height // 2
    row = lax.broadcasted_iota(jnp.int32, (groups * height, elems), 0)
    spot = lax.broadcasted_iota(jnp.int32, (groups * height, elems), 1)
    piece = row % height
    target = (groups * (piece % per_side) + row // height) * EX + (EX - 1) * (piece // per_side)
    placed = lax.dot_general(
        rows,
        flag(spot == target),
        (((0,), (0,)), ((), ())),
        precision=lax.Precision.HIGHEST,
        preferred_element_type=jnp.float32,
    ).reshape(8, 8, elems)
    rim[0] = placed[0]
    rim[1] = placed[7]
    for at in range(4):

        @pl.when(rim_sends[at])
        def _():
            rim_copy(at).start()

    def spread_out(column):
        return plane_sum(
            jnp.concatenate(
                [
                    (jnp.broadcast_to(column[j : j + 1, :], (8, elems)) * mark)[None]
                    for j in range(8)
                ],
                0,
            )
        )

    def in_plane(tile, along):
        along_y = along_y_ref[0] * tile[0:1]
        for j in range(1, 8):
            along_y = along_y + along_y_ref[j] * tile[j : j + 1]
        along_x = along_x_ref[0] * tile
        for step in range(1, 8):
            along_x = along_x + along_x_ref[step] * pltpu.roll(tile, step, 1)
        return along[0] * along_x + along[1] * along_y

    def inner_z(read, layer):
        total = read(1) * float(stiff[layer, 1])
        for k in range(2, 7):
            total = total + read(k) * float(stiff[layer, k])
        return total

    def outer_z(low, high, layer):
        return low * float(stiff[layer, 0]) + high * float(stiff[layer, 7])

    here = (g_x, g_y, g_z, g_m)
    edge = weights(0)

    for layer in ORDER:
        boundary[layer] = spread_out(placed[layer]) * sharing[layer]
    loads[6].wait()
    for layer in ORDER:
        along_z = inner_z(lambda k: boundary[k], layer)
        along_z = along_z + outer_z(boundary[0], boundary[7], layer)
        tile = boundary[layer]
        total = in_plane(tile, here) + g_z * along_z + g_m * (tile - forcing_ref[layer])
        total = weights(layer) * total
        if layer in (0, 7):
            total = plane_sum(total)
        residual[layer] = total
        if layer == 7:
            faces[0, 0] = residual[0]
            faces[0, 1] = residual[7]
            send_faces(0)

    beyond = []
    for side in range(2):

        @pl.when(near[side])
        def _():
            geometry_copy(side == 0).wait_recv()

        along = [geometry_halo[side, d : d + 1, :] for d in range(4)]
        own = boundary[0 if side == 0 else 7]
        term = in_plane(own, along)
        term = term + (along[2] * float(stiff[0, 0]) + along[3]) * own
        beyond.append((term, along[2] * float(stiff[0, 7])))
        walls = wall_plane + wall_marks([geometry_halo[side, 4:5, :], geometry_halo[side, 5:6, :]])
        layer, facing = (0, 7) if side == 0 else (7, 0)
        settle(layer, z_counts[side], walls, diagonal(here, layer) + diagonal(along, facing))
    serve_rest(1)

    with jax.named_scope('w_rim'):
        with_partners(lambda many: rims(many - 1).wait_recv())

    low = spread_out(rim_halo[0]) * sharing[0]
    high = spread_out(rim_halo[1]) * sharing[7]
    boundary[0] = boundary[0] + low
    boundary[7] = boundary[7] + high
    for layer in range(1, 7):
        more = weights(layer) * (g_z * outer_z(low, high, layer))
        residual[layer] = -free[layer] * plane_sum(residual[layer] + more)
        rho[layer] = residual[layer]
        vectors[0, layer] = inverse[layer] * residual[layer]
    half_share = 0.5 / plane_count
    ends = []
    for side, (own, layer) in enumerate(((low, 0), (high, 7))):
        more = in_plane(own, here) + g_m * own + g_z * outer_z(low, high, layer)
        term, across_z = beyond[side]
        more = more + term + across_z * (spread_out(rim_halo[2 + side]) * half_share)
        ends.append(residual[layer] + plane_sum(edge * more))

    def prepare_outer(turn):
        for layer in (0, 7):
            partial[layer] = g_z * inner_z(lambda k: vectors[turn, k], layer)

    def prepare_inner(turn):
        for layer in range(1, 7):
            tile = vectors[turn, layer]
            along_z = inner_z(lambda k: vectors[turn, k], layer)
            partial[layer] = in_plane(tile, here) + g_m * tile + g_z * along_z

    def prepare(turn):
        prepare_outer(turn)
        prepare_inner(turn)

    prepare(0)
    with jax.named_scope('w_f2'):
        wait_faces(0)
    for side, layer in ((0, 0), (1, 7)):
        residual[layer] = -free[layer] * (ends[side] + halo[0, side])
        rho[layer] = residual[layer]
        vectors[0, layer] = inverse[layer] * residual[layer]

    sums = {}

    def gather_sum(key, value):
        value = jnp.sum(value, axis=0)
        sums[key] = value if key not in sums else sums[key] + value

    def outer_tiles(turn):
        low = vectors[turn, 0]
        high = vectors[turn, 7]
        tiles = {}
        for layer in (0, 7):
            tile = vectors[turn, layer]
            total = in_plane(tile, here) + g_m * tile + g_z * outer_z(low, high, layer)
            tiles[layer] = edge * (total + partial[layer])
            images[turn, layer] = plane_sum(tiles[layer])
        return tiles

    def inner_tiles(turn, tiles):
        low = vectors[turn, 0]
        high = vectors[turn, 7]
        for layer in range(8):
            if layer in tiles:
                tile = tiles[layer]
            else:
                tile = partial[layer] + g_z * outer_z(low, high, layer)
                tile = weights(layer) * tile
            for other_turn in range(turn + 1):
                gather_sum((other_turn, turn), tile * vectors[other_turn, layer])
            gather_sum(turn, vectors[turn, layer] * residual[layer] * sharing[layer])
            if layer not in tiles:
                last = turn == ITERS - 1
                images[turn, layer] = tile if last else free[layer] * plane_sum(tile)

    def advance(turn, layers):
        for layer in layers:
            rho[layer] = images[turn, layer] - SHIFTS[turn] * rho[layer]
            vectors[turn + 1, layer] = inverse[layer] * rho[layer]

    sides = ((0, 0), (1, 7))
    tiles = outer_tiles(0)
    guesses = []
    for side, layer in sides:
        faces[1, side] = images[0, layer]
        far_faces[side] = inverse[layer] * images[0, layer]
    send_faces(1)
    send_far()
    for side, layer in sides:
        guesses.append(inverse[layer] * (images[0, layer] - SHIFTS[0] * rho[layer]))
    inner_tiles(0, tiles)
    advance(0, range(1, 7))
    prepare_outer(1)
    for side, layer in sides:
        faces[2, side] = partial[layer] + g_z * (guesses[1 - side] * float(stiff[0, 7]))
    send_faces(2)
    prepare_inner(1)
    serve_rest(WINDOW)
    with jax.named_scope('w_fc'):
        wait_faces(1)
        wait_far()
        wait_faces(2)
    for side, layer in sides:
        images[0, layer] = free[layer] * (images[0, layer] + halo[1, side])
    advance(0, (0, 7))
    tiles = outer_tiles(1)
    for side, layer in sides:
        along = [geometry_halo[side, d : d + 1, :] for d in range(4)]
        own = vectors[1, layer]
        term = in_plane(own, along) + (along[2] * float(stiff[0, 0]) + along[3]) * own
        term = term + halo[2, side] + (along[2] * float(stiff[0, 7])) * far_halo[side]
        images[1, layer] = free[layer] * (images[1, layer] + plane_sum(edge * term))
    inner_tiles(1, tiles)
    advance(1, range(8))
    prepare(2)
    tiles = outer_tiles(2)
    for side, layer in sides:
        faces[ITERS, side] = images[2, layer]
    send_faces(ITERS)
    inner_tiles(2, tiles)

    keys = list(range(ITERS)) + [(a, b) for b in range(ITERS) for a in range(b + 1)]
    spot = lax.broadcasted_iota(jnp.int32, (1, 128), 1)
    packed = jnp.zeros((1, 128), jnp.float32)
    for at, key in enumerate(keys):
        value = jnp.sum(jnp.sum(sums[key], axis=0, keepdims=True), axis=1, keepdims=True)
        packed = jnp.where(spot == at, value, packed)
    dots[...] = packed
    for step in range(1, n):
        dot_copy(step).start()
    all_dots[slab] = dots[...]
    with jax.named_scope('w_rest'):
        with_partners(lambda many: replies(many, 1).wait_recv())

    values = values + [gather_field(field) for field in range(1, fields)]
    for row in range(height):
        interface_ref[:, row * lanes : (row + 1) * lanes] = jnp.concatenate(
            [value[row : row + 1] for value in values], 0
        )
    for layer in range(1, 7):
        images[ITERS - 1, layer] = free[layer] * plane_sum(images[ITERS - 1, layer])
    with jax.named_scope('w_fc'):
        wait_faces(ITERS)
    for side, layer in ((0, 0), (1, 7)):
        images[ITERS - 1, layer] = free[layer] * (
            images[ITERS - 1, layer] + halo[ITERS, side]
        )
    with jax.named_scope('w_dots'):
        all_dot_copies().wait_recv()
    with jax.named_scope('solve'):
        total = jnp.sum(all_dots[...], axis=0)
        found = {
            key: jnp.broadcast_to(total[:, at : at + 1], (8, elems))
            for at, key in enumerate(keys)
        }
        steps_taken = solve(found)
    for layer in range(8):
        moved = boundary[layer]
        for turn in range(ITERS):
            moved = moved + steps_taken[turn] * vectors[turn, layer]
        velocity[layer] = moved
    for layer in range(8):
        left_over = residual[layer]
        for turn in range(ITERS):
            left_over = left_over - steps_taken[turn] * images[turn, layer]
        residual_out[layer] = left_over
    all_dot_copies().wait_send()
    for side in range(2):

        @pl.when(near[1 - side])
        def _():
            geometry_copy(side == 0).wait_send()

    with_partners(lambda many: rims(many - 1).wait_send())
    with_partners(lambda many: asks(many, 1).wait_send())
    for part in range(2):
        with_partners(lambda many: replies(many, part).wait_send())


def flush(*refs):
    count = (len(refs) - 1) // 2
    sem = refs[-1]
    copies = [
        pltpu.make_async_copy(refs[at], refs[count + at], sem.at[at]) for at in range(count)
    ]
    for copy in copies:
        copy.start()
    for copy in copies:
        copy.wait()


def body(n, donor_fields, interp_weights, donor_owner, donor_element, geometry, wall_flag, forcing):
    fields = donor_fields.shape[0]
    elems = geometry.shape[1]
    receptors = donor_element.shape[0]
    slots = 2 * REACH + 1
    lanes = 128
    count = receptors // lanes
    cube = (8, 8, 8, elems)
    phases = 1 + ITERS
    room = count // 2
    vmem = pl.BlockSpec(memory_space=pltpu.VMEM)
    hbm = pl.BlockSpec(memory_space=pltpu.HBM)
    shapes = (
        jax.ShapeDtypeStruct(cube, jnp.float32),
        jax.ShapeDtypeStruct(cube, jnp.float32),
        jax.ShapeDtypeStruct((fields, receptors), jnp.float32),
    )
    outputs = pl.pallas_call(
        functools.partial(kernel, n),
        out_shape=shapes,
        in_specs=[hbm] * 7,
        out_specs=(vmem, vmem, vmem),
        scratch_shapes=[
            pltpu.VMEM(cube, jnp.float32),
            pltpu.VMEM((fields, 512, elems), jnp.float32),
            pltpu.VMEM(cube, jnp.float32),
            pltpu.VMEM(interp_weights.shape, jnp.float32),
            pltpu.VMEM((count, lanes), jnp.int32),
            pltpu.VMEM((count, lanes), jnp.int32),
            pltpu.VMEM(geometry.shape, jnp.float32),
            pltpu.VMEM(wall_flag.shape, jnp.int32),
            pltpu.VMEM((3, count, lanes), jnp.float32),
            pltpu.VMEM((slots, 4, room, lanes), jnp.float32),
            pltpu.VMEM((slots * count, lanes), jnp.int32),
            pltpu.VMEM(cube, jnp.float32),
            pltpu.VMEM((8, 8, elems), jnp.float32),
            pltpu.VMEM((8, 8, elems), jnp.float32),
            pltpu.SemaphoreType.DMA((7,)),
            pltpu.VMEM((fields * 512, 2 * elems), jnp.bfloat16),
            pltpu.VMEM((slots, 4, room, lanes), jnp.float32),
            pltpu.VMEM((slots, fields, room, lanes), jnp.float32),
            pltpu.VMEM((slots, fields, room, lanes), jnp.float32),
            pltpu.VMEM((phases, 2, 8, 8, elems), jnp.float32),
            pltpu.VMEM((phases, 2, 8, 8, elems), jnp.float32),
            pltpu.VMEM((1, 128), jnp.float32),
            pltpu.VMEM((n, 1, 128), jnp.float32),
            pltpu.VMEM((ITERS,) + cube, jnp.float32),
            pltpu.VMEM((ITERS,) + cube, jnp.float32),
            pltpu.VMEM(cube, jnp.float32),
            pltpu.VMEM(cube, jnp.float32),
            pltpu.VMEM((2, 8, elems), jnp.float32),
            pltpu.VMEM((4, 8, elems), jnp.float32),
            pltpu.VMEM((2, 8, elems), jnp.float32),
            pltpu.VMEM((8, elems), jnp.float32),
            pltpu.VMEM((2, 8, 8, elems), jnp.float32),
            pltpu.VMEM((2, 8, 8, elems), jnp.float32),
        ]
        + [pltpu.VMEM(cube, jnp.float32)] * 4
        + [pltpu.SemaphoreType.DMA((3,)), pltpu.SemaphoreType.DMA((2, 2))]
        + [pltpu.SemaphoreType.DMA((3, 2))] * 2
        + [pltpu.SemaphoreType.DMA((2, 2))]
        + [pltpu.SemaphoreType.DMA((2,))]
        + [pltpu.SemaphoreType.DMA((2,))]
        + [pltpu.SemaphoreType.DMA((2,))] * 2,
        compiler_params=pltpu.CompilerParams(
            collective_id=0, has_side_effects=True, vmem_limit_bytes=48 * 1024 * 1024
        ),
    )(
        *[
            pltpu.with_memory_space_constraint(array, pltpu.HBM)
            for array in (
                donor_fields,
                interp_weights,
                donor_owner.reshape(count, lanes),
                donor_element.reshape(count, lanes),
                geometry,
                wall_flag,
                forcing.reshape(cube),
            )
        ]
    )
    velocity, residual, interface = pl.pallas_call(
        flush,
        out_shape=shapes,
        in_specs=[vmem] * 3,
        out_specs=(hbm,) * 3,
        scratch_shapes=[pltpu.SemaphoreType.DMA((3,))],
        compiler_params=pltpu.CompilerParams(vmem_limit_bytes=1024 * 1024),
    )(*outputs)
    return (velocity.reshape(512, elems), residual.reshape(512, elems), interface)


def solution(mesh):
    in_specs = (
        P(None, None, ("mesh", "dom")),
        P(None, None, ("mesh", "dom")),
        P(("mesh", "dom"), None),
        P(("mesh", "dom")),
        P(None, ("mesh", "dom")),
        P(None, ("mesh", "dom")),
        P(None, ("mesh", "dom")),
    )
    out_specs = (P(None, ("mesh", "dom")), P(None, ("mesh", "dom")), P(None, ("mesh", "dom")))
    return jax.shard_map(
        functools.partial(body, mesh.shape["dom"]),
        mesh=mesh,
        in_specs=in_specs,
        out_specs=out_specs,
        check_vma=False,
    )
```

```python
import functools

import jax
import jax.numpy as jnp
import numpy as np
from jax import lax
from jax.experimental import pallas as pl
from jax.experimental.pallas import tpu as pltpu
from jax.sharding import PartitionSpec as P

EX = 8
EY = 16
ITERS = 3
REACH = 2
CHUNK = 256
ORDER = (0, 7, 1, 2, 3, 4, 5, 6)
SHIFTS = (1.5, 0.5)
WINDOW = 2
MESH = pl.DeviceIdType.MESH


def legendre_pair(values, degree):
    previous = values * 0.0 + 1.0
    current = values * 1.0
    for poly_order in range(2, degree + 1):
        previous, current = (
            current,
            ((2 * poly_order - 1) * values * current - (poly_order - 1) * previous) / poly_order,
        )
    return (current, previous)


def gll_tables():
    degree = 7
    points_count = degree + 1
    abscissae = np.cos(np.pi * np.arange(points_count) / degree)
    for newton_turn in range(80):
        top_poly, lower_poly = legendre_pair(abscissae, degree)
        abscissae = abscissae - (abscissae * top_poly - lower_poly) / (points_count * top_poly)
    abscissae = np.sort(abscissae)
    top_poly, lower_poly = legendre_pair(abscissae, degree)
    quad_weights = 2.0 / (degree * points_count * top_poly * top_poly)
    identity_mat = np.eye(points_count)
    spacing = abscissae[:, None] - abscissae[None, :] + identity_mat
    derivative = top_poly[:, None] / (top_poly[None, :] * spacing) * (1.0 - identity_mat)
    derivative[0, 0] = -degree * points_count / 4.0
    derivative[degree, degree] = degree * points_count / 4.0
    return (abscissae, derivative, quad_weights)


def solve(found):
    matrix = [
        [found[(min(a, b), max(a, b))] for b in range(ITERS)] for a in range(ITERS)
    ]
    right = [found[a] for a in range(ITERS)]
    pivots = []
    for a in range(ITERS):
        pivots.append(1.0 / matrix[a][a])
        for b in range(a + 1, ITERS):
            factor = matrix[b][a] * pivots[a]
            for c in range(a + 1, ITERS):
                matrix[b][c] = matrix[b][c] - factor * matrix[a][c]
            right[b] = right[b] - factor * right[a]
    answer = [None] * ITERS
    for a in reversed(range(ITERS)):
        total = right[a]
        for b in range(a + 1, ITERS):
            total = total - matrix[a][b] * answer[b]
        answer[a] = total * pivots[a]
    return answer


def kernel(
    n,
    donor_hbm,
    weights_hbm,
    owner_hbm,
    element_hbm,
    geometry_hbm,
    wall_hbm,
    forcing_hbm,
    velocity,
    residual_out,
    interface_ref,
    residual,
    donor_ref,
    forcing_ref,
    weights_ref,
    owner_ref,
    element_ref,
    geometry_ref,
    wall_ref,
    position_ref,
    request_ref,
    ranks,
    along_y_ref,
    along_x_ref,
    plane_ref,
    load_sem,
    split,
    asked,
    answer,
    answered,
    faces,
    halo,
    dots,
    all_dots,
    vectors,
    images,
    partial,
    rho,
    rim,
    rim_halo,
    geometry_halo,
    packet,
    far_faces,
    far_halo,
    inverse,
    free,
    sharing,
    boundary,
    ask_sem,
    reply_sem,
    face_send,
    face_recv,
    far_sem,
    dot_sem,
    rim_sem,
    geometry_send,
    geometry_recv,
):
    points, derivative, quad = gll_tables()
    stiff = (derivative.T * quad) @ derivative / quad[:, None]
    fields = donor_ref.shape[0]
    elems = donor_ref.shape[2]
    height = owner_ref.shape[0]
    lanes = owner_ref.shape[1]
    receptors = height * lanes
    room = request_ref.shape[2]
    slots = 2 * REACH + 1
    mesh_id = lax.axis_index("mesh")
    slab = lax.axis_index("dom")
    other = 1 - mesh_id

    pairs = [
        (weights_hbm, weights_ref),
        (owner_hbm, owner_ref),
        (element_hbm, element_ref),
        (donor_hbm, donor_ref),
        (geometry_hbm, geometry_ref),
        (wall_hbm, wall_ref),
        (forcing_hbm, forcing_ref),
    ]
    loads = [
        pltpu.make_async_copy(source, target, load_sem.at[at])
        for at, (source, target) in enumerate(pairs)
    ]
    for load in loads:
        load.start()

    def inside(index):
        return jnp.logical_and(index >= 0, index < n)

    barrier = pltpu.get_barrier_semaphore()
    greeted = n - 1
    for step in range(1, n):
        pl.semaphore_signal(
            barrier, inc=1, device_id=(mesh_id, lax.rem(slab + step, n)), device_id_type=MESH
        )
    for shift in range(-REACH, REACH + 1):
        greeted = greeted + jnp.where(inside(slab + shift), 1, 0)

        @pl.when(inside(slab + shift))
        def _():
            pl.semaphore_signal(
                barrier, inc=1, device_id=(other, slab + shift), device_id_type=MESH
            )

    with jax.named_scope('w_loads'):
        for load in loads[:3]:
            load.wait()
    depth = lax.broadcasted_iota(jnp.int32, (8, lanes), 0)
    ladder = jnp.zeros((8, lanes), jnp.float32)
    for a in range(8):
        ladder = jnp.where(depth == a, float(points[a]), ladder)
    for d in range(3):
        for row in range(height):
            part = weights_ref[d, :, row * lanes : (row + 1) * lanes] * ladder
            position_ref[d, row : row + 1, :] = jnp.sum(part, axis=0, keepdims=True)
    owner = owner_ref[...]
    element_code = element_ref[...] * receptors
    members = [owner == slab + shift for shift in range(-REACH, REACH + 1)]
    tall = slots * height
    marks = jnp.concatenate([jnp.where(m, 1.0, 0.0) for m in members], 0).astype(jnp.bfloat16)
    before = lax.broadcasted_iota(jnp.int32, (lanes, lanes), 0)
    after = lax.broadcasted_iota(jnp.int32, (lanes, lanes), 1)
    upper = jnp.where(before < after, 1.0, 0.0).astype(jnp.bfloat16)
    left = jnp.dot(marks, upper, preferred_element_type=jnp.float32).astype(jnp.bfloat16)
    above = lax.broadcasted_iota(jnp.int32, (tall, tall), 0)
    below = lax.broadcasted_iota(jnp.int32, (tall, tall), 1)
    same = above // height == below // height
    block = jnp.where(same, 1.0, 0.0).astype(jnp.bfloat16)
    lower = jnp.where(same & (below < above), 1.0, 0.0).astype(jnp.bfloat16)
    rank = jnp.dot(block, left, preferred_element_type=jnp.float32)
    rank = rank + jnp.dot(lower, marks, preferred_element_type=jnp.float32)
    rank = rank.astype(jnp.int32)
    ranks[...] = rank
    row_index = lax.broadcasted_iota(jnp.int32, (height, lanes), 0)
    place = lax.broadcasted_iota(jnp.int32, (height, lanes), 1) * height + row_index
    row_bits = height.bit_length() - 1
    steps = receptors.bit_length() - 1

    def pull(tile, step):
        if step >= row_bits:
            return pltpu.roll(tile, lanes - (1 << (step - row_bits)), 1)
        jump = 1 << step
        near = pltpu.roll(tile, height - jump, 0)
        far = pltpu.roll(near, lanes - 1, 1)
        return jnp.where(row_index < height - jump, near, far)

    words = []
    comps = []
    start = [position_ref[d] for d in range(3)]
    for slot in range(slots):
        shift = place - rank[slot * height : (slot + 1) * height]
        words.append(jnp.where(members[slot], element_code + shift, 0))
        comps.append(list(start))
    for step in range(steps):
        for slot in range(slots):
            word = words[slot]
            moving = word & (1 << step)
            came = pull(word, step)
            take = (came & (1 << step)) != 0
            words[slot] = jnp.where(take, came - (1 << step), jnp.where(moving != 0, 0, word))
            comps[slot] = [jnp.where(take, pull(c, step), c) for c in comps[slot]]
    half = lanes // 2
    left_half = lax.broadcasted_iota(jnp.int32, (room, lanes), 1) < half
    for slot in range(slots):
        columns = comps[slot] + [(words[slot] >> steps).astype(jnp.float32)]
        for at, column in enumerate(columns):
            request_ref[slot, at] = jnp.where(
                left_half, column[:room], pltpu.roll(column[room:], half, 1)
            )

    with jax.named_scope('w_barrier'):
        pl.semaphore_wait(barrier, greeted)

    def ask(shift):
        return pltpu.make_async_remote_copy(
            src_ref=request_ref.at[shift + REACH],
            dst_ref=asked.at[shift + REACH],
            send_sem=ask_sem.at[0],
            recv_sem=ask_sem.at[1 if shift == 0 else 2],
            device_id=(other, lax.rem(slab + shift + n, n)),
            device_id_type=MESH,
        )

    def reply(shift, part):
        span = pl.ds(0, 1) if part == 0 else pl.ds(1, fields - 1)
        return pltpu.make_async_remote_copy(
            src_ref=answer.at[shift + REACH, span],
            dst_ref=answered.at[shift + REACH, span],
            send_sem=reply_sem.at[0, part],
            recv_sem=reply_sem.at[1, part],
            device_id=(other, lax.rem(slab - shift + n, n)),
            device_id_type=MESH,
        )

    def asks(many, sem):
        return pltpu.make_async_remote_copy(
            src_ref=asked.at[pl.ds(0, many)],
            dst_ref=asked.at[pl.ds(0, many)],
            send_sem=ask_sem.at[0],
            recv_sem=ask_sem.at[sem],
            device_id=(other, slab),
            device_id_type=MESH,
        )

    def replies(many, part):
        span = pl.ds(0, 1) if part == 0 else pl.ds(1, fields - 1)
        return pltpu.make_async_remote_copy(
            src_ref=answered.at[pl.ds(0, many), span],
            dst_ref=answered.at[pl.ds(0, many), span],
            send_sem=reply_sem.at[0, part],
            recv_sem=reply_sem.at[1, part],
            device_id=(other, slab),
            device_id_type=MESH,
        )

    partners = 0
    for shift in range(-REACH, REACH + 1):
        partners = partners + jnp.where(inside(slab + shift), 1, 0)

    def with_partners(action):
        for many in range(REACH + 1, slots + 1):

            @pl.when(partners == many)
            def _():
                action(many)

    def face_copy(phase, up):
        step = 1 if up else n - 1
        return pltpu.make_async_remote_copy(
            src_ref=faces.at[phase, 1 if up else 0],
            dst_ref=halo.at[phase, 0 if up else 1],
            send_sem=face_send.at[phase % 3, 1 if up else 0],
            recv_sem=face_recv.at[phase % 3, 0 if up else 1],
            device_id=(mesh_id, lax.rem(slab + step, n)),
            device_id_type=MESH,
        )

    def send_faces(phase):
        @pl.when(slab < n - 1)
        def _():
            face_copy(phase, True).start()

        @pl.when(slab > 0)
        def _():
            face_copy(phase, False).start()

    def wait_faces(phase):
        @pl.when(slab > 0)
        def _():
            face_copy(phase, True).wait_recv()

        @pl.when(slab < n - 1)
        def _():
            face_copy(phase, False).wait_recv()

        @pl.when(slab < n - 1)
        def _():
            face_copy(phase, True).wait_send()

        @pl.when(slab > 0)
        def _():
            face_copy(phase, False).wait_send()

    def dot_copy(step):
        return pltpu.make_async_remote_copy(
            src_ref=dots,
            dst_ref=all_dots.at[slab],
            send_sem=dot_sem.at[0],
            recv_sem=dot_sem.at[1],
            device_id=(mesh_id, lax.rem(slab + step, n)),
            device_id_type=MESH,
        )

    def far_copy(up):
        side = 0 if up else 1
        return pltpu.make_async_remote_copy(
            src_ref=far_faces.at[1 - side],
            dst_ref=far_halo.at[side],
            send_sem=far_sem.at[0, side],
            recv_sem=far_sem.at[1, side],
            device_id=(mesh_id, lax.rem(slab + (2 if up else n - 2), n)),
            device_id_type=MESH,
        )

    above_far = slab < n - 2
    below_far = slab > 1

    def send_far():
        @pl.when(above_far)
        def _():
            far_copy(True).start()

        @pl.when(below_far)
        def _():
            far_copy(False).start()

    def wait_far():
        @pl.when(below_far)
        def _():
            far_copy(True).wait_recv()

        @pl.when(above_far)
        def _():
            far_copy(False).wait_recv()

        @pl.when(above_far)
        def _():
            far_copy(True).wait_send()

        @pl.when(below_far)
        def _():
            far_copy(False).wait_send()

    def all_dot_copies():
        return pltpu.make_async_remote_copy(
            src_ref=all_dots.at[pl.ds(0, n - 1)],
            dst_ref=all_dots.at[pl.ds(0, n - 1)],
            send_sem=dot_sem.at[0],
            recv_sem=dot_sem.at[1],
            device_id=(mesh_id, lax.rem(slab + 1, n)),
            device_id_type=MESH,
        )

    rim_jumps = (1, -1, 2, -2)
    rim_sends = [inside(slab + jump) for jump in rim_jumps]
    rim_comes = [inside(slab - jump) for jump in rim_jumps]
    near = (slab > 0, slab < n - 1)

    def rim_copy(at):
        return pltpu.make_async_remote_copy(
            src_ref=rim.at[1 - at % 2],
            dst_ref=rim_halo.at[at],
            send_sem=rim_sem.at[0],
            recv_sem=rim_sem.at[1],
            device_id=(mesh_id, lax.rem(slab + rim_jumps[at] + n, n)),
            device_id_type=MESH,
        )

    def rims(many):
        return pltpu.make_async_remote_copy(
            src_ref=rim_halo.at[pl.ds(0, many)],
            dst_ref=rim_halo.at[pl.ds(0, many)],
            send_sem=rim_sem.at[0],
            recv_sem=rim_sem.at[1],
            device_id=(mesh_id, lax.rem(slab + 1, n)),
            device_id_type=MESH,
        )

    def geometry_copy(up):
        side = 0 if up else 1
        return pltpu.make_async_remote_copy(
            src_ref=packet,
            dst_ref=geometry_halo.at[side],
            send_sem=geometry_send.at[side],
            recv_sem=geometry_recv.at[side],
            device_id=(mesh_id, lax.rem(slab + (1 if up else n - 1), n)),
            device_id_type=MESH,
        )

    for distance in range(REACH + 1):
        for shift in sorted({distance, -distance}):

            @pl.when(inside(slab + shift))
            def _():
                ask(shift).start()

    phases = halo.shape[0]
    blank = jnp.zeros(halo.shape[2:], jnp.float32)

    for shift in range(-REACH, REACH + 1):

        @pl.when(jnp.logical_not(inside(slab + shift)))
        def _():
            answered[shift + REACH] = jnp.zeros(answered.shape[1:], jnp.float32)

        @pl.when(jnp.logical_not(inside(slab - shift)))
        def _():
            asked[shift + REACH] = jnp.zeros(asked.shape[1:], jnp.float32)

    for at in range(4):

        @pl.when(jnp.logical_not(rim_comes[at]))
        def _():
            rim_halo[at] = jnp.zeros(rim_halo.shape[1:], jnp.float32)

    for side in range(2):

        @pl.when(jnp.logical_not(near[side]))
        def _():
            geometry_halo[side] = jnp.zeros(geometry_halo.shape[1:], jnp.float32)

    @pl.when(jnp.logical_not(below_far))
    def _():
        far_halo[0] = blank

    @pl.when(jnp.logical_not(above_far))
    def _():
        far_halo[1] = blank

    @pl.when(slab == 0)
    def _():
        for phase in range(phases):
            halo[phase, 0] = blank

    @pl.when(slab == n - 1)
    def _():
        for phase in range(phases):
            halo[phase, 1] = blank

    node = lax.broadcasted_iota(jnp.int32, (8, elems), 0)
    element = lax.broadcasted_iota(jnp.int32, (8, elems), 1)
    x_index = element % EX
    y_index = element // EX % EY

    across = jnp.zeros((8, elems), jnp.float32)
    for a in range(8):
        across = jnp.where(node == a, float(quad[a]), across)
    for j in range(8):
        plane_ref[j] = across * float(quad[j])
        for m in range(8):
            along_y_ref[m, j] = jnp.full((8, elems), float(stiff[j, m]), jnp.float32)
    for step in range(8):
        turned = jnp.zeros((8, elems), jnp.float32)
        for i in range(8):
            turned = jnp.where(node == i, float(stiff[i, (i - step) % 8]), turned)
        along_x_ref[step] = turned

    def flag(condition):
        return jnp.where(condition, 1.0, 0.0)

    x_low = flag((node == 0) & (x_index > 0))
    x_high = flag((node == 7) & (x_index < EX - 1))
    y_low = flag(y_index > 0)
    y_high = flag(y_index < EY - 1)

    def plane_sum(tile):
        below = pltpu.roll(pltpu.roll(tile, 1, 1), 1, 2)
        above = pltpu.roll(pltpu.roll(tile, 7, 1), elems - 1, 2)
        tile = tile + below * x_low + above * x_high
        low = tile[0] + y_low * pltpu.roll(tile[7], EX, 1)
        high = tile[7] + y_high * pltpu.roll(tile[0], elems - EX, 1)
        return jnp.concatenate([low[None], tile[1:7], high[None]], 0)

    def weights(layer):
        return plane_ref[...] * float(quad[layer])

    loads[4].wait()
    loads[5].wait()

    wall_rows = []
    for side in range(2):
        wall_row = jnp.zeros((1, elems), jnp.float32)
        for x in range(EX):
            bit = wall_ref[side : side + 1, x : x + 1].astype(jnp.float32)
            wall_row = jnp.where(x_index[0:1] == x, bit, wall_row)
        wall_rows.append(wall_row)
    g_x, g_y, g_z, g_m = [geometry_ref[d : d + 1, :] for d in range(4)]

    packet[...] = jnp.concatenate(
        [geometry_ref[...]] + wall_rows + [jnp.zeros((2, elems), jnp.float32)], 0
    )

    @pl.when(near[1])
    def _():
        geometry_copy(True).start()

    @pl.when(near[0])
    def _():
        geometry_copy(False).start()

    diag_y = [jnp.full((8, elems), float(stiff[j, j]), jnp.float32)[None] for j in range(8)]
    diag_y = jnp.concatenate(diag_y, 0)

    def diagonal(along, layer):
        total = along[0] * along_x_ref[0] + along[1] * diag_y
        total = total + (along[2] * float(stiff[layer, layer]) + along[3])
        return plane_sum(weights(layer) * total)

    nothing = jnp.zeros((6, 8, elems), jnp.float32)

    def wall_marks(rows):
        low_wall = flag(y_index == 0) * rows[0]
        high_wall = flag(y_index == EY - 1) * rows[1]
        return plane_sum(jnp.concatenate([low_wall[None], nothing, high_wall[None]], 0))

    wall_plane = wall_marks(wall_rows)
    x_count = 1.0 + x_low + x_high
    y_count_low = 1.0 + y_low
    y_count_high = 1.0 + y_high
    plane_count = jnp.concatenate(
        [(x_count * y_count_low)[None]]
        + [x_count[None]] * 6
        + [(x_count * y_count_high)[None]],
        0,
    )
    mark = flag((node == 0) & (x_index == 0)) + flag((node == 7) & (x_index == EX - 1))

    def settle(layer, z_count, walls, diag):
        count = plane_count * z_count
        open_part = 1.0 - jnp.minimum(mark * count + walls, 1.0)
        sharing[layer] = 1.0 / count
        free[layer] = open_part
        inverse[layer] = open_part / diag

    for layer in range(1, 7):
        settle(layer, 1.0, wall_plane, diagonal((g_x, g_y, g_z, g_m), layer))
    z_counts = (jnp.where(slab > 0, 2.0, 1.0), jnp.where(slab < n - 1, 2.0, 1.0))
    for side, layer in ((0, 0), (1, 7)):
        sharing[layer] = 1.0 / (plane_count * z_counts[side])

    with jax.named_scope('w_donor'):
        loads[3].wait()
    donors = donor_ref[...].reshape(fields * 512, elems)
    coarse = donors.astype(jnp.bfloat16)
    split[:, :elems] = coarse
    split[:, elems:] = (donors - coarse.astype(jnp.float32)).astype(jnp.bfloat16)

    code = lax.broadcasted_iota(jnp.int32, (elems, CHUNK), 0)
    code = code.astype(jnp.float32)
    basis = lax.broadcasted_iota(jnp.int32, (8, CHUNK), 0)
    norms = [
        float(1.0 / np.prod([points[a] - points[b] for b in range(8) if b != a])) for a in range(8)
    ]
    scale = jnp.zeros((8, CHUNK), jnp.float32)
    for a in range(8):
        scale = jnp.where(basis == a, norms[a], scale)

    def lagrange(position):
        value = scale
        for b in range(8):
            value = value * jnp.where(basis == b, 1.0, position - float(points[b]))
        return value

    def evaluate(shift, first, last):
        group = CHUNK // lanes
        for chunk in range(room // group):
            block = [
                jnp.concatenate(
                    [
                        asked[shift + REACH, c, chunk * group + t : chunk * group + t + 1, :]
                        for t in range(group)
                    ],
                    1,
                )
                for c in range(4)
            ]
            chosen = jnp.where(block[3] == code, 1.0, 0.0).astype(jnp.bfloat16)
            chosen = jnp.concatenate([chosen, chosen], 0)
            w_x, w_y, w_z = [lagrange(block[d]) for d in range(3)]
            picked = jnp.dot(
                split[first * 512 : last * 512], chosen, preferred_element_type=jnp.float32
            )
            for field in range(first, last):
                cube = picked[(field - first) * 512 : (field - first + 1) * 512]
                cube = cube.reshape(8, 64, CHUNK)
                total = cube[0] * w_z[0:1, :]
                for k in range(1, 8):
                    total = total + cube[k] * w_z[k : k + 1, :]
                total = total.reshape(8, 8, CHUNK)
                line = total[0] * w_y[0:1, :]
                for j in range(1, 8):
                    line = line + total[j] * w_y[j : j + 1, :]
                value = jnp.sum(line * w_x, axis=0, keepdims=True)
                for t in range(group):
                    row = chunk * group + t
                    answer[shift + REACH, field, row : row + 1, :] = value[
                        :, t * lanes : (t + 1) * lanes
                    ]

    near_first = [0] + [sign * reach for reach in range(1, REACH + 1) for sign in (1, -1)]
    with jax.named_scope('w_ask'):
        asks(1, 1).wait_recv()
    evaluate(0, 0, 1)
    reply(0, 0).start()
    with jax.named_scope('w_ask'):
        with_partners(lambda many: asks(many - 1, 2).wait_recv())
    for shift in near_first[1:]:
        evaluate(shift, 0, 1)
    for shift in near_first[1:]:

        @pl.when(inside(slab - shift))
        def _():
            reply(shift, 0).start()

    turns_left = list(range(slots))

    def serve_rest(many):
        for _ in range(many):
            shift = near_first[turns_left.pop(0)]

            @pl.when(inside(slab - shift))
            def _():
                with jax.named_scope('rest'):
                    evaluate(shift, 1, fields)
                reply(shift, 1).start()

    room_index = lax.broadcasted_iota(jnp.int32, (room, lanes), 0)
    plans = []
    for slot in range(slots):
        table = ranks[slot * height : (slot + 1) * height, :]
        base = jnp.broadcast_to(table[0:1], (room, lanes))
        first = jnp.minimum(base >> row_bits, half - 1)
        second = jnp.minimum(first + 1, half - 1)
        offset = base & (height - 1)
        spots = table & (height - 1)
        plans.append((first, second, offset, spots))

    serve_rest(2)
    with jax.named_scope('w_reply'):
        with_partners(lambda many: replies(many, 0).wait_recv())

    def along_lanes(tile, index):
        return jnp.take_along_axis(tile, index, axis=1, mode="promise_in_bounds")

    def along_rows(tile, index):
        return jnp.take_along_axis(tile, index, axis=0, mode="promise_in_bounds")

    def gather_field(field):
        result = [jnp.zeros((room, lanes), jnp.float32)] * 2
        for slot in range(slots):
            packed = answered[slot, field]
            first, second, offset, spots = plans[slot]
            windows = [
                jnp.where(
                    room_index + part * room >= offset,
                    along_lanes(packed, first + part * half),
                    along_lanes(packed, second + part * half),
                )
                for part in range(2)
            ]
            for part in range(2):
                spot = spots[part * room : (part + 1) * room]
                member = members[slot][part * room : (part + 1) * room]
                low, high = [along_rows(window, spot & (room - 1)) for window in windows]
                tile = jnp.where(spot < room, low, high)
                result[part] = jnp.where(member, tile, result[part])
        return jnp.concatenate(result, 0)

    values = [gather_field(0)]
    groups = lanes // 64
    rows = jnp.concatenate([values[0][:, t * 64 : (t + 1) * 64] for t in range(groups)], 0)
    per_side = height // 2
    row = lax.broadcasted_iota(jnp.int32, (groups * height, elems), 0)
    spot = lax.broadcasted_iota(jnp.int32, (groups * height, elems), 1)
    piece = row % height
    target = (groups * (piece % per_side) + row // height) * EX + (EX - 1) * (piece // per_side)
    pieces = []
    rest = rows
    for _ in range(3):
        piece = rest.astype(jnp.bfloat16)
        pieces.append(piece)
        rest = rest - piece.astype(jnp.float32)
    placed = lax.dot_general(
        jnp.concatenate(pieces, 0),
        jnp.concatenate([flag(spot == target).astype(jnp.bfloat16)] * 3, 0),
        (((0,), (0,)), ((), ())),
        preferred_element_type=jnp.float32,
    ).reshape(8, 8, elems)
    rim[0] = placed[0]
    rim[1] = placed[7]
    for at in range(4):

        @pl.when(rim_sends[at])
        def _():
            rim_copy(at).start()

    def spread_out(column):
        return plane_sum(
            jnp.concatenate(
                [
                    (jnp.broadcast_to(column[j : j + 1, :], (8, elems)) * mark)[None]
                    for j in range(8)
                ],
                0,
            )
        )

    def in_plane(tile, along):
        along_y = along_y_ref[0] * tile[0:1]
        for j in range(1, 8):
            along_y = along_y + along_y_ref[j] * tile[j : j + 1]
        along_x = along_x_ref[0] * tile
        for step in range(1, 8):
            along_x = along_x + along_x_ref[step] * pltpu.roll(tile, step, 1)
        return along[0] * along_x + along[1] * along_y

    def inner_z(read, layer):
        total = read(1) * float(stiff[layer, 1])
        for k in range(2, 7):
            total = total + read(k) * float(stiff[layer, k])
        return total

    def outer_z(low, high, layer):
        return low * float(stiff[layer, 0]) + high * float(stiff[layer, 7])

    here = (g_x, g_y, g_z, g_m)
    edge = weights(0)

    for layer in ORDER:
        boundary[layer] = spread_out(placed[layer]) * sharing[layer]
    loads[6].wait()
    for layer in ORDER:
        along_z = inner_z(lambda k: boundary[k], layer)
        along_z = along_z + outer_z(boundary[0], boundary[7], layer)
        tile = boundary[layer]
        total = in_plane(tile, here) + g_z * along_z + g_m * (tile - forcing_ref[layer])
        total = weights(layer) * total
        if layer in (0, 7):
            total = plane_sum(total)
        residual[layer] = total
        if layer == 7:
            faces[0, 0] = residual[0]
            faces[0, 1] = residual[7]
            send_faces(0)

    beyond = []
    for side in range(2):

        @pl.when(near[side])
        def _():
            geometry_copy(side == 0).wait_recv()

        along = [geometry_halo[side, d : d + 1, :] for d in range(4)]
        own = boundary[0 if side == 0 else 7]
        term = in_plane(own, along)
        term = term + (along[2] * float(stiff[0, 0]) + along[3]) * own
        beyond.append((term, along[2] * float(stiff[0, 7])))
        walls = wall_plane + wall_marks([geometry_halo[side, 4:5, :], geometry_halo[side, 5:6, :]])
        layer, facing = (0, 7) if side == 0 else (7, 0)
        settle(layer, z_counts[side], walls, diagonal(here, layer) + diagonal(along, facing))
    serve_rest(1)

    with jax.named_scope('w_rim'):
        with_partners(lambda many: rims(many - 1).wait_recv())

    low = spread_out(rim_halo[0]) * sharing[0]
    high = spread_out(rim_halo[1]) * sharing[7]
    boundary[0] = boundary[0] + low
    boundary[7] = boundary[7] + high
    for layer in range(1, 7):
        more = weights(layer) * (g_z * outer_z(low, high, layer))
        residual[layer] = -free[layer] * plane_sum(residual[layer] + more)
        rho[layer] = residual[layer]
        vectors[0, layer] = inverse[layer] * residual[layer]
    half_share = 0.5 / plane_count
    ends = []
    for side, (own, layer) in enumerate(((low, 0), (high, 7))):
        more = in_plane(own, here) + g_m * own + g_z * outer_z(low, high, layer)
        term, across_z = beyond[side]
        more = more + term + across_z * (spread_out(rim_halo[2 + side]) * half_share)
        ends.append(residual[layer] + plane_sum(edge * more))

    def prepare_outer(turn):
        for layer in (0, 7):
            partial[layer] = g_z * inner_z(lambda k: vectors[turn, k], layer)

    def prepare_inner(turn):
        for layer in range(1, 7):
            tile = vectors[turn, layer]
            along_z = inner_z(lambda k: vectors[turn, k], layer)
            partial[layer] = in_plane(tile, here) + g_m * tile + g_z * along_z

    def prepare(turn):
        prepare_outer(turn)
        prepare_inner(turn)

    prepare(0)
    with jax.named_scope('w_f2'):
        wait_faces(0)
    for side, layer in ((0, 0), (1, 7)):
        residual[layer] = -free[layer] * (ends[side] + halo[0, side])
        rho[layer] = residual[layer]
        vectors[0, layer] = inverse[layer] * residual[layer]

    sums = {}

    def gather_sum(key, value):
        value = jnp.sum(value, axis=0)
        sums[key] = value if key not in sums else sums[key] + value

    def outer_tiles(turn):
        low = vectors[turn, 0]
        high = vectors[turn, 7]
        tiles = {}
        for layer in (0, 7):
            tile = vectors[turn, layer]
            total = in_plane(tile, here) + g_m * tile + g_z * outer_z(low, high, layer)
            tiles[layer] = edge * (total + partial[layer])
            images[turn, layer] = plane_sum(tiles[layer])
        return tiles

    def inner_tiles(turn, tiles):
        low = vectors[turn, 0]
        high = vectors[turn, 7]
        for layer in range(8):
            if layer in tiles:
                tile = tiles[layer]
            else:
                tile = partial[layer] + g_z * outer_z(low, high, layer)
                tile = weights(layer) * tile
            for other_turn in range(turn + 1):
                gather_sum((other_turn, turn), tile * vectors[other_turn, layer])
            gather_sum(turn, vectors[turn, layer] * residual[layer] * sharing[layer])
            if layer not in tiles:
                last = turn == ITERS - 1
                images[turn, layer] = tile if last else free[layer] * plane_sum(tile)

    def advance(turn, layers):
        for layer in layers:
            rho[layer] = images[turn, layer] - SHIFTS[turn] * rho[layer]
            vectors[turn + 1, layer] = inverse[layer] * rho[layer]

    sides = ((0, 0), (1, 7))
    tiles = outer_tiles(0)
    guesses = []
    for side, layer in sides:
        faces[1, side] = images[0, layer]
        far_faces[side] = inverse[layer] * images[0, layer]
    send_faces(1)
    send_far()
    for side, layer in sides:
        guesses.append(inverse[layer] * (images[0, layer] - SHIFTS[0] * rho[layer]))
    inner_tiles(0, tiles)
    advance(0, range(1, 7))
    prepare_outer(1)
    for side, layer in sides:
        faces[2, side] = partial[layer] + g_z * (guesses[1 - side] * float(stiff[0, 7]))
    send_faces(2)
    prepare_inner(1)
    serve_rest(WINDOW)
    with jax.named_scope('w_fc'):
        wait_faces(1)
        wait_far()
        wait_faces(2)
    for side, layer in sides:
        images[0, layer] = free[layer] * (images[0, layer] + halo[1, side])
    advance(0, (0, 7))
    tiles = outer_tiles(1)
    for side, layer in sides:
        along = [geometry_halo[side, d : d + 1, :] for d in range(4)]
        own = vectors[1, layer]
        term = in_plane(own, along) + (along[2] * float(stiff[0, 0]) + along[3]) * own
        term = term + halo[2, side] + (along[2] * float(stiff[0, 7])) * far_halo[side]
        images[1, layer] = free[layer] * (images[1, layer] + plane_sum(edge * term))
    inner_tiles(1, tiles)
    advance(1, range(8))
    prepare(2)
    tiles = outer_tiles(2)
    for side, layer in sides:
        faces[ITERS, side] = images[2, layer]
    send_faces(ITERS)
    inner_tiles(2, tiles)

    keys = list(range(ITERS)) + [(a, b) for b in range(ITERS) for a in range(b + 1)]
    spot = lax.broadcasted_iota(jnp.int32, (1, 128), 1)
    packed = jnp.zeros((1, 128), jnp.float32)
    for at, key in enumerate(keys):
        value = jnp.sum(jnp.sum(sums[key], axis=0, keepdims=True), axis=1, keepdims=True)
        packed = jnp.where(spot == at, value, packed)
    dots[...] = packed
    for step in range(1, n):
        dot_copy(step).start()
    all_dots[slab] = dots[...]
    with jax.named_scope('w_rest'):
        with_partners(lambda many: replies(many, 1).wait_recv())

    values = values + [gather_field(field) for field in range(1, fields)]
    for row in range(height):
        interface_ref[:, row * lanes : (row + 1) * lanes] = jnp.concatenate(
            [value[row : row + 1] for value in values], 0
        )
    for layer in range(1, 7):
        images[ITERS - 1, layer] = free[layer] * plane_sum(images[ITERS - 1, layer])
    with jax.named_scope('w_fc'):
        wait_faces(ITERS)
    for side, layer in ((0, 0), (1, 7)):
        images[ITERS - 1, layer] = free[layer] * (
            images[ITERS - 1, layer] + halo[ITERS, side]
        )
    with jax.named_scope('w_dots'):
        all_dot_copies().wait_recv()
    with jax.named_scope('solve'):
        total = jnp.sum(all_dots[...], axis=0)
        found = {
            key: jnp.broadcast_to(total[:, at : at + 1], (8, elems))
            for at, key in enumerate(keys)
        }
        steps_taken = solve(found)
    for layer in range(8):
        moved = boundary[layer]
        for turn in range(ITERS):
            moved = moved + steps_taken[turn] * vectors[turn, layer]
        velocity[layer] = moved
    for layer in range(8):
        left_over = residual[layer]
        for turn in range(ITERS):
            left_over = left_over - steps_taken[turn] * images[turn, layer]
        residual_out[layer] = left_over
    all_dot_copies().wait_send()
    for side in range(2):

        @pl.when(near[1 - side])
        def _():
            geometry_copy(side == 0).wait_send()

    with_partners(lambda many: rims(many - 1).wait_send())
    with_partners(lambda many: asks(many, 1).wait_send())
    for part in range(2):
        with_partners(lambda many: replies(many, part).wait_send())


def flush(*refs):
    count = (len(refs) - 1) // 2
    sem = refs[-1]
    copies = [
        pltpu.make_async_copy(refs[at], refs[count + at], sem.at[at]) for at in range(count)
    ]
    for copy in copies:
        copy.start()
    for copy in copies:
        copy.wait()


def body(n, donor_fields, interp_weights, donor_owner, donor_element, geometry, wall_flag, forcing):
    fields = donor_fields.shape[0]
    elems = geometry.shape[1]
    receptors = donor_element.shape[0]
    slots = 2 * REACH + 1
    lanes = 128
    count = receptors // lanes
    cube = (8, 8, 8, elems)
    phases = 1 + ITERS
    room = count // 2
    vmem = pl.BlockSpec(memory_space=pltpu.VMEM)
    hbm = pl.BlockSpec(memory_space=pltpu.HBM)
    shapes = (
        jax.ShapeDtypeStruct(cube, jnp.float32),
        jax.ShapeDtypeStruct(cube, jnp.float32),
        jax.ShapeDtypeStruct((fields, receptors), jnp.float32),
    )
    outputs = pl.pallas_call(
        functools.partial(kernel, n),
        out_shape=shapes,
        in_specs=[hbm] * 7,
        out_specs=(vmem, vmem, vmem),
        scratch_shapes=[
            pltpu.VMEM(cube, jnp.float32),
            pltpu.VMEM((fields, 512, elems), jnp.float32),
            pltpu.VMEM(cube, jnp.float32),
            pltpu.VMEM(interp_weights.shape, jnp.float32),
            pltpu.VMEM((count, lanes), jnp.int32),
            pltpu.VMEM((count, lanes), jnp.int32),
            pltpu.VMEM(geometry.shape, jnp.float32),
            pltpu.VMEM(wall_flag.shape, jnp.int32),
            pltpu.VMEM((3, count, lanes), jnp.float32),
            pltpu.VMEM((slots, 4, room, lanes), jnp.float32),
            pltpu.VMEM((slots * count, lanes), jnp.int32),
            pltpu.VMEM(cube, jnp.float32),
            pltpu.VMEM((8, 8, elems), jnp.float32),
            pltpu.VMEM((8, 8, elems), jnp.float32),
            pltpu.SemaphoreType.DMA((7,)),
            pltpu.VMEM((fields * 512, 2 * elems), jnp.bfloat16),
            pltpu.VMEM((slots, 4, room, lanes), jnp.float32),
            pltpu.VMEM((slots, fields, room, lanes), jnp.float32),
            pltpu.VMEM((slots, fields, room, lanes), jnp.float32),
            pltpu.VMEM((phases, 2, 8, 8, elems), jnp.float32),
            pltpu.VMEM((phases, 2, 8, 8, elems), jnp.float32),
            pltpu.VMEM((1, 128), jnp.float32),
            pltpu.VMEM((n, 1, 128), jnp.float32),
            pltpu.VMEM((ITERS,) + cube, jnp.float32),
            pltpu.VMEM((ITERS,) + cube, jnp.float32),
            pltpu.VMEM(cube, jnp.float32),
            pltpu.VMEM(cube, jnp.float32),
            pltpu.VMEM((2, 8, elems), jnp.float32),
            pltpu.VMEM((4, 8, elems), jnp.float32),
            pltpu.VMEM((2, 8, elems), jnp.float32),
            pltpu.VMEM((8, elems), jnp.float32),
            pltpu.VMEM((2, 8, 8, elems), jnp.float32),
            pltpu.VMEM((2, 8, 8, elems), jnp.float32),
        ]
        + [pltpu.VMEM(cube, jnp.float32)] * 4
        + [pltpu.SemaphoreType.DMA((3,)), pltpu.SemaphoreType.DMA((2, 2))]
        + [pltpu.SemaphoreType.DMA((3, 2))] * 2
        + [pltpu.SemaphoreType.DMA((2, 2))]
        + [pltpu.SemaphoreType.DMA((2,))]
        + [pltpu.SemaphoreType.DMA((2,))]
        + [pltpu.SemaphoreType.DMA((2,))] * 2,
        compiler_params=pltpu.CompilerParams(
            collective_id=0, has_side_effects=True, vmem_limit_bytes=48 * 1024 * 1024
        ),
    )(
        *[
            pltpu.with_memory_space_constraint(array, pltpu.HBM)
            for array in (
                donor_fields,
                interp_weights,
                donor_owner.reshape(count, lanes),
                donor_element.reshape(count, lanes),
                geometry,
                wall_flag,
                forcing.reshape(cube),
            )
        ]
    )
    velocity, residual, interface = pl.pallas_call(
        flush,
        out_shape=shapes,
        in_specs=[vmem] * 3,
        out_specs=(hbm,) * 3,
        scratch_shapes=[pltpu.SemaphoreType.DMA((3,))],
        compiler_params=pltpu.CompilerParams(vmem_limit_bytes=1024 * 1024),
    )(*outputs)
    return (velocity.reshape(512, elems), residual.reshape(512, elems), interface)


def solution(mesh):
    in_specs = (
        P(None, None, ("mesh", "dom")),
        P(None, None, ("mesh", "dom")),
        P(("mesh", "dom"), None),
        P(("mesh", "dom")),
        P(None, ("mesh", "dom")),
        P(None, ("mesh", "dom")),
        P(None, ("mesh", "dom")),
    )
    out_specs = (P(None, ("mesh", "dom")), P(None, ("mesh", "dom")), P(None, ("mesh", "dom")))
    return jax.shard_map(
        functools.partial(body, mesh.shape["dom"]),
        mesh=mesh,
        in_specs=in_specs,
        out_specs=out_specs,
        check_vma=False,
    )
```
